16 devices in a mesh: tp: 2 (over z), dp: 8 (over y, x, core).
Axes of the slice: x: 2, y: 2, z: 2, core: 2. Of those that a mesh axis runs over, the one named last changes fastest.
Arguments:
- w_query: bfloat16 [1024, 1024], P(('dp', 'tp'))
- b_query: bfloat16 [1024], P(('dp', 'tp'))
- w_key: bfloat16 [1024, 1024], P(('dp', 'tp'))
- b_key: bfloat16 [1024], P(('dp', 'tp'))
- w_value: bfloat16 [1024, 1024], P(('dp', 'tp'))
- b_value: bfloat16 [1024], P(('dp', 'tp'))
- w_out: bfloat16 [1024, 1024], P(('dp', 'tp'))
- w_gate: bfloat16 [2816, 1024], P(('dp', 'tp'))
- w_up: bfloat16 [2816, 1024], P(('dp', 'tp'))
- w_down: bfloat16 [1024, 2816], P(('dp', 'tp'))
- gain_attn: bfloat16 [1024], P(('dp', 'tp'))
- gain_mlp: bfloat16 [1024], P(('dp', 'tp'))
- hidden: bfloat16 [2048, 1024], P('dp')
- k_cache: bfloat16 [2048, 64, 16, 64], P('dp', None, 'tp')
- v_cache: bfloat16 [2048, 64, 16, 64], P('dp', None, 'tp')
- lengths: int32 [2048], P('dp')
Outputs:
- output 1: bfloat16 [1024, 1024], P('tp')
- output 2: bfloat16 [1024], P('tp')
- output 3: bfloat16 [1024, 1024], P('tp')
- output 4: bfloat16 [1024], P('tp')
- output 5: bfloat16 [1024, 1024], P('tp')
- output 6: bfloat16 [1024], P('tp')
- output 7: bfloat16 [1024, 1024], P(None, 'tp')
- output 8: bfloat16 [2816, 1024], P('tp')
- output 9: bfloat16 [2816, 1024], P('tp')
- output 10: bfloat16 [1024, 2816], P(None, 'tp')
- output 11: bfloat16 [1024], replicated
- output 12: bfloat16 [1024], replicated
- output 13: bfloat16 [2048, 1024], P('dp')
- output 14: bfloat16 [2048, 64, 16, 64], P('dp', None, 'tp')
- output 15: bfloat16 [2048, 64, 16, 64], P('dp', None, 'tp')
All inputs are finite; a program needn't handle non-finite values.
Results may differ from the reference program's by a relative error of at most 0.0153168.
Values are sent between devices in bfloat16 or wider.
A program may use at most 1 GiB of HBM per device.

```python
import jax
import jax.numpy as jnp
from jax import lax

HIDDEN = 1024
Q_HEADS = 16
KV_HEADS = 16
HEAD_DIM = 64
FF_DIM = 2816
TP_SIZE = 2
DP_SIZE = 8
ROLLOUTS = 256
CACHE_LEN = 64

BATCH = DP_SIZE * ROLLOUTS
KV_SLOTS = max(KV_HEADS, TP_SIZE)
REPEATS = KV_SLOTS // KV_HEADS
Q_ROWS = Q_HEADS * HEAD_DIM
KV_ROWS = KV_HEADS * HEAD_DIM
EPS = 1e-6
THETA = 1000000.0


def draw_lengths(key_a, key_b):
    first_draw = jax.random.randint(key_a, (BATCH,), 0, CACHE_LEN)
    second_draw = jax.random.randint(key_b, (BATCH,), 0, CACHE_LEN)
    lengths = 1 + (first_draw * second_draw) // CACHE_LEN
    row_index = jnp.arange(BATCH)
    lengths = jnp.where(row_index == 0, CACHE_LEN - 1, lengths)
    return jnp.where(row_index == 1, 1, lengths).astype(jnp.int32)


def setup_inputs(seed: int = 0) -> dict:
    keys = jax.random.split(jax.random.key(seed), 17)

    def normal_bf16(key_index, shape, scale):
        return (jax.random.normal(keys[key_index], shape, jnp.float32) * scale).astype(jnp.bfloat16)

    def gain_bf16(key_index):
        return (1.0 + 0.3 * jax.random.normal(keys[key_index], (HIDDEN,), jnp.float32)).astype(jnp.bfloat16)

    k_base = jax.random.normal(keys[13], (BATCH, CACHE_LEN, KV_HEADS, HEAD_DIM), jnp.float32)
    v_base = jax.random.normal(keys[14], (BATCH, CACHE_LEN, KV_HEADS, HEAD_DIM), jnp.float32)
    return {
        "w_query": normal_bf16(0, (Q_ROWS, HIDDEN), 3.0 * HIDDEN ** -0.5),
        "b_query": normal_bf16(1, (Q_ROWS,), 1.0),
        "w_key": normal_bf16(2, (KV_ROWS, HIDDEN), HIDDEN ** -0.5),
        "b_key": normal_bf16(3, (KV_ROWS,), 0.5),
        "w_value": normal_bf16(4, (KV_ROWS, HIDDEN), HIDDEN ** -0.5),
        "b_value": normal_bf16(5, (KV_ROWS,), 0.5),
        "w_out": normal_bf16(6, (HIDDEN, Q_ROWS), Q_ROWS ** -0.5),
        "w_gate": normal_bf16(7, (FF_DIM, HIDDEN), HIDDEN ** -0.5),
        "w_up": normal_bf16(8, (FF_DIM, HIDDEN), HIDDEN ** -0.5),
        "w_down": normal_bf16(9, (HIDDEN, FF_DIM), FF_DIM ** -0.5),
        "gain_attn": gain_bf16(10),
        "gain_mlp": gain_bf16(11),
        "hidden": normal_bf16(12, (BATCH, HIDDEN), 1.0),
        "k_cache": jnp.repeat(k_base, REPEATS, axis=2).astype(jnp.bfloat16),
        "v_cache": jnp.repeat(v_base, REPEATS, axis=2).astype(jnp.bfloat16),
        "lengths": draw_lengths(keys[15], keys[16]),
    }


def rms_scale(act_rows, gain_vec):
    rows_f32 = act_rows.astype(jnp.float32)
    inv_rms = lax.rsqrt(jnp.mean(rows_f32 * rows_f32, axis=-1, keepdims=True) + EPS)
    return (rows_f32 * inv_rms * gain_vec.astype(jnp.float32)).astype(jnp.bfloat16)


def linear_bias(act_rows, weight, bias_vec):
    result = jnp.dot(act_rows, weight.T, preferred_element_type=jnp.float32)
    return (result + bias_vec.astype(jnp.float32)).astype(jnp.bfloat16)


def linear_plain(act_rows, weight):
    return jnp.dot(act_rows, weight.T, preferred_element_type=jnp.float32).astype(jnp.bfloat16)


def rotary(vectors, positions):
    half_dim = HEAD_DIM // 2
    inv_freq = 1.0 / (THETA ** (jnp.arange(0, HEAD_DIM, 2, dtype=jnp.float32) / HEAD_DIM))
    angles = positions.astype(jnp.float32)[:, None] * inv_freq[None, :]
    cosine = jnp.cos(angles)[:, None, :]
    sine_tab = jnp.sin(angles)[:, None, :]
    vectors_f32 = vectors.astype(jnp.float32)
    first_half = vectors_f32[..., :half_dim]
    second_half = vectors_f32[..., half_dim:]
    return jnp.concatenate([first_half * cosine - second_half * sine_tab, second_half * cosine + first_half * sine_tab], axis=-1).astype(jnp.bfloat16)


def attend_block(block):
    query_block, keys_block, values_block, lens_block = block
    grouped = query_block.reshape(ROLLOUTS, KV_SLOTS, Q_HEADS // KV_SLOTS, HEAD_DIM).astype(jnp.float32)
    scores = jnp.einsum("bkgd,bskd->bkgs", grouped, keys_block.astype(jnp.float32)) * HEAD_DIM ** -0.5
    visible = (jnp.arange(CACHE_LEN)[None, :] <= lens_block[:, None])[:, None, None, :]
    attn_probs = jax.nn.softmax(jnp.where(visible, scores, -1e30), axis=-1).astype(jnp.bfloat16)
    mixed = jnp.einsum("bkgs,bskd->bkgd", attn_probs.astype(jnp.float32), values_block.astype(jnp.float32))
    return mixed.astype(jnp.bfloat16).reshape(ROLLOUTS, Q_ROWS)


def reference(w_query, b_query, w_key, b_key, w_value, b_value, w_out, w_gate, w_up, w_down, gain_attn, gain_mlp, hidden, k_cache, v_cache, lengths):
    w_key_tp = jnp.repeat(w_key.reshape(KV_HEADS, HEAD_DIM, HIDDEN), REPEATS, axis=0).reshape(KV_SLOTS * HEAD_DIM, HIDDEN)
    b_key_tp = jnp.repeat(b_key.reshape(KV_HEADS, HEAD_DIM), REPEATS, axis=0).reshape(KV_SLOTS * HEAD_DIM)
    w_value_tp = jnp.repeat(w_value.reshape(KV_HEADS, HEAD_DIM, HIDDEN), REPEATS, axis=0).reshape(KV_SLOTS * HEAD_DIM, HIDDEN)
    b_value_tp = jnp.repeat(b_value.reshape(KV_HEADS, HEAD_DIM), REPEATS, axis=0).reshape(KV_SLOTS * HEAD_DIM)
    normed = rms_scale(hidden, gain_attn)
    query_rot = rotary(linear_bias(normed, w_query, b_query).reshape(BATCH, Q_HEADS, HEAD_DIM), lengths)
    key_rot = rotary(linear_bias(normed, w_key_tp, b_key_tp).reshape(BATCH, KV_SLOTS, HEAD_DIM), lengths)
    value_new = linear_bias(normed, w_value_tp, b_value_tp).reshape(BATCH, KV_SLOTS, HEAD_DIM)
    at_slot = (jnp.arange(CACHE_LEN)[None, :] == lengths[:, None])[:, :, None, None]
    k_cache_out = jnp.where(at_slot, key_rot[:, None], k_cache)
    v_cache_out = jnp.where(at_slot, value_new[:, None], v_cache)
    attended = lax.map(attend_block, (
        query_rot.reshape(DP_SIZE, ROLLOUTS, Q_HEADS, HEAD_DIM),
        k_cache_out.reshape(DP_SIZE, ROLLOUTS, CACHE_LEN, KV_SLOTS, HEAD_DIM),
        v_cache_out.reshape(DP_SIZE, ROLLOUTS, CACHE_LEN, KV_SLOTS, HEAD_DIM),
        lengths.reshape(DP_SIZE, ROLLOUTS))).reshape(BATCH, Q_ROWS)
    attn_proj = linear_plain(attended, w_out)
    mid_hidden = (hidden.astype(jnp.float32) + attn_proj.astype(jnp.float32)).astype(jnp.bfloat16)
    normed_mlp = rms_scale(mid_hidden, gain_mlp)
    gate_val = linear_plain(normed_mlp, w_gate)
    up_val = linear_plain(normed_mlp, w_up)
    gated = (jax.nn.silu(gate_val.astype(jnp.float32)) * up_val.astype(jnp.float32)).astype(jnp.bfloat16)
    down_val = linear_plain(gated, w_down)
    hidden_out = (mid_hidden.astype(jnp.float32) + down_val.astype(jnp.float32)).astype(jnp.bfloat16)
    return (w_query, b_query, w_key_tp, b_key_tp, w_value_tp, b_value_tp, w_out, w_gate, w_up, w_down, gain_attn, gain_mlp, hidden_out, k_cache_out, v_cache_out)
```

```python
import jax
import jax.numpy as jnp
from jax import lax
from jax.experimental import pallas as pl
from jax.experimental.pallas import tpu as pltpu
from jax.sharding import PartitionSpec as P

EPS = 1e-6
THETA = 1000000.0
MESH = pl.DeviceIdType.MESH
F32 = jnp.float32
BF16 = jnp.bfloat16
ROW_BYTES = (((1,), (1,)), ((), ()))
NAT = (((1,), (0,)), ((), ()))
GROUP = 8


def dot(lhs, rhs, dims):
    return lax.dot_general(lhs, rhs, dims, preferred_element_type=F32)


class Place:
    def __init__(self):
        tp = lax.axis_index("tp")
        dp = lax.axis_index("dp")
        self.z = tp
        self.dp = dp
        self.y = dp // 4
        self.x = (dp // 2) % 2
        self.c = dp % 2
        self.home = lax.rem(self.y + self.z, 2) == 0
        self.away = lax.rem(self.y + self.z, 2) == 1
        self.to_x = (tp, dp + 2 - 4 * self.x)
        self.to_y = (tp, dp + 4 - 8 * self.y)
        self.to_c = (tp, dp + 1 - 2 * self.c)
        self.to_z = (1 - tp, dp)


def remote(src, dst, send, recv, device):
    return pltpu.make_async_remote_copy(
        src_ref=src, dst_ref=dst, send_sem=send, recv_sem=recv, device_id=device, device_id_type=MESH)


class Rows:
    def __init__(self, place, buf, pieces, sems):
        self.p, self.buf, self.pieces = place, buf, pieces
        self.sx, self.sy, self.sz, self.sc, self.r, self.rc = sems

    def block(self, k, core=0):
        p = self.p
        x = 1 - p.x if k & 1 else p.x
        z = 1 - p.z if k & 2 else p.z
        c = 1 - p.c if core else p.c
        return (x * 2 + c) * 2 + z

    def at(self, k, core=0):
        return self.buf.at[self.block(k, core)]

    def _own(self, send, recv, device):
        start = 0
        for ref in self.pieces:
            n = ref.shape[0]
            remote(ref, self.buf.at[self.block(0), pl.ds(start, n)], send, recv, device).start()
            start += n

    def _fwd(self, k, send, recv, device):
        remote(self.at(k), self.at(k), send, recv, device).start()

    def wait(self, k):
        remote(self.at(k), self.at(k), self.sx.at[k], self.r.at[k], self.p.to_x).wait_recv()

    def wait_core(self, k):
        remote(self.at(k, 1), self.at(k, 1), self.sc.at[k], self.rc.at[k], self.p.to_c).wait_recv()

    def own_away(self):
        @pl.when(self.p.away)
        def _():
            self._own(self.sz.at[0], self.r.at[2], self.p.to_z)

    def own_home(self):
        @pl.when(self.p.home)
        def _():
            self._own(self.sx.at[0], self.r.at[1], self.p.to_x)
            self._own(self.sy.at[0], self.r.at[0], self.p.to_y)
            self._own(self.sc.at[0], self.rc.at[0], self.p.to_c)

    def local(self):
        @pl.when(self.p.home)
        def _():
            start = 0
            for ref in self.pieces:
                n = ref.shape[0]
                self.buf[self.block(0), pl.ds(start, n)] = ref[...]
                start += n

    def k0(self):
        @pl.when(self.p.away)
        def _():
            self.wait(0)
            self._fwd(0, self.sx.at[0], self.r.at[1], self.p.to_x)
            self._fwd(0, self.sc.at[0], self.rc.at[0], self.p.to_c)

    def k2(self):
        self.wait(2)
        self._fwd(2, self.sx.at[2], self.r.at[3], self.p.to_x)

        @pl.when(self.p.home)
        def _():
            self._fwd(2, self.sy.at[2], self.r.at[2], self.p.to_y)

        self._fwd(2, self.sc.at[2], self.rc.at[2], self.p.to_c)

    def last(self, k):
        self.wait(k)
        self._fwd(k, self.sc.at[k], self.rc.at[k], self.p.to_c)

    def drain(self):
        p = self.p
        for k in (0, 2):
            remote(self.at(k), self.at(k), self.sx.at[k], self.r.at[k], p.to_x).wait_send()
        for k in range(4):
            remote(self.at(k), self.at(k), self.sc.at[k], self.rc.at[k], p.to_c).wait_send()

        @pl.when(p.home)
        def _():
            for k in (0, 2):
                remote(self.at(k), self.at(k), self.sy.at[k], self.r.at[k], p.to_y).wait_send()

        @pl.when(p.away)
        def _():
            remote(self.at(0), self.at(0), self.sz.at[0], self.r.at[0], p.to_z).wait_send()


class Cols:
    def __init__(self, place, buf, own, sems):
        self.p, self.buf, self.own = place, buf, own
        self.n = buf.shape[-1]
        self.sx, self.sy, self.sz, self.sc, self.r, self.rc = sems

    def block(self, k, core=0):
        p = self.p
        x = 1 - p.x if k & 1 else p.x
        y = 1 - p.y if k & 2 else p.y
        z = 1 - p.z if k & 4 else p.z
        c = 1 - p.c if core else p.c
        return (y * 4 + x * 2 + c) * 2 + z

    def at(self, k, core=0):
        return self.buf.at[self.block(k, core)]

    def half(self, z):
        return self.own.at[:, pl.ds(pl.multiple_of(z * self.n, 128), self.n)]

    def wait(self, k):
        remote(self.at(k), self.at(k), self.sx.at[k], self.r.at[k], self.p.to_x).wait_recv()

    def wait_core(self, k):
        remote(self.at(k, 1), self.at(k, 1), self.sc.at[k], self.rc.at[k], self.p.to_c).wait_recv()

    def send_z(self):
        remote(self.half(1 - self.p.z), self.at(0), self.sz.at[0], self.r.at[4], self.p.to_z).start()

    def _send(self, k, to, src=None):
        p = self.p
        src = self.at(k) if src is None else src
        if "x" in to:
            remote(src, self.at(k), self.sx.at[k], self.r.at[k ^ 1], p.to_x).start()
        if "y" in to:
            remote(src, self.at(k), self.sy.at[k], self.r.at[k ^ 2], p.to_y).start()
        if "c" in to:
            remote(src, self.at(k), self.sc.at[k], self.rc.at[k], p.to_c).start()

    def own_sends(self):
        self._send(0, "xyc", self.half(self.p.z))

    def local(self):
        self.buf[self.block(0)] = self.own[:, pl.ds(pl.multiple_of(self.p.z * self.n, 128), self.n)]

    ROUTE = {4: "xyc", 1: "yc", 2: "c", 5: "c", 6: "xc", 3: "c", 7: "c"}

    def step(self, k):
        self.wait(k)
        self._send(k, self.ROUTE[k])

    def drain(self):
        p = self.p
        for k, to in [(0, "xyc"), *self.ROUTE.items()]:
            for axis, sem, dev in (("x", self.sx, p.to_x), ("y", self.sy, p.to_y), ("c", self.sc, p.to_c)):
                if axis in to:
                    remote(self.at(k), self.at(k), sem.at[k], self.r.at[k], dev).wait_send()
        remote(self.at(0), self.at(0), self.sz.at[0], self.r.at[0], p.to_z).wait_send()


def row_sems():
    dma = pltpu.SemaphoreType.DMA
    return [dma((4,)), dma((4,)), dma((1,)), dma((4,)), dma((4,)), dma((4,))]


def col_sems():
    dma = pltpu.SemaphoreType.DMA
    return [dma((8,)), dma((8,)), dma((1,)), dma((8,)), dma((8,)), dma((8,))]


def layer_kernel(wq, wk, wv, wo, wg, wu, wd, small, x_ref, cos_ref, sin_ref, len_ref, k_hbm, v_hbm,
                 wqkv, wgu, wout, wdn, k_buf, v_buf, smalls, hid,
                 h_ref, sc_ref, o_ref, part, part_in, x1_ref, h2_ref, a_ref, down, down_in,
                 k_sem, v_sem, s_send, s_recv, p_send, p_recv, d_send, d_recv, *sems):
    place = Place()
    me = place.dp * 2 + place.z
    qkv = Rows(place, wqkv, (wq, wk, wv), sems[0:6])
    gu = Rows(place, wgu, (wg, wu), sems[6:12])
    out = Cols(place, wout, wo, sems[12:18])
    dn = Cols(place, wdn, wd, sems[18:24])
    order = [(0, 0), (0, 1), (2, 0), (2, 1), (1, 0), (1, 1), (3, 0), (3, 1)]

    def cache_copy(i):
        head = qkv.block(*order[i])
        return (pltpu.make_async_copy(k_hbm.at[:, head], k_buf.at[:, head], k_sem.at[i]),
                pltpu.make_async_copy(v_hbm.at[:, head], v_buf.at[:, head], v_sem.at[i]))

    barrier = pltpu.get_barrier_semaphore()
    for i in range(1, 16):
        other = lax.rem(me + i, 16)
        pl.semaphore_signal(barrier, inc=1, device_id=(other % 2, other // 2), device_id_type=MESH)
    for i in range(8):
        for copy in cache_copy(i):
            copy.start()
    pl.semaphore_wait(barrier, 15)

    def small_copy(i):
        other = lax.rem(me + i, 16)
        return remote(small, smalls.at[me], s_send.at[i], s_recv.at[i], (other % 2, other // 2))

    for i in range(1, 16):
        small_copy(i).start()
    qkv.own_away()
    qkv.own_home()
    out.send_z()
    gu.own_away()
    dn.send_z()

    qkv.local()
    gu.local()
    out.local()
    dn.local()
    smalls[me] = small[...]
    for i in range(1, 16):
        small_copy(i).wait_recv()

    def gain_row(i):
        pair = smalls[...].astype(F32).reshape(8, 2, 8, 128)
        rows = pair[:, 0, i] + pair[:, 1, i]
        return jnp.concatenate([rows[d:d + 1] for d in range(8)], axis=1)

    def normed(rows, i):
        inv = lax.rsqrt(jnp.mean(rows * rows, axis=-1, keepdims=True) + EPS)
        return (rows * inv * gain_row(i)).astype(BF16)

    h_ref[...] = normed(x_ref[...].astype(F32), 3)

    eye = lax.broadcasted_iota(jnp.int32, (64, 128), 1) % 64 == lax.broadcasted_iota(jnp.int32, (64, 128), 0)

    def bias_column(head, i):
        row = smalls[place.z * 8 + head].astype(F32)[i:i + 1]
        return jnp.sum(jnp.where(eye, row, 0.0), axis=1, keepdims=True)

    def attend(i):
        k, core = order[i]
        head = qkv.block(k, core)
        if core:
            qkv.wait_core(k)
        res = dot(wqkv[head], h_ref[...], ROW_BYTES)
        cos, sin = cos_ref[...], sin_ref[...]

        def rotated(start, b):
            v = (res[start:start + 64] + bias_column(head, b)).astype(BF16).astype(F32)
            lo, hi = v[:32], v[32:]
            return jnp.concatenate([lo * cos - hi * sin, hi * cos + lo * sin], axis=0).astype(BF16)

        q = rotated(0, 0).astype(F32)
        k_new = rotated(64, 1)
        v_new = (res[128:192] + bias_column(head, 2)).astype(BF16)
        lens = len_ref[...]
        for copy in cache_copy(i):
            copy.wait()

        def score_group(g, carry):
            rows = []
            for j in range(GROUP):
                s = g * GROUP + j
                kv = jnp.where(lens == s.astype(F32), k_new.astype(F32), k_buf[s, head].astype(F32))
                k_buf[s, head] = kv.astype(BF16)
                rows.append(jnp.sum(q * kv, axis=0, keepdims=True))
            sc_ref[pl.ds(pl.multiple_of(g * GROUP, GROUP), GROUP)] = jnp.concatenate(rows, axis=0)
            return carry

        lax.fori_loop(0, 64 // GROUP, score_group, 0)
        slot = lax.broadcasted_iota(jnp.int32, (64, 256), 0).astype(F32)
        scores = jnp.where(slot <= lens, sc_ref[...] * 0.125, -1e30)
        e = jnp.exp(scores - jnp.max(scores, axis=0, keepdims=True))
        sc_ref[...] = (e / jnp.sum(e, axis=0, keepdims=True)).astype(BF16).astype(F32)

        def value_group(g, acc):
            probs = sc_ref[pl.ds(pl.multiple_of(g * GROUP, GROUP), GROUP)]
            for j in range(GROUP):
                s = g * GROUP + j
                vv = jnp.where(lens == s.astype(F32), v_new.astype(F32), v_buf[s, head].astype(F32))
                v_buf[s, head] = vv.astype(BF16)
                acc = acc + probs[j:j + 1] * vv
            return acc

        acc = lax.fori_loop(0, 64 // GROUP, value_group, jnp.zeros((64, 256), F32))
        o_ref[pl.ds(pl.multiple_of(head * 64, 64), 64)] = acc.astype(BF16)

    qkv.k0()
    attend(0)
    attend(1)
    qkv.k2()
    out.own_sends()
    gu.own_home()
    dn.own_sends()
    attend(2)
    out.step(4)
    attend(3)
    out.step(1)
    out.step(2)
    qkv.last(1)
    attend(4)
    out.step(6)
    attend(5)
    qkv.last(3)
    attend(6)
    attend(7)
    for k in (5, 3, 7):
        out.step(k)
    gu.k0()
    gu.k2()
    dn.step(4)
    for k in range(8):
        out.wait_core(k)

    o = o_ref[...].T
    part[...] = dot(o, wout[...].reshape(1024, 512), ROW_BYTES).astype(BF16)
    swap = remote(part, part_in, p_send, p_recv, place.to_z)
    swap.start()
    dn.step(1)
    dn.step(2)
    swap.wait_recv()
    total = (part[...].astype(F32) + part_in[...].astype(F32)).astype(BF16)
    x1 = (x_ref[...].astype(F32) + total.astype(F32)).astype(BF16)
    x1_ref[...] = x1
    h2_ref[...] = normed(x1.astype(F32), 4)

    def gated(i):
        k, core = order[i]
        if core:
            gu.wait_core(k)
        block = gu.block(k, core)
        res = dot(wgu[block], h2_ref[...], ROW_BYTES).astype(BF16).astype(F32)
        g, u = res[:176], res[176:]
        a_ref[block] = (g / (1.0 + jnp.exp(-g)) * u).astype(BF16)

    for i in range(4):
        gated(i)
    dn.step(6)
    gu.last(1)
    gated(4)
    gated(5)
    dn.step(5)
    dn.step(3)
    gu.last(3)
    gated(6)
    gated(7)

    def down_copy(i, pair):
        rows = pl.ds(pl.multiple_of(pair * 128, 128), 128)
        return remote(down.at[rows], down_in.at[rows], d_send.at[i], d_recv.at[i], place.to_z)

    def down_pair(i):
        k, core = i // 2, i % 2
        if core:
            dn.wait_core(k)
            dn.wait_core(k + 4)
        pair = dn.block(k, core) // 2
        w = wdn[pl.ds(pair * 2, 2)].reshape(128, 1408)
        rows = pl.ds(pl.multiple_of(pair * 128, 128), 128)
        down[rows] = dot(w, a_ref[...].reshape(1408, 256), NAT).astype(BF16)
        down_copy(i, pair).start()

    for i in range(6):
        down_pair(i)
    dn.step(7)
    down_pair(6)
    down_pair(7)
    for i in range(8):
        pair = dn.block(i // 2, i % 2) // 2
        down_copy(i, pair).wait_recv()
        rows = pl.ds(pl.multiple_of(pair * 128, 128), 128)
        both = (down[rows].astype(F32) + down_in[rows].astype(F32)).T.astype(BF16).astype(F32)
        hid[:, rows] = (x1_ref[:, rows].astype(F32) + both).astype(BF16)

    for group in (qkv, gu, out, dn):
        group.drain()
    for i in range(1, 16):
        small_copy(i).wait_send()
    swap.wait_send()
    for i in range(8):
        down_copy(i, dn.block(i // 2, i % 2) // 2).wait_send()


def store_kernel(wqkv, wgu, wout, wdn, smalls, hid,
                 wq, wk, wv, wo, wg, wu, wd, hid_out, bq, bk, bv, ga, gm, sem):
    pairs = [(wdn, wd), (wgu.at[:, pl.ds(0, 176)], wg), (wgu.at[:, pl.ds(176, 176)], wu),
             (wqkv.at[:, pl.ds(0, 64)], wq), (wqkv.at[:, pl.ds(64, 64)], wk), (wqkv.at[:, pl.ds(128, 64)], wv),
             (wout, wo), (hid, hid_out)]
    copies = [pltpu.make_async_copy(src, dst, sem.at[i]) for i, (src, dst) in enumerate(pairs)]
    for copy in copies:
        copy.start()
    z = lax.axis_index("tp")
    plane = smalls[pl.ds(z * 8, 8)].astype(F32).reshape(4, 2, 8, 128)
    whole = smalls[...].astype(F32).reshape(8, 2, 8, 128)
    for i, ref in enumerate((bq, bk, bv)):
        ref[...] = (plane[:, 0, i] + plane[:, 1, i]).astype(BF16)
    for i, ref in enumerate((ga, gm)):
        ref[...] = (whole[:, 0, 3 + i] + whole[:, 1, 3 + i]).astype(BF16)
    for copy in copies:
        copy.wait()


def local_step(w_query, b_query, w_key, b_key, w_value, b_value, w_out, w_gate, w_up, w_down, gain_attn, gain_mlp,
               hidden, k_cache, v_cache, lengths):
    z = lax.axis_index("tp")
    vectors = jnp.stack([b_query, b_key, b_value, gain_attn, gain_mlp])
    zeros = jnp.zeros_like(vectors)
    small = jnp.concatenate([jnp.where(z == 0, vectors, zeros), jnp.where(z == 0, zeros, vectors)], axis=1)
    small = jnp.pad(small, ((0, 3), (0, 0)))
    inv_freq = 1.0 / (THETA ** (jnp.arange(0, 64, 2, dtype=F32) / 64))
    angles = inv_freq[:, None] * lengths.astype(F32)[None, :]
    cos, sin = jnp.cos(angles), jnp.sin(angles)
    lens = lengths.astype(F32)[None, :]
    k_view = jnp.transpose(k_cache, (1, 2, 3, 0))
    v_view = jnp.transpose(v_cache, (1, 2, 3, 0))

    vmem = pl.BlockSpec(memory_space=pltpu.VMEM)
    hbm = pl.BlockSpec(memory_space=pltpu.HBM)
    anywhere = pl.BlockSpec(memory_space=pl.ANY)
    dma = pltpu.SemaphoreType.DMA
    shapes = [(8, 192, 1024), (8, 352, 1024), (16, 64, 512), (16, 64, 1408), k_view.shape, v_view.shape,
              (16, 8, 128), (256, 1024)]
    held = pl.pallas_call(
        layer_kernel,
        out_shape=[pltpu.VMEM(s, BF16) for s in shapes],
        in_specs=[vmem] * 12 + [hbm] * 2,
        out_specs=[vmem] * 8,
        scratch_shapes=[
            pltpu.VMEM((256, 1024), BF16),
            pltpu.VMEM((64, 256), F32),
            pltpu.VMEM((512, 256), BF16),
            pltpu.VMEM((256, 1024), BF16),
            pltpu.VMEM((256, 1024), BF16),
            pltpu.VMEM((256, 1024), BF16),
            pltpu.VMEM((256, 1024), BF16),
            pltpu.VMEM((8, 176, 256), BF16),
            pltpu.VMEM((1024, 256), BF16),
            pltpu.VMEM((1024, 256), BF16),
            dma((8,)), dma((8,)), dma((16,)), dma((16,)), dma, dma, dma((8,)), dma((8,)),
            *row_sems(), *row_sems(), *col_sems(), *col_sems(),
        ],
        compiler_params=pltpu.CompilerParams(collective_id=0, has_side_effects=True, vmem_limit_bytes=9 * 2**20),
        name="layer",
    )(w_query, w_key, w_value, w_out, w_gate, w_up, w_down, small, hidden, cos, sin, lens, k_view, v_view)

    def shape(*dims):
        return jax.ShapeDtypeStruct(dims, BF16)

    outs = pl.pallas_call(
        store_kernel,
        out_shape=[shape(8, 64, 1024)] * 3 + [shape(16, 64, 512), shape(8, 176, 1024), shape(8, 176, 1024),
                   shape(16, 64, 1408), shape(256, 1024),
                   shape(4, 128), shape(4, 128), shape(4, 128), shape(8, 128), shape(8, 128)],
        in_specs=[anywhere] * 4 + [vmem, anywhere],
        out_specs=[hbm] * 8 + [vmem] * 5,
        scratch_shapes=[dma((10,))],
        compiler_params=pltpu.CompilerParams(vmem_limit_bytes=2 * 2**20),
        name="store",
    )(*held[:4], *held[6:])
    k_out, v_out = held[4:6]
    wq, wk, wv, wo, wg, wu, wd, hid, bq, bk, bv, ga, gm = outs
    flat = lambda a, n: a.reshape(-1, n)
    return (flat(wq, 1024), bq.reshape(512), flat(wk, 1024), bk.reshape(512), flat(wv, 1024), bv.reshape(512),
            flat(wo, 512), flat(wg, 1024), flat(wu, 1024), flat(wd, 1408), ga.reshape(1024), gm.reshape(1024),
            hid, jnp.transpose(k_out, (3, 0, 1, 2)), jnp.transpose(v_out, (3, 0, 1, 2)))


def solution(mesh):
    row_spec = P(("dp", "tp"), None)
    flat_spec = P(("dp", "tp"))
    cache_spec = P("dp", None, "tp", None)
    in_specs = (row_spec, flat_spec, row_spec, flat_spec, row_spec, flat_spec, row_spec, row_spec, row_spec, row_spec,
                flat_spec, flat_spec, P("dp", None), cache_spec, cache_spec, P("dp"))
    out_specs = (P("tp", None), P("tp"), P("tp", None), P("tp"), P("tp", None), P("tp"), P(None, "tp"), P("tp", None),
                 P("tp", None), P(None, "tp"), P(None), P(None), P("dp", None), cache_spec, cache_spec)
    return jax.shard_map(local_step, mesh=mesh, in_specs=in_specs, out_specs=out_specs, check_vma=False)
```

```python
import jax
import jax.numpy as jnp
from jax import lax
from jax.experimental import pallas as pl
from jax.experimental.pallas import tpu as pltpu
from jax.sharding import PartitionSpec as P

EPS = 1e-6
THETA = 1000000.0
MESH = pl.DeviceIdType.MESH
F32 = jnp.float32
BF16 = jnp.bfloat16
ROW_BYTES = (((1,), (1,)), ((), ()))
NAT = (((1,), (0,)), ((), ()))
GROUP = 8


def dot(lhs, rhs, dims):
    return lax.dot_general(lhs, rhs, dims, preferred_element_type=F32)


HOME_STEPS = (
    (
        ("s", "q0", 0, "c", 0), ("s", "q1", 0, "c", 0), ("s", "q2", 0, "c", 0), ("s", "g0", 0, "c", 0),
        ("s", "g1", 0, "c", 0), ("s", "u0", 0, "c", 0), ("s", "u1", 0, "c", 0), ("s", "o", 0, "c", 0),
        ("s", "d", 0, "c", 0), ("s", "o", "z", "z", 4), ("s", "d", "z", "z", 4), ("s", "q0", 0, "y", 0),
        ("s", "q0", 0, "x", 1),
    ),
    (
        ("s", "q2", 0, "y", 0), ("s", "q2", 0, "x", 1),
    ),
    (
        ("s", "o", 0, "y", 2), ("s", "o", 0, "x", 1), ("w", "q0", "c", 0), ("w", "q1", "c", 0), ("w", "q2", "c", 0),
    ),
    (
        ("w", "q0", "t"), ("w", "q0", 1), ("s", "q0", 1, "c", 1), ("w", "q0", 2), ("s", "q0", 2, "c", 2),
        ("s", "q0", "t", "z", 2), ("s", "q1", 0, "y", 0), ("s", "q1", 0, "x", 1), ("w", "o", 2), ("s", "o", 2, "c", 2),
        ("w", "q2", 1), ("s", "q2", 1, "c", 1), ("w", "q2", 2), ("s", "q2", 2, "c", 2), ("s", "q2", 2, "y", 2),
        ("s", "q2", 2, "x", 3), ("w", "o", 1), ("s", "o", 1, "c", 1), ("w", "o", 4), ("s", "o", 4, "c", 4),
        ("w", "q1", "t"), ("s", "q1", "t", "z", 2), ("w", "o", 6), ("s", "o", 6, "c", 6), ("s", "o", 4, "y", 6),
        ("s", "o", 4, "x", 5), ("w", "q1", 1), ("s", "q1", 1, "c", 1), ("w", "q1", 2), ("s", "q1", 2, "c", 2),
    ),
    (
        ("s", "q1", 1, "y", 1), ("s", "o", 2, "x", 3), ("w", "q0", "c", 1), ("w", "q1", "c", 1), ("w", "q2", "c", 1),
    ),
    (
        ("w", "u1", "t"), ("w", "q2", 3), ("s", "q2", 3, "c", 3), ("s", "u1", "t", "z", 2), ("s", "u1", 0, "y", 0),
        ("s", "o", 6, "x", 7), ("s", "q1", 2, "x", 3),
    ),
    (
        ("w", "u1", 2), ("s", "u1", 2, "c", 2), ("w", "o", 5), ("s", "o", 5, "c", 5), ("w", "q0", "c", 2),
        ("w", "q1", "c", 2), ("w", "q2", "c", 2),
    ),
    (
        ("w", "o", 3), ("s", "o", 3, "c", 3), ("w", "g0", "t"), ("w", "o", 7), ("s", "o", 7, "c", 7),
        ("s", "g0", "t", "z", 2), ("s", "o", 5, "y", 7), ("s", "u1", 0, "x", 1), ("w", "u0", 2), ("s", "u0", 2, "c", 2),
        ("s", "u0", 0, "y", 0), ("w", "q1", 3), ("s", "q1", 3, "c", 3), ("w", "g1", "t"), ("s", "g1", "t", "z", 2),
        ("s", "u0", 0, "x", 1), ("w", "g0", 2), ("s", "g0", 2, "c", 2), ("s", "u0", 2, "y", 2), ("w", "q0", 3),
        ("s", "q0", 3, "c", 3),
    ),
    (
        ("w", "u1", 1), ("s", "u1", 1, "c", 1), ("s", "g0", 0, "x", 1), ("w", "q0", "c", 3), ("w", "q1", "c", 3),
        ("w", "q2", "c", 3),
    ),
    (
        ("w", "g1", 2), ("s", "g1", 2, "c", 2), ("s", "g0", 0, "y", 0), ("w", "o", "c", 0), ("w", "o", "c", 1),
        ("w", "o", "c", 2), ("w", "o", "c", 3), ("w", "o", "c", 4), ("w", "o", "c", 5), ("w", "o", "c", 6),
        ("w", "o", "c", 7),
    ),
    (
        ("w", "d", 2), ("s", "d", 2, "c", 2), ("w", "u0", 1), ("s", "u0", 1, "c", 1), ("s", "g1", 0, "x", 1),
        ("w", "d", 4), ("s", "d", 4, "c", 4), ("s", "u0", 1, "y", 1), ("w", "d", 6), ("s", "d", 6, "c", 6),
        ("w", "g0", 1), ("s", "g0", 1, "c", 1), ("s", "g1", 2, "x", 3), ("s", "g1", 0, "y", 0), ("w", "u1", 3),
        ("s", "u1", 3, "c", 3), ("w", "g1", 1), ("s", "g1", 1, "c", 1), ("s", "d", 0, "x", 1), ("s", "g1", 1, "y", 1),
        ("w", "g1", 3), ("s", "g1", 3, "c", 3), ("s", "d", 4, "x", 5), ("w", "g0", 3), ("s", "g0", 3, "c", 3),
    ),
    (
        ("s", "d", 0, "y", 2),
    ),
    (
        ("w", "d", 1), ("s", "d", 1, "c", 1), ("w", "g0", "c", 0), ("w", "g1", "c", 0), ("w", "u0", "c", 0),
        ("w", "u1", "c", 0),
    ),
    (
        ("s", "d", 2, "x", 3),
    ),
    (
        ("w", "u0", 3), ("s", "u0", 3, "c", 3), ("w", "g0", "c", 1), ("w", "g1", "c", 1), ("w", "u0", "c", 1),
        ("w", "u1", "c", 1),
    ),
    (),
    (
        ("s", "d", 4, "y", 6), ("w", "g0", "c", 2), ("w", "g1", "c", 2), ("w", "u0", "c", 2), ("w", "u1", "c", 2),
    ),
    (),
    (
        ("w", "d", 5), ("s", "d", 5, "c", 5), ("w", "g0", "c", 3), ("w", "g1", "c", 3), ("w", "u0", "c", 3),
        ("w", "u1", "c", 3),
    ),
    (),
    (
        ("w", "d", "c", 0), ("w", "d", "c", 4),
    ),
    (),
    (
        ("s", "d", 5, "y", 7), ("w", "d", "c", 1), ("w", "d", "c", 5),
    ),
    (),
    (
        ("w", "d", "c", 2), ("w", "d", "c", 6),
    ),
    (
        ("w", "d", 3), ("s", "d", 3, "c", 3), ("w", "d", 7), ("s", "d", 7, "c", 7),
    ),
    (
        ("w", "d", "c", 3), ("w", "d", "c", 7),
    ),
    (),
    (),
    (),
    (),
    (),
    (),
    (),
    (),
    (),
)
HOME_BLOCKS = {
    "attend": ((0, 0), (0, 1), (1, 0), (1, 1), (2, 0), (2, 1), (3, 0), (3, 1)),
    "gated": ((0, 0), (0, 1), (1, 0), (1, 1), (2, 0), (2, 1), (3, 0), (3, 1)),
    "down": ((0, 0), (0, 1), (1, 0), (1, 1), (2, 0), (2, 1), (3, 0), (3, 1)),
}
AWAY_STEPS = (
    (
        ("s", "o", 0, "c", 0), ("s", "d", 0, "c", 0), ("s", "q0", "own", "z", 2), ("s", "q0", "own", "y", "t"),
        ("s", "o", 0, "x", 1), ("s", "d", 0, "x", 1),
    ),
    (
        ("s", "q2", "own", "z", 2), ("s", "o", 0, "y", 2), ("s", "q1", "own", "y", "t"), ("w", "o", 1),
        ("s", "o", 1, "c", 1), ("w", "o", 4), ("s", "o", 4, "c", 4), ("s", "o", 4, "x", 5), ("s", "o", "z", "z", 4),
        ("w", "q0", 0), ("s", "q0", 0, "c", 0), ("s", "q0", 0, "x", 1), ("s", "q1", "own", "z", 2),
        ("s", "o", 4, "y", 6), ("s", "u1", "own", "y", "t"), ("w", "d", 1), ("s", "d", 1, "c", 1), ("w", "d", 4),
        ("s", "d", 4, "c", 4), ("w", "q2", 0), ("s", "q2", 0, "c", 0), ("s", "q2", 0, "x", 1),
        ("s", "u1", "own", "z", 2), ("w", "o", 5), ("s", "o", 5, "c", 5), ("w", "o", 2), ("s", "o", 2, "c", 2),
        ("s", "g0", "own", "y", "t"), ("s", "o", 2, "x", 3), ("w", "q0", 2), ("s", "q0", 2, "c", 2), ("w", "q0", 1),
        ("s", "q0", 1, "c", 1), ("w", "q1", 0), ("s", "q1", 0, "c", 0),
    ),
    (
        ("s", "u0", "own", "z", 2), ("s", "q0", 2, "x", 3), ("w", "q0", "c", 0), ("w", "q1", "c", 0),
        ("w", "q2", "c", 0),
    ),
    (
        ("w", "q1", 2), ("s", "q1", 2, "c", 2), ("w", "q2", 1), ("s", "q2", 1, "c", 1), ("w", "q2", 2),
        ("s", "q2", 2, "c", 2), ("s", "g1", "own", "y", "t"), ("s", "q2", 2, "x", 3),
    ),
    (
        ("w", "o", 3), ("s", "o", 3, "c", 3), ("w", "o", 6), ("s", "o", 6, "c", 6), ("s", "g0", "own", "z", 2),
        ("s", "q1", 2, "x", 3), ("w", "q0", "c", 2), ("w", "q1", "c", 2), ("w", "q2", "c", 2),
    ),
    (
        ("w", "q0", 3), ("s", "q0", 3, "c", 3), ("w", "q1", 1), ("s", "q1", 1, "c", 1), ("s", "q0", 3, "y", 3),
    ),
    (
        ("w", "q2", 3), ("s", "q2", 3, "c", 3), ("w", "u1", 2), ("s", "u1", 2, "c", 2), ("s", "g1", "own", "z", 2),
        ("s", "d", 0, "y", 2), ("s", "u1", 2, "x", 3), ("w", "q0", "c", 1), ("w", "q1", "c", 1), ("w", "q2", "c", 1),
    ),
    (
        ("w", "u1", 0), ("s", "u1", 0, "c", 0), ("s", "d", "z", "z", 4), ("w", "o", 7), ("s", "o", 7, "c", 7),
        ("w", "q1", 3), ("s", "q1", 3, "c", 3),
    ),
    (
        ("w", "g0", 2), ("s", "g0", 2, "c", 2), ("s", "d", 4, "y", 6), ("s", "u1", 0, "x", 1), ("w", "q0", "c", 3),
        ("w", "q1", "c", 3), ("w", "q2", "c", 3),
    ),
    (
        ("w", "u0", 0), ("s", "u0", 0, "c", 0), ("w", "o", "c", 0), ("w", "o", "c", 1), ("w", "o", "c", 2),
        ("w", "o", "c", 3), ("w", "o", "c", 4), ("w", "o", "c", 5), ("w", "o", "c", 6), ("w", "o", "c", 7),
    ),
    (
        ("w", "u1", 3), ("s", "u1", 3, "c", 3), ("s", "u1", 3, "y", 3), ("s", "g0", 2, "x", 3), ("w", "g1", 2),
        ("s", "g1", 2, "c", 2), ("w", "u0", 2), ("s", "u0", 2, "c", 2), ("w", "u1", 1), ("s", "u1", 1, "c", 1),
        ("s", "u0", 2, "x", 3), ("w", "g0", 0), ("s", "g0", 0, "c", 0), ("w", "g0", 3), ("s", "g0", 3, "c", 3),
        ("s", "g0", 3, "y", 3), ("s", "g0", 0, "x", 1), ("w", "u0", 1), ("s", "u0", 1, "c", 1), ("w", "u0", 3),
        ("s", "u0", 3, "c", 3), ("s", "u0", 3, "y", 3), ("s", "g1", 2, "x", 3),
    ),
    (
        ("w", "g1", 0), ("s", "g1", 0, "c", 0), ("w", "g0", 1), ("s", "g0", 1, "c", 1), ("s", "d", 4, "x", 5),
    ),
    (),
    (
        ("w", "g0", "c", 2), ("w", "g1", "c", 2), ("w", "u0", "c", 2), ("w", "u1", "c", 2),
    ),
    (
        ("w", "g0", "c", 0), ("w", "g1", "c", 0), ("w", "u0", "c", 0), ("w", "u1", "c", 0),
    ),
    (
        ("w", "g1", 1), ("s", "g1", 1, "c", 1),
    ),
    (
        ("w", "g1", 3), ("s", "g1", 3, "c", 3),
    ),
    (
        ("w", "g0", "c", 1), ("w", "g1", "c", 1), ("w", "u0", "c", 1), ("w", "u1", "c", 1),
    ),
    (
        ("w", "g0", "c", 3), ("w", "g1", "c", 3), ("w", "u0", "c", 3), ("w", "u1", "c", 3),
    ),
    (),
    (
        ("w", "d", 2), ("s", "d", 2, "c", 2), ("s", "d", 2, "x", 3), ("w", "d", "c", 0), ("w", "d", "c", 4),
    ),
    (
        ("w", "d", 5), ("s", "d", 5, "c", 5), ("s", "d", 5, "y", 7),
    ),
    (
        ("w", "d", "c", 1), ("w", "d", "c", 5),
    ),
    (
        ("w", "d", 6), ("s", "d", 6, "c", 6),
    ),
    (
        ("w", "d", "c", 2), ("w", "d", "c", 6),
    ),
    (
        ("w", "d", 3), ("s", "d", 3, "c", 3), ("w", "d", 7), ("s", "d", 7, "c", 7),
    ),
    (
        ("w", "d", "c", 3), ("w", "d", "c", 7),
    ),
    (),
    (),
    (),
    (),
    (),
    (),
    (),
    (),
    (),
)
AWAY_BLOCKS = {
    "attend": ((0, 0), (0, 1), (2, 0), (2, 1), (1, 0), (1, 1), (3, 0), (3, 1)),
    "gated": ((0, 0), (2, 0), (2, 1), (0, 1), (1, 0), (3, 0), (1, 1), (3, 1)),
    "down": ((0, 0), (0, 1), (1, 0), (1, 1), (2, 0), (2, 1), (3, 0), (3, 1)),
}


class Place:
    def __init__(self):
        tp = lax.axis_index("tp")
        dp = lax.axis_index("dp")
        self.z = tp
        self.dp = dp
        self.y = dp // 4
        self.x = (dp // 2) % 2
        self.c = dp % 2
        self.far = lax.rem(self.y + self.z, 2)
        self.device = {
            "x": (tp, dp + 2 - 4 * self.x),
            "y": (tp, dp + 4 - 8 * self.y),
            "c": (tp, dp + 1 - 2 * self.c),
            "z": (1 - tp, dp),
        }

    def at(self, axis, flip):
        here = getattr(self, axis)
        return 1 - here if flip else here

    def row_block(self, k, core=0):
        return (self.at("x", k & 1) * 2 + self.at("c", core)) * 2 + self.at("z", k & 2)

    def col_block(self, k, core=0):
        return (self.at("y", k & 2) * 4 + self.at("x", k & 1) * 2 + self.at("c", core)) * 2 + self.at("z", k & 4)


def remote(src, dst, send, recv, device):
    return pltpu.make_async_remote_copy(
        src_ref=src, dst_ref=dst, send_sem=send, recv_sem=recv, device_id=device, device_id_type=MESH)


class Rows:
    def __init__(self, place, buf, start, own, through, index, sems):
        self.p, self.buf, self.start, self.own, self.through = place, buf, start, own, through
        self.i, (self.send, self.r, self.rc) = index, sems
        self.n = own.shape[0]

    def block(self, k, core=0):
        return self.buf.at[self.p.row_block(k, core), pl.ds(self.start, self.n)]

    def copy(self, k, link, home):
        p = self.p
        slot = {"own": 0, "t": 4}.get(k, k)
        send = self.send.at[self.i, "xyzc".index(link), slot]
        if k == "own" or (home and k == 0):
            src = self.own
        elif k == "t":
            src = self.through
        else:
            src = self.block(k)
        if k == "own" and link == "y":
            dst, recv = self.through, self.r.at[self.i, 4]
        else:
            dst = self.block(0 if k in ("own", "t") else k)
            got = 2 if link == "z" else k ^ 1 if link == "x" else k
            recv = self.rc.at[self.i, k] if link == "c" else self.r.at[self.i, got]
        return remote(src, dst, send, recv, p.device[link])

    def wait(self, k, core):
        if k == "t":
            ref, recv = self.through, self.r.at[self.i, 4]
        else:
            ref, recv = self.block(k, core), (self.rc if core else self.r).at[self.i, k]
        remote(ref, ref, self.send.at[self.i, 0, 0], recv, self.p.device["x"]).wait_recv()

    def local(self):
        @pl.when(self.p.far == 0)
        def _():
            self.buf[self.p.row_block(0), pl.ds(self.start, self.n)] = self.own[...]


class Cols:
    def __init__(self, place, buf, own, index, sems):
        self.p, self.buf, self.own = place, buf, own
        self.n = buf.shape[-1]
        self.i, (self.send, self.r, self.rc) = index, sems

    def block(self, k, core=0):
        return self.buf.at[self.p.col_block(k, core)]

    def half(self, z):
        return self.own.at[:, pl.ds(pl.multiple_of(z * self.n, 128), self.n)]

    def copy(self, k, link, home):
        p = self.p
        if link == "z":
            return remote(self.half(1 - p.z), self.block(0), self.send.at[self.i, 2, 0], self.r.at[self.i, 4], p.device["z"])
        src = self.half(p.z) if k == 0 else self.block(k)
        got = k ^ 1 if link == "x" else k ^ 2
        recv = self.rc.at[self.i, k] if link == "c" else self.r.at[self.i, got]
        return remote(src, self.block(k), self.send.at[self.i, "xyzc".index(link), k], recv, p.device[link])

    def wait(self, k, core):
        ref, recv = self.block(k, core), (self.rc if core else self.r).at[self.i, k]
        remote(ref, ref, self.send.at[self.i, 0, 0], recv, self.p.device["x"]).wait_recv()

    def local(self):
        self.buf[self.p.col_block(0)] = self.own[:, pl.ds(pl.multiple_of(self.p.z * self.n, 128), self.n)]


def layer_kernel(wq, wk, wv, wo, wg, wu, wd, small, x_ref, cos_ref, sin_ref, len_ref, k_hbm, v_hbm,
                 wqkv, wgu, wout, wdn, k_lo, k_hi, v_lo, v_hi, smalls, hid,
                 h_ref, sc_ref, o_ref, part, part_in, x1_ref, h2_ref, a_ref, down, down_in, t_q, t_gu,
                 k_sem, v_sem, s_send, s_recv, p_send, p_recv, d_send, d_recv, row_s, row_r, row_c, col_s, col_r, col_c):
    place = Place()
    me = place.dp * 2 + place.z
    row_sem, col_sem = (row_s, row_r, row_c), (col_s, col_r, col_c)
    half = pl.ds(0, 88), pl.ds(88, 88)
    chunks = {}
    for i, ref in enumerate((wq, wk, wv)):
        chunks[f"q{i}"] = Rows(place, wqkv, 64 * i, ref, t_q.at[i], i, row_sem)
    for i in range(4):
        ref = (wg, wu)[i // 2].at[half[i % 2]]
        chunks["gu"[i // 2] + str(i % 2)] = Rows(place, wgu, 88 * i, ref, t_gu.at[i], 3 + i, row_sem)
    chunks["o"] = Cols(place, wout, wo, 0, col_sem)
    chunks["d"] = Cols(place, wdn, wd, 1, col_sem)
    roles = ((0, HOME_STEPS, HOME_BLOCKS), (1, AWAY_STEPS, AWAY_BLOCKS))
    step = iter(range(len(HOME_STEPS)))

    def go():
        now = next(step)
        for far, steps, _ in roles:
            if steps[now]:
                @pl.when(place.far == far)
                def _(far=far, steps=steps):
                    for action in steps[now]:
                        chunk = chunks[action[1]]
                        if action[0] == "s":
                            chunk.copy(action[2], action[3], far == 0).start()
                        elif action[2] == "c":
                            chunk.wait(action[3], 1)
                        else:
                            chunk.wait(action[2], 0)

    def by_role(kind, i, place_of, swap=False):
        home, away = (place_of(*blocks[kind][i]) for _, _, blocks in roles)
        if swap:
            home, away = away, home
        return home + place.far * (away - home)

    def cache_copy(i):
        head = by_role("attend", i, place.row_block)
        copies = []
        for hbm, lo, hi, sem in ((k_hbm, k_lo, k_hi, k_sem), (v_hbm, v_lo, v_hi, v_sem)):
            copies.append(pltpu.make_async_copy(hbm.at[pl.ds(0, 32), head], lo.at[:, head], sem.at[2 * i]))
            copies.append(pltpu.make_async_copy(hbm.at[pl.ds(32, 32), head], hi.at[:, head], sem.at[2 * i + 1]))
        return copies

    barrier = pltpu.get_barrier_semaphore()
    for i in range(1, 16):
        other = lax.rem(me + i, 16)
        pl.semaphore_signal(barrier, inc=1, device_id=(other % 2, other // 2), device_id_type=MESH)
    for i in range(8):
        for copy in cache_copy(i):
            copy.start()
    pl.semaphore_wait(barrier, 15)

    def small_copy(i):
        other = lax.rem(me + i, 16)
        return remote(small, smalls.at[me], s_send.at[i], s_recv.at[i], (other % 2, other // 2))

    for i in range(1, 16):
        small_copy(i).start()
    go()

    for chunk in chunks.values():
        chunk.local()
    smalls[me] = small[...]
    for i in range(1, 16):
        small_copy(i).wait_recv()

    def gain_row(i):
        pair = smalls[...].astype(F32).reshape(8, 2, 8, 128)
        rows = pair[:, 0, i] + pair[:, 1, i]
        return jnp.concatenate([rows[d:d + 1] for d in range(8)], axis=1)

    def normed(rows, i):
        inv = lax.rsqrt(jnp.mean(rows * rows, axis=-1, keepdims=True) + EPS)
        return (rows * inv * gain_row(i)).astype(BF16)

    h_ref[...] = normed(x_ref[...].astype(F32), 3)

    eye = lax.broadcasted_iota(jnp.int32, (64, 128), 1) % 64 == lax.broadcasted_iota(jnp.int32, (64, 128), 0)

    def bias_column(head, i):
        row = smalls[place.z * 8 + head].astype(F32)[i:i + 1]
        return jnp.sum(jnp.where(eye, row, 0.0), axis=1, keepdims=True)

    def attend(i):
        head = by_role("attend", i, place.row_block)
        res = dot(wqkv[head], h_ref[...], ROW_BYTES)
        cos, sin = cos_ref[...], sin_ref[...]

        def rotated(start, b):
            v = (res[start:start + 64] + bias_column(head, b)).astype(BF16).astype(F32)
            lo, hi = v[:32], v[32:]
            return jnp.concatenate([lo * cos - hi * sin, hi * cos + lo * sin], axis=0).astype(BF16)

        q = rotated(0, 0).astype(F32)
        k_new = rotated(64, 1)
        v_new = (res[128:192] + bias_column(head, 2)).astype(BF16)
        lens = len_ref[...]
        for copy in cache_copy(i):
            copy.wait()

        for base, buf in ((0, k_lo), (32, k_hi)):
            def score_group(g, carry, base=base, buf=buf):
                rows = []
                for j in range(GROUP):
                    s = g * GROUP + j
                    kv = jnp.where(lens == (base + s).astype(F32), k_new.astype(F32), buf[s, head].astype(F32))
                    buf[s, head] = kv.astype(BF16)
                    rows.append(jnp.sum(q * kv, axis=0, keepdims=True))
                sc_ref[pl.ds(pl.multiple_of(base + g * GROUP, GROUP), GROUP)] = jnp.concatenate(rows, axis=0)
                return carry

            lax.fori_loop(0, 32 // GROUP, score_group, 0)
        slot = lax.broadcasted_iota(jnp.int32, (64, 256), 0).astype(F32)
        scores = jnp.where(slot <= lens, sc_ref[...] * 0.125, -1e30)
        e = jnp.exp(scores - jnp.max(scores, axis=0, keepdims=True))
        sc_ref[...] = (e / jnp.sum(e, axis=0, keepdims=True)).astype(BF16).astype(F32)

        acc = jnp.zeros((64, 256), F32)
        for base, buf in ((0, v_lo), (32, v_hi)):
            def value_group(g, acc, base=base, buf=buf):
                probs = sc_ref[pl.ds(pl.multiple_of(base + g * GROUP, GROUP), GROUP)]
                for j in range(GROUP):
                    s = g * GROUP + j
                    vv = jnp.where(lens == (base + s).astype(F32), v_new.astype(F32), buf[s, head].astype(F32))
                    buf[s, head] = vv.astype(BF16)
                    acc = acc + probs[j:j + 1] * vv
                return acc

            acc = lax.fori_loop(0, 32 // GROUP, value_group, acc)
        o_ref[pl.ds(pl.multiple_of(head * 64, 64), 64)] = acc.astype(BF16)

    go()
    for i in range(8):
        attend(i)
        go()

    o = o_ref[...].T
    part[...] = dot(o, wout[...].reshape(1024, 512), ROW_BYTES).astype(BF16)
    swap = remote(part, part_in, p_send, p_recv, place.device["z"])
    swap.start()
    go()
    swap.wait_recv()
    total = (part[...].astype(F32) + part_in[...].astype(F32)).astype(BF16)
    x1 = (x_ref[...].astype(F32) + total.astype(F32)).astype(BF16)
    x1_ref[...] = x1
    h2_ref[...] = normed(x1.astype(F32), 4)
    go()

    for i in range(8):
        block = by_role("gated", i, place.row_block)
        res = dot(wgu[block], h2_ref[...], ROW_BYTES).astype(BF16).astype(F32)
        g, u = res[:176], res[176:]
        a_ref[block] = (g / (1.0 + jnp.exp(-g)) * u).astype(BF16)
        go()

    def pair_of(k, core):
        return place.col_block(k, core) // 2

    def down_copy(i, swap=False):
        pair = by_role("down", i, pair_of, swap)
        rows = pl.ds(pl.multiple_of(pair * 128, 128), 128)
        return rows, pair, remote(down.at[rows], down_in.at[rows], d_send.at[pair], d_recv.at[pair], place.device["z"])

    for i in range(8):
        rows, pair, copy = down_copy(i)
        w = wdn[pl.ds(pair * 2, 2)].reshape(128, 1408)
        down[rows] = dot(w, a_ref[...].reshape(1408, 256), NAT).astype(BF16)
        copy.start()
        go()
    for i in range(8):
        rows, _, copy = down_copy(i, True)
        copy.wait_recv()
        both = (down[rows].astype(F32) + down_in[rows].astype(F32)).T.astype(BF16).astype(F32)
        hid[:, rows] = (x1_ref[:, rows].astype(F32) + both).astype(BF16)
        go()

    for far, steps, _ in roles:
        @pl.when(place.far == far)
        def _(far=far, steps=steps):
            for action in sum(steps, ()):
                if action[0] == "s":
                    chunks[action[1]].copy(action[2], action[3], far == 0).wait_send()

    for i in range(1, 16):
        small_copy(i).wait_send()
    swap.wait_send()
    for i in range(8):
        down_copy(i)[2].wait_send()


def store_kernel(wqkv, wgu, wout, wdn, k_lo, k_hi, v_lo, v_hi, smalls, hid,
                 wq, wk, wv, wo, wg, wu, wd, k_out, v_out, hid_out, bq, bk, bv, ga, gm, sem):
    lo, hi = pl.ds(0, 32), pl.ds(32, 32)
    pairs = [(k_lo, k_out.at[lo]), (k_hi, k_out.at[hi]), (v_lo, v_out.at[lo]), (v_hi, v_out.at[hi]),
             (wdn, wd), (wgu.at[:, pl.ds(0, 176)], wg), (wgu.at[:, pl.ds(176, 176)], wu),
             (wqkv.at[:, pl.ds(0, 64)], wq), (wqkv.at[:, pl.ds(64, 64)], wk), (wqkv.at[:, pl.ds(128, 64)], wv),
             (wout, wo), (hid, hid_out)]
    copies = [pltpu.make_async_copy(src, dst, sem.at[i]) for i, (src, dst) in enumerate(pairs)]
    for copy in copies:
        copy.start()
    z = lax.axis_index("tp")
    plane = smalls[pl.ds(z * 8, 8)].astype(F32).reshape(4, 2, 8, 128)
    whole = smalls[...].astype(F32).reshape(8, 2, 8, 128)
    for i, ref in enumerate((bq, bk, bv)):
        ref[...] = (plane[:, 0, i] + plane[:, 1, i]).astype(BF16)
    for i, ref in enumerate((ga, gm)):
        ref[...] = (whole[:, 0, 3 + i] + whole[:, 1, 3 + i]).astype(BF16)
    for copy in copies:
        copy.wait()


def local_step(w_query, b_query, w_key, b_key, w_value, b_value, w_out, w_gate, w_up, w_down, gain_attn, gain_mlp,
               hidden, k_cache, v_cache, lengths):
    z = lax.axis_index("tp")
    vectors = jnp.stack([b_query, b_key, b_value, gain_attn, gain_mlp])
    zeros = jnp.zeros_like(vectors)
    small = jnp.concatenate([jnp.where(z == 0, vectors, zeros), jnp.where(z == 0, zeros, vectors)], axis=1)
    small = jnp.pad(small, ((0, 3), (0, 0)))
    inv_freq = 1.0 / (THETA ** (jnp.arange(0, 64, 2, dtype=F32) / 64))
    angles = inv_freq[:, None] * lengths.astype(F32)[None, :]
    cos, sin = jnp.cos(angles), jnp.sin(angles)
    lens = lengths.astype(F32)[None, :]
    k_view = jnp.transpose(k_cache, (1, 2, 3, 0))
    v_view = jnp.transpose(v_cache, (1, 2, 3, 0))

    vmem = pl.BlockSpec(memory_space=pltpu.VMEM)
    hbm = pl.BlockSpec(memory_space=pltpu.HBM)
    anywhere = pl.BlockSpec(memory_space=pl.ANY)
    dma = pltpu.SemaphoreType.DMA
    shapes = [(8, 192, 1024), (8, 352, 1024), (16, 64, 512), (16, 64, 1408), *[(32, 8, 64, 256)] * 4,
              (16, 8, 128), (256, 1024)]
    held = pl.pallas_call(
        layer_kernel,
        out_shape=[pltpu.VMEM(s, BF16) for s in shapes],
        in_specs=[vmem] * 12 + [hbm] * 2,
        out_specs=[vmem] * 10,
        scratch_shapes=[
            pltpu.VMEM((256, 1024), BF16),
            pltpu.VMEM((64, 256), F32),
            pltpu.VMEM((512, 256), BF16),
            pltpu.VMEM((256, 1024), BF16),
            pltpu.VMEM((256, 1024), BF16),
            pltpu.VMEM((256, 1024), BF16),
            pltpu.VMEM((256, 1024), BF16),
            pltpu.VMEM((8, 176, 256), BF16),
            pltpu.VMEM((1024, 256), BF16),
            pltpu.VMEM((1024, 256), BF16),
            pltpu.VMEM((3, 64, 1024), BF16),
            pltpu.VMEM((4, 88, 1024), BF16),
            dma((16,)), dma((16,)), dma((16,)), dma((16,)), dma, dma, dma((8,)), dma((8,)),
            dma((7, 4, 5)), dma((7, 5)), dma((7, 4)), dma((2, 4, 8)), dma((2, 8)), dma((2, 8)),
        ],
        compiler_params=pltpu.CompilerParams(collective_id=0, has_side_effects=True, vmem_limit_bytes=10 * 2**20),
        name="layer",
    )(w_query, w_key, w_value, w_out, w_gate, w_up, w_down, small, hidden, cos, sin, lens, k_view, v_view)

    def shape(*dims):
        return jax.ShapeDtypeStruct(dims, BF16)

    outs = pl.pallas_call(
        store_kernel,
        out_shape=[shape(8, 64, 1024)] * 3 + [shape(16, 64, 512), shape(8, 176, 1024), shape(8, 176, 1024),
                   shape(16, 64, 1408), shape(*k_view.shape), shape(*v_view.shape), shape(256, 1024),
                   shape(4, 128), shape(4, 128), shape(4, 128), shape(8, 128), shape(8, 128)],
        in_specs=[anywhere] * 8 + [vmem, anywhere],
        out_specs=[hbm] * 10 + [vmem] * 5,
        scratch_shapes=[dma((12,))],
        compiler_params=pltpu.CompilerParams(vmem_limit_bytes=2 * 2**20),
        name="store",
    )(*held)
    wq, wk, wv, wo, wg, wu, wd, k_out, v_out, hid, bq, bk, bv, ga, gm = outs
    flat = lambda a, n: a.reshape(-1, n)
    return (flat(wq, 1024), bq.reshape(512), flat(wk, 1024), bk.reshape(512), flat(wv, 1024), bv.reshape(512),
            flat(wo, 512), flat(wg, 1024), flat(wu, 1024), flat(wd, 1408), ga.reshape(1024), gm.reshape(1024),
            hid, jnp.transpose(k_out, (3, 0, 1, 2)), jnp.transpose(v_out, (3, 0, 1, 2)))


def solution(mesh):
    row_spec = P(("dp", "tp"), None)
    flat_spec = P(("dp", "tp"))
    cache_spec = P("dp", None, "tp", None)
    in_specs = (row_spec, flat_spec, row_spec, flat_spec, row_spec, flat_spec, row_spec, row_spec, row_spec, row_spec,
                flat_spec, flat_spec, P("dp", None), cache_spec, cache_spec, P("dp"))
    out_specs = (P("tp", None), P("tp"), P("tp", None), P("tp"), P("tp", None), P("tp"), P(None, "tp"), P("tp", None),
                 P("tp", None), P(None, "tp"), P(None), P(None), P("dp", None), cache_spec, cache_spec)
    return jax.shard_map(local_step, mesh=mesh, in_specs=in_specs, out_specs=out_specs, check_vma=False)
```

```python
import jax
import jax.numpy as jnp
from jax import lax
from jax.experimental import pallas as pl
from jax.experimental.pallas import tpu as pltpu
from jax.sharding import PartitionSpec as P

EPS = 1e-6
THETA = 1000000.0
MESH = pl.DeviceIdType.MESH
F32 = jnp.float32
BF16 = jnp.bfloat16
ROW_BYTES = (((1,), (1,)), ((), ()))
NAT = (((1,), (0,)), ((), ()))
GROUP = 8


def dot(lhs, rhs, dims):
    return lax.dot_general(lhs, rhs, dims, preferred_element_type=F32)


HOME_STEPS = (
    (
        ("s", "q0", 0, "c", 0), ("s", "q1", 0, "c", 0), ("s", "q2", 0, "c", 0), ("s", "g0", 0, "c", 0),
        ("s", "g1", 0, "c", 0), ("s", "u0", 0, "c", 0), ("s", "u1", 0, "c", 0), ("s", "o", 0, "c", 0),
        ("s", "d", 0, "c", 0), ("s", "o", "z", "z", 4), ("s", "d", "z", "z", 4), ("s", "q1", 0, "y", 0),
        ("s", "q1", 0, "x", 1),
    ),
    (
        ("s", "o", 0, "y", 2), ("s", "q2", 0, "y", 0), ("s", "o", 0, "x", 1), ("s", "q2", 0, "x", 1),
    ),
    (
        ("w", "o", 4), ("s", "o", 4, "c", 4), ("w", "q0", "c", 0), ("w", "q1", "c", 0), ("w", "q2", "c", 0),
    ),
    (
        ("w", "q1", "t"), ("w", "q1", 1), ("s", "q1", 1, "c", 1), ("s", "q1", "t", "z", 2), ("s", "o", 4, "y", 6),
        ("s", "o", 4, "x", 5), ("w", "q1", 2), ("s", "q1", 2, "c", 2), ("w", "o", 1), ("s", "o", 1, "c", 1),
        ("s", "q0", 0, "y", 0), ("s", "q0", 0, "x", 1), ("w", "q2", "t"), ("s", "q2", "t", "z", 2), ("w", "q2", 1),
        ("s", "q2", 1, "c", 1), ("w", "q2", 2), ("s", "q2", 2, "c", 2), ("s", "g0", 0, "y", 0), ("s", "q1", 2, "x", 3),
        ("w", "o", 5), ("s", "o", 5, "c", 5), ("w", "q0", "t"), ("s", "q0", "t", "z", 2), ("w", "o", 2),
        ("s", "o", 2, "c", 2), ("w", "q0", 2), ("s", "q0", 2, "c", 2),
    ),
    (
        ("w", "o", 6), ("s", "o", 6, "c", 6), ("w", "q0", 1), ("s", "q0", 1, "c", 1), ("s", "q0", 1, "y", 1),
        ("s", "q2", 2, "x", 3),
    ),
    (
        ("s", "q0", 2, "x", 3), ("w", "q0", "c", 1), ("w", "q1", "c", 1), ("w", "q2", "c", 1),
    ),
    (
        ("w", "g0", 2), ("s", "g0", 2, "c", 2), ("w", "q1", 3), ("s", "q1", 3, "c", 3), ("w", "g0", "t"),
        ("s", "g0", "t", "z", 2), ("s", "q1", 3, "y", 3), ("w", "q0", "c", 2), ("w", "q1", "c", 2), ("w", "q2", "c", 2),
    ),
    (
        ("w", "q2", 3), ("s", "q2", 3, "c", 3), ("s", "o", 1, "y", 3), ("s", "g0", 0, "x", 1), ("w", "d", 4),
        ("s", "d", 4, "c", 4), ("s", "o", 5, "y", 7), ("w", "u0", "t"), ("s", "u0", "t", "z", 2),
        ("s", "u0", 0, "y", 0), ("s", "o", 6, "x", 7), ("w", "q0", 3), ("s", "q0", 3, "c", 3),
    ),
    (
        ("w", "u0", 2), ("s", "u0", 2, "c", 2), ("s", "u0", 0, "x", 1), ("w", "q0", "c", 3), ("w", "q1", "c", 3),
        ("w", "q2", "c", 3),
    ),
    (
        ("w", "u1", "t"), ("s", "u1", "t", "z", 2), ("s", "u1", 0, "y", 0), ("w", "g0", 1), ("s", "g0", 1, "c", 1),
        ("s", "u1", 0, "x", 1), ("w", "o", 7), ("s", "o", 7, "c", 7), ("w", "u1", 2), ("s", "u1", 2, "c", 2),
        ("w", "g1", "t"), ("s", "g1", "t", "z", 2), ("s", "g1", 0, "y", 0), ("w", "o", 3), ("s", "o", 3, "c", 3),
        ("s", "g1", 0, "x", 1), ("w", "u0", 1), ("s", "u0", 1, "c", 1), ("w", "g1", 2), ("s", "g1", 2, "c", 2),
        ("w", "o", "c", 0), ("w", "o", "c", 1), ("w", "o", "c", 2), ("w", "o", "c", 3), ("w", "o", "c", 4),
        ("w", "o", "c", 5), ("w", "o", "c", 6), ("w", "o", "c", 7),
    ),
    (
        ("s", "d", 0, "y", 2), ("w", "d", 2), ("s", "d", 2, "c", 2), ("s", "d", 0, "x", 1), ("w", "u1", 1),
        ("s", "u1", 1, "c", 1), ("s", "d", 4, "y", 6), ("w", "d", 6), ("s", "d", 6, "c", 6), ("s", "d", 4, "x", 5),
        ("w", "g1", 1), ("s", "g1", 1, "c", 1), ("s", "u0", 1, "y", 1), ("w", "g0", 3), ("s", "g0", 3, "c", 3),
        ("s", "g1", 2, "x", 3), ("w", "d", 1), ("s", "d", 1, "c", 1),
    ),
    (
        ("s", "d", 1, "y", 3),
    ),
    (
        ("w", "u0", 3), ("s", "u0", 3, "c", 3), ("w", "g0", "c", 0), ("w", "g1", "c", 0), ("w", "u0", "c", 0),
        ("w", "u1", "c", 0),
    ),
    (
        ("w", "d", 5), ("s", "d", 5, "c", 5), ("s", "d", 6, "x", 7),
    ),
    (
        ("w", "g0", "c", 1), ("w", "g1", "c", 1), ("w", "u0", "c", 1), ("w", "u1", "c", 1),
    ),
    (),
    (
        ("w", "g0", "c", 2), ("w", "g1", "c", 2), ("w", "u0", "c", 2), ("w", "u1", "c", 2),
    ),
    (
        ("w", "u1", 3), ("s", "u1", 3, "c", 3), ("w", "g1", 3), ("s", "g1", 3, "c", 3),
    ),
    (
        ("w", "g0", "c", 3), ("w", "g1", "c", 3), ("w", "u0", "c", 3), ("w", "u1", "c", 3),
    ),
    (),
    (
        ("w", "d", "c", 0), ("w", "d", "c", 4),
    ),
    (
        ("w", "d", 3), ("s", "d", 3, "c", 3),
    ),
    (
        ("w", "d", 7), ("s", "d", 7, "c", 7), ("w", "d", "c", 1), ("w", "d", "c", 5),
    ),
    (),
    (
        ("w", "d", "c", 2), ("w", "d", "c", 6),
    ),
    (),
    (
        ("w", "d", "c", 3), ("w", "d", "c", 7),
    ),
    (),
)
HOME_BLOCKS = {
    "attend": ((0, 0), (0, 1), (2, 0), (1, 0), (1, 1), (2, 1), (3, 0), (3, 1)),
    "gated": ((0, 0), (0, 1), (1, 0), (1, 1), (2, 0), (2, 1), (3, 0), (3, 1)),
    "down": ((0, 0), (0, 1), (1, 0), (1, 1), (2, 0), (2, 1), (3, 0), (3, 1)),
}
AWAY_STEPS = (
    (
        ("s", "o", 0, "c", 0), ("s", "d", 0, "c", 0), ("s", "o", "z", "z", 4), ("s", "q1", "own", "z", 2),
        ("s", "q1", "own", "y", "t"), ("s", "o", 0, "x", 1), ("s", "d", 0, "x", 1),
    ),
    (
        ("s", "q2", "own", "z", 2), ("s", "q2", "own", "y", "t"), ("w", "o", 1), ("s", "o", 1, "c", 1), ("w", "o", 4),
        ("s", "o", 4, "c", 4), ("s", "o", 4, "x", 5), ("s", "q0", "own", "y", "t"), ("w", "q1", 0),
        ("s", "q1", 0, "c", 0), ("s", "q1", 0, "x", 1), ("s", "q0", "own", "z", 2), ("w", "o", 2),
        ("s", "o", 2, "c", 2), ("s", "o", 0, "y", 2), ("w", "d", 1), ("s", "d", 1, "c", 1), ("w", "d", 4),
        ("s", "d", 4, "c", 4), ("s", "d", 4, "x", 5), ("s", "g0", "own", "z", 2), ("s", "o", 4, "y", 6), ("w", "o", 5),
        ("s", "o", 5, "c", 5), ("w", "q2", 0), ("s", "q2", 0, "c", 0), ("s", "g0", "own", "y", "t"), ("w", "o", 6),
        ("s", "o", 6, "c", 6), ("w", "q1", 2), ("s", "q1", 2, "c", 2), ("s", "q2", 0, "x", 1), ("w", "q1", 1),
        ("s", "q1", 1, "c", 1), ("s", "d", "z", "z", 4), ("s", "u0", "own", "y", "t"), ("w", "q0", 0),
        ("s", "q0", 0, "c", 0),
    ),
    (
        ("w", "q2", 2), ("s", "q2", 2, "c", 2), ("s", "q2", 2, "x", 3), ("w", "q0", "c", 0), ("w", "q1", "c", 0),
        ("w", "q2", "c", 0),
    ),
    (
        ("w", "d", 5), ("s", "d", 5, "c", 5), ("w", "q0", 2), ("s", "q0", 2, "c", 2), ("s", "u0", "own", "z", 2),
        ("s", "u1", "own", "y", "t"), ("s", "q0", 2, "x", 3),
    ),
    (
        ("w", "g0", 0), ("s", "g0", 0, "c", 0), ("w", "q2", 1), ("s", "q2", 1, "c", 1), ("w", "q0", "c", 2),
        ("w", "q1", "c", 2), ("w", "q2", "c", 2),
    ),
    (
        ("w", "q0", 1), ("s", "q0", 1, "c", 1), ("s", "u1", "own", "z", 2), ("s", "g1", "own", "y", "t"),
        ("s", "g0", 0, "x", 1),
    ),
    (
        ("w", "q2", 3), ("s", "q2", 3, "c", 3), ("w", "q1", 3), ("s", "q1", 3, "c", 3), ("w", "q0", "c", 1),
        ("w", "q1", "c", 1), ("w", "q2", "c", 1),
    ),
    (
        ("w", "g0", 2), ("s", "g0", 2, "c", 2), ("w", "q0", 3), ("s", "q0", 3, "c", 3), ("w", "o", 3),
        ("s", "o", 3, "c", 3), ("s", "g1", "own", "z", 2), ("s", "o", 1, "y", 3), ("s", "g0", 2, "x", 3),
    ),
    (
        ("w", "o", 7), ("s", "o", 7, "c", 7), ("s", "d", 0, "y", 2), ("w", "q0", "c", 3), ("w", "q1", "c", 3),
        ("w", "q2", "c", 3),
    ),
    (
        ("w", "u0", 2), ("s", "u0", 2, "c", 2), ("w", "g0", 1), ("s", "g0", 1, "c", 1), ("s", "u0", 2, "x", 3),
        ("w", "o", "c", 0), ("w", "o", "c", 1), ("w", "o", "c", 2), ("w", "o", "c", 3), ("w", "o", "c", 4),
        ("w", "o", "c", 5), ("w", "o", "c", 6), ("w", "o", "c", 7),
    ),
    (
        ("w", "u0", 0), ("s", "u0", 0, "c", 0), ("s", "d", 4, "y", 6), ("w", "u1", 2), ("s", "u1", 2, "c", 2),
        ("s", "u1", 2, "x", 3), ("w", "g0", 3), ("s", "g0", 3, "c", 3), ("w", "u1", 0), ("s", "u1", 0, "c", 0),
        ("s", "g0", 3, "y", 3), ("s", "u1", 0, "x", 1), ("w", "g1", 2), ("s", "g1", 2, "c", 2), ("w", "u0", 3),
        ("s", "u0", 3, "c", 3), ("w", "g1", 0), ("s", "g1", 0, "c", 0), ("s", "u0", 3, "y", 3), ("s", "g1", 0, "x", 1),
        ("w", "u1", 3), ("s", "u1", 3, "c", 3), ("w", "d", 2), ("s", "d", 2, "c", 2), ("s", "u1", 3, "y", 3),
        ("s", "g1", 2, "x", 3), ("w", "u1", 1), ("s", "u1", 1, "c", 1), ("w", "d", 6), ("s", "d", 6, "c", 6),
        ("s", "d", 1, "y", 3),
    ),
    (
        ("w", "g1", 1), ("s", "g1", 1, "c", 1), ("s", "d", 6, "x", 7),
    ),
    (
        ("w", "u0", 1), ("s", "u0", 1, "c", 1), ("w", "g0", "c", 0), ("w", "g1", "c", 0), ("w", "u0", "c", 0),
        ("w", "u1", "c", 0),
    ),
    (),
    (),
    (
        ("w", "g1", 3), ("s", "g1", 3, "c", 3), ("w", "g0", "c", 1), ("w", "g1", "c", 1), ("w", "u0", "c", 1),
        ("w", "u1", "c", 1),
    ),
    (
        ("w", "g0", "c", 2), ("w", "g1", "c", 2), ("w", "u0", "c", 2), ("w", "u1", "c", 2),
    ),
    (),
    (
        ("w", "d", 3), ("s", "d", 3, "c", 3), ("w", "g0", "c", 3), ("w", "g1", "c", 3), ("w", "u0", "c", 3),
        ("w", "u1", "c", 3),
    ),
    (),
    (
        ("w", "d", "c", 0), ("w", "d", "c", 4),
    ),
    (
        ("w", "d", 7), ("s", "d", 7, "c", 7),
    ),
    (
        ("w", "d", "c", 1), ("w", "d", "c", 5),
    ),
    (),
    (
        ("w", "d", "c", 2), ("w", "d", "c", 6),
    ),
    (),
    (
        ("w", "d", "c", 3), ("w", "d", "c", 7),
    ),
    (),
)
AWAY_BLOCKS = {
    "attend": ((0, 0), (0, 1), (2, 0), (2, 1), (1, 0), (1, 1), (3, 0), (3, 1)),
    "gated": ((0, 0), (0, 1), (1, 0), (2, 0), (1, 1), (2, 1), (3, 0), (3, 1)),
    "down": ((0, 0), (0, 1), (1, 0), (1, 1), (2, 0), (2, 1), (3, 0), (3, 1)),
}


class Place:
    def __init__(self):
        tp = lax.axis_index("tp")
        dp = lax.axis_index("dp")
        self.z = tp
        self.dp = dp
        self.y = dp // 4
        self.x = (dp // 2) % 2
        self.c = dp % 2
        self.far = lax.rem(self.y + self.z, 2)
        self.device = {
            "x": (tp, dp + 2 - 4 * self.x),
            "y": (tp, dp + 4 - 8 * self.y),
            "c": (tp, dp + 1 - 2 * self.c),
            "z": (1 - tp, dp),
        }

    def at(self, axis, flip):
        here = getattr(self, axis)
        return 1 - here if flip else here

    def row_block(self, k, core=0):
        return (self.at("x", k & 1) * 2 + self.at("c", core)) * 2 + self.at("z", k & 2)

    def col_block(self, k, core=0):
        return (self.at("y", k & 2) * 4 + self.at("x", k & 1) * 2 + self.at("c", core)) * 2 + self.at("z", k & 4)


def remote(src, dst, send, recv, device):
    return pltpu.make_async_remote_copy(
        src_ref=src, dst_ref=dst, send_sem=send, recv_sem=recv, device_id=device, device_id_type=MESH)


class Rows:
    def __init__(self, place, buf, start, own, through, index, sems):
        self.p, self.buf, self.start, self.own, self.through = place, buf, start, own, through
        self.i, (self.send, self.r, self.rc) = index, sems
        self.n = own.shape[0]

    def block(self, k, core=0):
        return self.buf.at[self.p.row_block(k, core), pl.ds(self.start, self.n)]

    def copy(self, k, link, home):
        p = self.p
        slot = {"own": 0, "t": 4}.get(k, k)
        send = self.send.at[self.i, "xyzc".index(link), slot]
        if k == "own" or (home and k == 0):
            src = self.own
        elif k == "t":
            src = self.through
        else:
            src = self.block(k)
        if k == "own" and link == "y":
            dst, recv = self.through, self.r.at[self.i, 4]
        else:
            dst = self.block(0 if k in ("own", "t") else k)
            got = 2 if link == "z" else k ^ 1 if link == "x" else k
            recv = self.rc.at[self.i, k] if link == "c" else self.r.at[self.i, got]
        return remote(src, dst, send, recv, p.device[link])

    def wait(self, k, core):
        if k == "t":
            ref, recv = self.through, self.r.at[self.i, 4]
        else:
            ref, recv = self.block(k, core), (self.rc if core else self.r).at[self.i, k]
        remote(ref, ref, self.send.at[self.i, 0, 0], recv, self.p.device["x"]).wait_recv()

    def local(self):
        @pl.when(self.p.far == 0)
        def _():
            self.buf[self.p.row_block(0), pl.ds(self.start, self.n)] = self.own[...]


class Cols:
    def __init__(self, place, buf, own, index, sems):
        self.p, self.buf, self.own = place, buf, own
        self.n = buf.shape[-1]
        self.i, (self.send, self.r, self.rc) = index, sems

    def block(self, k, core=0):
        return self.buf.at[self.p.col_block(k, core)]

    def half(self, z):
        return self.own.at[:, pl.ds(pl.multiple_of(z * self.n, 128), self.n)]

    def copy(self, k, link, home):
        p = self.p
        if link == "z":
            return remote(self.half(1 - p.z), self.block(0), self.send.at[self.i, 2, 0], self.r.at[self.i, 4], p.device["z"])
        src = self.half(p.z) if k == 0 else self.block(k)
        got = k ^ 1 if link == "x" else k ^ 2
        recv = self.rc.at[self.i, k] if link == "c" else self.r.at[self.i, got]
        return remote(src, self.block(k), self.send.at[self.i, "xyzc".index(link), k], recv, p.device[link])

    def wait(self, k, core):
        ref, recv = self.block(k, core), (self.rc if core else self.r).at[self.i, k]
        remote(ref, ref, self.send.at[self.i, 0, 0], recv, self.p.device["x"]).wait_recv()

    def local(self):
        self.buf[self.p.col_block(0)] = self.own[:, pl.ds(pl.multiple_of(self.p.z * self.n, 128), self.n)]


def layer_kernel(wq, wk, wv, wo, wg, wu, wd, small, x_ref, cos_ref, sin_ref, len_ref, k_hbm, v_hbm,
                 wqkv, wgu, wout, wdn, k_lo, k_hi, v_lo, v_hi, smalls, x1_ref, down,
                 h_ref, sc_ref, o_ref, a_ref, t_q, t_gu,
                 k_sem, v_sem, s_send, s_recv, p_send, p_recv, row_s, row_r, row_c, col_s, col_r, col_c):
    place = Place()
    me = place.dp * 2 + place.z
    row_sem, col_sem = (row_s, row_r, row_c), (col_s, col_r, col_c)
    half = pl.ds(0, 88), pl.ds(88, 88)
    chunks = {}
    for i, ref in enumerate((wq, wk, wv)):
        chunks[f"q{i}"] = Rows(place, wqkv, 64 * i, ref, t_q.at[i], i, row_sem)
    for i in range(4):
        ref = (wg, wu)[i // 2].at[half[i % 2]]
        chunks["gu"[i // 2] + str(i % 2)] = Rows(place, wgu, 88 * i, ref, t_gu.at[i], 3 + i, row_sem)
    chunks["o"] = Cols(place, wout, wo, 0, col_sem)
    chunks["d"] = Cols(place, wdn, wd, 1, col_sem)
    roles = ((0, HOME_STEPS, HOME_BLOCKS), (1, AWAY_STEPS, AWAY_BLOCKS))
    step = iter(range(len(HOME_STEPS)))

    def go():
        now = next(step)
        for far, steps, _ in roles:
            if steps[now]:
                @pl.when(place.far == far)
                def _(far=far, steps=steps):
                    for action in steps[now]:
                        chunk = chunks[action[1]]
                        if action[0] == "s":
                            chunk.copy(action[2], action[3], far == 0).start()
                        elif action[2] == "c":
                            chunk.wait(action[3], 1)
                        else:
                            chunk.wait(action[2], 0)

    def by_role(kind, i, place_of, swap=False):
        home, away = (place_of(*blocks[kind][i]) for _, _, blocks in roles)
        if swap:
            home, away = away, home
        return home + place.far * (away - home)

    def cache_copy(i):
        head = by_role("attend", i, place.row_block)
        copies = []
        for hbm, lo, hi, sem in ((k_hbm, k_lo, k_hi, k_sem), (v_hbm, v_lo, v_hi, v_sem)):
            copies.append(pltpu.make_async_copy(hbm.at[pl.ds(0, 32), head], lo.at[:, head], sem.at[2 * i]))
            copies.append(pltpu.make_async_copy(hbm.at[pl.ds(32, 32), head], hi.at[:, head], sem.at[2 * i + 1]))
        return copies

    barrier = pltpu.get_barrier_semaphore()
    for i in range(1, 16):
        other = lax.rem(me + i, 16)
        pl.semaphore_signal(barrier, inc=1, device_id=(other % 2, other // 2), device_id_type=MESH)
    for i in range(8):
        for copy in cache_copy(i):
            copy.start()
    pl.semaphore_wait(barrier, 15)

    def small_copy(i):
        other = lax.rem(me + i, 16)
        return remote(small, smalls.at[me], s_send.at[i], s_recv.at[i], (other % 2, other // 2))

    for i in range(1, 16):
        small_copy(i).start()
    go()

    for chunk in chunks.values():
        chunk.local()
    smalls[me] = small[...]
    for i in range(1, 16):
        small_copy(i).wait_recv()

    def gain_row(i):
        pair = smalls[...].astype(F32).reshape(8, 2, 8, 128)
        rows = pair[:, 0, i] + pair[:, 1, i]
        return jnp.concatenate([rows[d:d + 1] for d in range(8)], axis=1)

    def normed(rows, i):
        inv = lax.rsqrt(jnp.mean(rows * rows, axis=-1, keepdims=True) + EPS)
        return (rows * inv * gain_row(i)).astype(BF16)

    h_ref[...] = normed(x_ref[...].astype(F32), 3)

    eye = lax.broadcasted_iota(jnp.int32, (64, 128), 1) % 64 == lax.broadcasted_iota(jnp.int32, (64, 128), 0)

    def bias_column(head, i):
        row = smalls[place.z * 8 + head].astype(F32)[i:i + 1]
        return jnp.sum(jnp.where(eye, row, 0.0), axis=1, keepdims=True)

    def attend(i):
        head = by_role("attend", i, place.row_block)
        res = dot(wqkv[head], h_ref[...], ROW_BYTES)
        cos, sin = cos_ref[...], sin_ref[...]

        def rotated(start, b):
            v = (res[start:start + 64] + bias_column(head, b)).astype(BF16).astype(F32)
            lo, hi = v[:32], v[32:]
            return jnp.concatenate([lo * cos - hi * sin, hi * cos + lo * sin], axis=0).astype(BF16)

        q = rotated(0, 0).astype(F32)
        k_new = rotated(64, 1)
        v_new = (res[128:192] + bias_column(head, 2)).astype(BF16)
        lens = len_ref[...]
        for copy in cache_copy(i):
            copy.wait()

        for base, buf in ((0, k_lo), (32, k_hi)):
            def score_group(g, carry, base=base, buf=buf):
                rows = []
                for j in range(GROUP):
                    s = g * GROUP + j
                    kv = jnp.where(lens == (base + s).astype(F32), k_new.astype(F32), buf[s, head].astype(F32))
                    buf[s, head] = kv.astype(BF16)
                    rows.append(jnp.sum(q * kv, axis=0, keepdims=True))
                sc_ref[pl.ds(pl.multiple_of(base + g * GROUP, GROUP), GROUP)] = jnp.concatenate(rows, axis=0)
                return carry

            lax.fori_loop(0, 32 // GROUP, score_group, 0)
        slot = lax.broadcasted_iota(jnp.int32, (64, 256), 0).astype(F32)
        scores = jnp.where(slot <= lens, sc_ref[...] * 0.125, -1e30)
        e = jnp.exp(scores - jnp.max(scores, axis=0, keepdims=True))
        sc_ref[...] = (e / jnp.sum(e, axis=0, keepdims=True)).astype(BF16).astype(F32)

        acc = jnp.zeros((64, 256), F32)
        for base, buf in ((0, v_lo), (32, v_hi)):
            def value_group(g, acc, base=base, buf=buf):
                probs = sc_ref[pl.ds(pl.multiple_of(base + g * GROUP, GROUP), GROUP)]
                for j in range(GROUP):
                    s = g * GROUP + j
                    vv = jnp.where(lens == (base + s).astype(F32), v_new.astype(F32), buf[s, head].astype(F32))
                    buf[s, head] = vv.astype(BF16)
                    acc = acc + probs[j:j + 1] * vv
                return acc

            acc = lax.fori_loop(0, 32 // GROUP, value_group, acc)
        o_ref[pl.ds(pl.multiple_of(head * 64, 64), 64)] = acc.astype(BF16)

    go()
    for i in range(8):
        attend(i)
        go()

    o = o_ref[...].T
    part, part_in, h2_ref = down, x1_ref, h_ref
    part[...] = dot(o, wout[...].reshape(1024, 512), ROW_BYTES).astype(BF16)
    swap = remote(part, part_in, p_send, p_recv, place.device["z"])
    swap.start()
    go()
    swap.wait_recv()
    swap.wait_send()
    total = (part[...].astype(F32) + part_in[...].astype(F32)).astype(BF16)
    x1 = (x_ref[...].astype(F32) + total.astype(F32)).astype(BF16)
    x1_ref[...] = x1
    h2_ref[...] = normed(x1.astype(F32), 4)
    go()

    for i in range(8):
        block = by_role("gated", i, place.row_block)
        res = dot(wgu[block], h2_ref[...], ROW_BYTES).astype(BF16).astype(F32)
        g, u = res[:176], res[176:]
        a_ref[block] = (g / (1.0 + jnp.exp(-g)) * u).astype(BF16)
        go()

    for i in range(8):
        pair = by_role("down", i, lambda k, core: place.col_block(k, core) // 2)
        w = wdn[pl.ds(pair * 2, 2)].reshape(128, 1408)
        cols = pl.ds(pl.multiple_of(pair * 128, 128), 128)
        down[:, cols] = dot(w, a_ref[...].reshape(1408, 256), NAT).T.astype(BF16)
        go()

    for far, steps, _ in roles:
        @pl.when(place.far == far)
        def _(far=far, steps=steps):
            for action in sum(steps, ()):
                if action[0] == "s":
                    chunks[action[1]].copy(action[2], action[3], far == 0).wait_send()

    for i in range(1, 16):
        small_copy(i).wait_send()


def store_kernel(wqkv, wgu, wout, wdn, k_lo, k_hi, v_lo, v_hi, smalls,
                 wq, wk, wv, wo, wg, wu, wd, k_out, v_out, bq, bk, bv, ga, gm, sem):
    lo, hi = pl.ds(0, 32), pl.ds(32, 32)
    pairs = [(k_lo, k_out.at[lo]), (k_hi, k_out.at[hi]), (v_lo, v_out.at[lo]), (v_hi, v_out.at[hi]),
             (wdn, wd), (wgu.at[:, pl.ds(0, 176)], wg), (wgu.at[:, pl.ds(176, 176)], wu),
             (wqkv.at[:, pl.ds(0, 64)], wq), (wqkv.at[:, pl.ds(64, 64)], wk), (wqkv.at[:, pl.ds(128, 64)], wv),
             (wout, wo)]
    copies = [pltpu.make_async_copy(src, dst, sem.at[i]) for i, (src, dst) in enumerate(pairs)]
    for copy in copies:
        copy.start()
    z = lax.axis_index("tp")
    plane = smalls[pl.ds(z * 8, 8)].astype(F32).reshape(4, 2, 8, 128)
    whole = smalls[...].astype(F32).reshape(8, 2, 8, 128)
    for i, ref in enumerate((bq, bk, bv)):
        ref[...] = (plane[:, 0, i] + plane[:, 1, i]).astype(BF16)
    for i, ref in enumerate((ga, gm)):
        ref[...] = (whole[:, 0, 3 + i] + whole[:, 1, 3 + i]).astype(BF16)
    for copy in copies:
        copy.wait()


def finish_kernel(x1, mine, peer, hid):
    total = (mine[...].astype(F32) + peer[...].astype(F32)).astype(BF16)
    hid[...] = (x1[...].astype(F32) + total.astype(F32)).astype(BF16)


def local_step(w_query, b_query, w_key, b_key, w_value, b_value, w_out, w_gate, w_up, w_down, gain_attn, gain_mlp,
               hidden, k_cache, v_cache, lengths):
    z = lax.axis_index("tp")
    vectors = jnp.stack([b_query, b_key, b_value, gain_attn, gain_mlp])
    zeros = jnp.zeros_like(vectors)
    small = jnp.concatenate([jnp.where(z == 0, vectors, zeros), jnp.where(z == 0, zeros, vectors)], axis=1)
    small = jnp.pad(small, ((0, 3), (0, 0)))
    inv_freq = 1.0 / (THETA ** (jnp.arange(0, 64, 2, dtype=F32) / 64))
    angles = inv_freq[:, None] * lengths.astype(F32)[None, :]
    cos, sin = jnp.cos(angles), jnp.sin(angles)
    lens = lengths.astype(F32)[None, :]
    k_view = jnp.transpose(k_cache, (1, 2, 3, 0))
    v_view = jnp.transpose(v_cache, (1, 2, 3, 0))

    vmem = pl.BlockSpec(memory_space=pltpu.VMEM)
    hbm = pl.BlockSpec(memory_space=pltpu.HBM)
    anywhere = pl.BlockSpec(memory_space=pl.ANY)
    dma = pltpu.SemaphoreType.DMA
    shapes = [(8, 192, 1024), (8, 352, 1024), (16, 64, 512), (16, 64, 1408), *[(32, 8, 64, 256)] * 4,
              (16, 8, 128), (256, 1024), (256, 1024)]
    held = pl.pallas_call(
        layer_kernel,
        out_shape=[pltpu.VMEM(s, BF16) for s in shapes],
        in_specs=[vmem] * 12 + [hbm] * 2,
        out_specs=[vmem] * 11,
        scratch_shapes=[
            pltpu.VMEM((256, 1024), BF16),
            pltpu.VMEM((64, 256), F32),
            pltpu.VMEM((512, 256), BF16),
            pltpu.VMEM((8, 176, 256), BF16),
            pltpu.VMEM((3, 64, 1024), BF16),
            pltpu.VMEM((4, 88, 1024), BF16),
            dma((16,)), dma((16,)), dma((16,)), dma((16,)), dma, dma,
            dma((7, 4, 5)), dma((7, 5)), dma((7, 4)), dma((2, 4, 8)), dma((2, 8)), dma((2, 8)),
        ],
        compiler_params=pltpu.CompilerParams(collective_id=0, has_side_effects=True, vmem_limit_bytes=5 * 2**20),
        name="layer",
    )(w_query, w_key, w_value, w_out, w_gate, w_up, w_down, small, hidden, cos, sin, lens, k_view, v_view)

    def shape(*dims):
        return jax.ShapeDtypeStruct(dims, BF16)

    peer = lax.ppermute(held[10], "tp", [(0, 1), (1, 0)])
    outs = pl.pallas_call(
        store_kernel,
        out_shape=[shape(8, 64, 1024)] * 3 + [shape(16, 64, 512), shape(8, 176, 1024), shape(8, 176, 1024),
                   shape(16, 64, 1408), shape(*k_view.shape), shape(*v_view.shape),
                   shape(4, 128), shape(4, 128), shape(4, 128), shape(8, 128), shape(8, 128)],
        in_specs=[anywhere] * 8 + [vmem],
        out_specs=[hbm] * 9 + [vmem] * 5,
        scratch_shapes=[dma((11,))],
        compiler_params=pltpu.CompilerParams(vmem_limit_bytes=2**20),
        cost_estimate=pl.CostEstimate(flops=2 * 10**10, bytes_accessed=5 * 10**7, transcendentals=0),
        name="store",
    )(*held[:9])
    hid = pl.pallas_call(
        finish_kernel,
        out_shape=shape(256, 1024),
        in_specs=[vmem] * 3,
        out_specs=vmem,
        compiler_params=pltpu.CompilerParams(vmem_limit_bytes=4 * 2**20),
        name="finish",
    )(held[9], held[10], peer)
    wq, wk, wv, wo, wg, wu, wd, k_out, v_out, bq, bk, bv, ga, gm = outs
    flat = lambda a, n: a.reshape(-1, n)
    return (flat(wq, 1024), bq.reshape(512), flat(wk, 1024), bk.reshape(512), flat(wv, 1024), bv.reshape(512),
            flat(wo, 512), flat(wg, 1024), flat(wu, 1024), flat(wd, 1408), ga.reshape(1024), gm.reshape(1024),
            hid, jnp.transpose(k_out, (3, 0, 1, 2)), jnp.transpose(v_out, (3, 0, 1, 2)))


def solution(mesh):
    row_spec = P(("dp", "tp"), None)
    flat_spec = P(("dp", "tp"))
    cache_spec = P("dp", None, "tp", None)
    in_specs = (row_spec, flat_spec, row_spec, flat_spec, row_spec, flat_spec, row_spec, row_spec, row_spec, row_spec,
                flat_spec, flat_spec, P("dp", None), cache_spec, cache_spec, P("dp"))
    out_specs = (P("tp", None), P("tp"), P("tp", None), P("tp"), P("tp", None), P("tp"), P(None, "tp"), P("tp", None),
                 P("tp", None), P(None, "tp"), P(None), P(None), P("dp", None), cache_spec, cache_spec)
    return jax.shard_map(local_step, mesh=mesh, in_specs=in_specs, out_specs=out_specs, check_vma=False)
```

```python
import jax
import jax.numpy as jnp
from jax import lax
from jax.experimental import pallas as pl
from jax.experimental.pallas import tpu as pltpu
from jax.sharding import PartitionSpec as P

EPS = 1e-6
THETA = 1000000.0
MESH = pl.DeviceIdType.MESH
F32 = jnp.float32
BF16 = jnp.bfloat16
ROW_BYTES = (((1,), (1,)), ((), ()))
NAT = (((1,), (0,)), ((), ()))
GROUP = 8


def dot(lhs, rhs, dims):
    return lax.dot_general(lhs, rhs, dims, preferred_element_type=F32)


HOME_STEPS = (
    (
        ("s", "q0", 0, "c", 0), ("s", "q1", 0, "c", 0), ("s", "q2", 0, "c", 0), ("s", "g0", 0, "c", 0),
        ("s", "g1", 0, "c", 0), ("s", "u0", 0, "c", 0), ("s", "u1", 0, "c", 0), ("s", "o", 0, "c", 0),
        ("s", "d", 0, "c", 0), ("s", "o", "z", "z", 4), ("s", "d", "z", "z", 4), ("s", "q1", 0, "y", 0),
        ("s", "q1", 0, "x", 1),
    ),
    (
        ("s", "o", 0, "y", 2), ("s", "q2", 0, "y", 0), ("s", "o", 0, "x", 1), ("s", "q2", 0, "x", 1),
    ),
    (
        ("w", "o", 4), ("s", "o", 4, "c", 4), ("w", "q0", "c", 0), ("w", "q1", "c", 0), ("w", "q2", "c", 0),
    ),
    (
        ("w", "q1", "t"), ("w", "q1", 1), ("s", "q1", 1, "c", 1), ("s", "q1", "t", "z", 2), ("s", "o", 4, "y", 6),
        ("s", "o", 4, "x", 5), ("w", "q1", 2), ("s", "q1", 2, "c", 2), ("w", "o", 1), ("s", "o", 1, "c", 1),
        ("s", "q0", 0, "y", 0), ("s", "q0", 0, "x", 1), ("w", "q2", "t"), ("s", "q2", "t", "z", 2), ("w", "q2", 1),
        ("s", "q2", 1, "c", 1), ("w", "q2", 2), ("s", "q2", 2, "c", 2), ("s", "g0", 0, "y", 0), ("s", "q1", 2, "x", 3),
        ("w", "o", 5), ("s", "o", 5, "c", 5), ("w", "q0", "t"), ("s", "q0", "t", "z", 2), ("w", "o", 2),
        ("s", "o", 2, "c", 2), ("w", "q0", 2), ("s", "q0", 2, "c", 2),
    ),
    (
        ("w", "o", 6), ("s", "o", 6, "c", 6), ("w", "q0", 1), ("s", "q0", 1, "c", 1), ("s", "q0", 1, "y", 1),
        ("s", "q2", 2, "x", 3),
    ),
    (
        ("s", "q0", 2, "x", 3), ("w", "q0", "c", 1), ("w", "q1", "c", 1), ("w", "q2", "c", 1),
    ),
    (
        ("w", "g0", 2), ("s", "g0", 2, "c", 2), ("w", "q1", 3), ("s", "q1", 3, "c", 3), ("w", "g0", "t"),
        ("s", "g0", "t", "z", 2), ("s", "q1", 3, "y", 3), ("w", "q0", "c", 2), ("w", "q1", "c", 2), ("w", "q2", "c", 2),
    ),
    (
        ("w", "q2", 3), ("s", "q2", 3, "c", 3), ("s", "o", 1, "y", 3), ("s", "g0", 0, "x", 1), ("w", "d", 4),
        ("s", "d", 4, "c", 4), ("s", "o", 5, "y", 7), ("w", "u0", "t"), ("s", "u0", "t", "z", 2),
        ("s", "u0", 0, "y", 0), ("s", "o", 6, "x", 7), ("w", "q0", 3), ("s", "q0", 3, "c", 3),
    ),
    (
        ("w", "u0", 2), ("s", "u0", 2, "c", 2), ("s", "u0", 0, "x", 1), ("w", "q0", "c", 3), ("w", "q1", "c", 3),
        ("w", "q2", "c", 3),
    ),
    (
        ("w", "u1", "t"), ("s", "u1", "t", "z", 2), ("s", "u1", 0, "y", 0), ("w", "g0", 1), ("s", "g0", 1, "c", 1),
        ("s", "u1", 0, "x", 1), ("w", "o", 7), ("s", "o", 7, "c", 7), ("w", "u1", 2), ("s", "u1", 2, "c", 2),
        ("w", "g1", "t"), ("s", "g1", "t", "z", 2), ("s", "g1", 0, "y", 0), ("w", "o", 3), ("s", "o", 3, "c", 3),
        ("s", "g1", 0, "x", 1), ("w", "u0", 1), ("s", "u0", 1, "c", 1), ("w", "g1", 2), ("s", "g1", 2, "c", 2),
        ("w", "o", "c", 0), ("w", "o", "c", 1), ("w", "o", "c", 2), ("w", "o", "c", 3), ("w", "o", "c", 4),
        ("w", "o", "c", 5), ("w", "o", "c", 6), ("w", "o", "c", 7),
    ),
    (
        ("s", "d", 0, "y", 2), ("w", "d", 2), ("s", "d", 2, "c", 2), ("s", "d", 0, "x", 1), ("w", "u1", 1),
        ("s", "u1", 1, "c", 1), ("s", "d", 4, "y", 6), ("w", "d", 6), ("s", "d", 6, "c", 6), ("s", "d", 4, "x", 5),
        ("w", "g1", 1), ("s", "g1", 1, "c", 1), ("s", "u0", 1, "y", 1), ("w", "g0", 3), ("s", "g0", 3, "c", 3),
        ("s", "g1", 2, "x", 3), ("w", "d", 1), ("s", "d", 1, "c", 1),
    ),
    (
        ("s", "d", 1, "y", 3),
    ),
    (
        ("w", "u0", 3), ("s", "u0", 3, "c", 3), ("w", "g0", "c", 0), ("w", "g1", "c", 0), ("w", "u0", "c", 0),
        ("w", "u1", "c", 0),
    ),
    (
        ("w", "d", 5), ("s", "d", 5, "c", 5), ("s", "d", 6, "x", 7),
    ),
    (
        ("w", "g0", "c", 1), ("w", "g1", "c", 1), ("w", "u0", "c", 1), ("w", "u1", "c", 1),
    ),
    (),
    (
        ("w", "g0", "c", 2), ("w", "g1", "c", 2), ("w", "u0", "c", 2), ("w", "u1", "c", 2),
    ),
    (
        ("w", "u1", 3), ("s", "u1", 3, "c", 3), ("w", "g1", 3), ("s", "g1", 3, "c", 3),
    ),
    (
        ("w", "g0", "c", 3), ("w", "g1", "c", 3), ("w", "u0", "c", 3), ("w", "u1", "c", 3),
    ),
    (),
    (
        ("w", "d", "c", 0), ("w", "d", "c", 4),
    ),
    (
        ("w", "d", 3), ("s", "d", 3, "c", 3),
    ),
    (
        ("w", "d", 7), ("s", "d", 7, "c", 7), ("w", "d", "c", 1), ("w", "d", "c", 5),
    ),
    (),
    (
        ("w", "d", "c", 2), ("w", "d", "c", 6),
    ),
    (),
    (
        ("w", "d", "c", 3), ("w", "d", "c", 7),
    ),
    (),
)
HOME_BLOCKS = {
    "attend": ((0, 0), (0, 1), (2, 0), (1, 0), (1, 1), (2, 1), (3, 0), (3, 1)),
    "gated": ((0, 0), (0, 1), (1, 0), (1, 1), (2, 0), (2, 1), (3, 0), (3, 1)),
    "down": ((0, 0), (0, 1), (1, 0), (1, 1), (2, 0), (2, 1), (3, 0), (3, 1)),
}
AWAY_STEPS = (
    (
        ("s", "o", 0, "c", 0), ("s", "d", 0, "c", 0), ("s", "o", "z", "z", 4), ("s", "q1", "own", "z", 2),
        ("s", "q1", "own", "y", "t"), ("s", "o", 0, "x", 1), ("s", "d", 0, "x", 1),
    ),
    (
        ("s", "q2", "own", "z", 2), ("s", "q2", "own", "y", "t"), ("w", "o", 1), ("s", "o", 1, "c", 1), ("w", "o", 4),
        ("s", "o", 4, "c", 4), ("s", "o", 4, "x", 5), ("s", "q0", "own", "y", "t"), ("w", "q1", 0),
        ("s", "q1", 0, "c", 0), ("s", "q1", 0, "x", 1), ("s", "q0", "own", "z", 2), ("w", "o", 2),
        ("s", "o", 2, "c", 2), ("s", "o", 0, "y", 2), ("w", "d", 1), ("s", "d", 1, "c", 1), ("w", "d", 4),
        ("s", "d", 4, "c", 4), ("s", "d", 4, "x", 5), ("s", "g0", "own", "z", 2), ("s", "o", 4, "y", 6), ("w", "o", 5),
        ("s", "o", 5, "c", 5), ("w", "q2", 0), ("s", "q2", 0, "c", 0), ("s", "g0", "own", "y", "t"), ("w", "o", 6),
        ("s", "o", 6, "c", 6), ("w", "q1", 2), ("s", "q1", 2, "c", 2), ("s", "q2", 0, "x", 1), ("w", "q1", 1),
        ("s", "q1", 1, "c", 1), ("s", "d", "z", "z", 4), ("s", "u0", "own", "y", "t"), ("w", "q0", 0),
        ("s", "q0", 0, "c", 0),
    ),
    (
        ("w", "q2", 2), ("s", "q2", 2, "c", 2), ("s", "q2", 2, "x", 3), ("w", "q0", "c", 0), ("w", "q1", "c", 0),
        ("w", "q2", "c", 0),
    ),
    (
        ("w", "d", 5), ("s", "d", 5, "c", 5), ("w", "q0", 2), ("s", "q0", 2, "c", 2), ("s", "u0", "own", "z", 2),
        ("s", "u1", "own", "y", "t"), ("s", "q0", 2, "x", 3),
    ),
    (
        ("w", "g0", 0), ("s", "g0", 0, "c", 0), ("w", "q2", 1), ("s", "q2", 1, "c", 1), ("w", "q0", "c", 2),
        ("w", "q1", "c", 2), ("w", "q2", "c", 2),
    ),
    (
        ("w", "q0", 1), ("s", "q0", 1, "c", 1), ("s", "u1", "own", "z", 2), ("s", "g1", "own", "y", "t"),
        ("s", "g0", 0, "x", 1),
    ),
    (
        ("w", "q2", 3), ("s", "q2", 3, "c", 3), ("w", "q1", 3), ("s", "q1", 3, "c", 3), ("w", "q0", "c", 1),
        ("w", "q1", "c", 1), ("w", "q2", "c", 1),
    ),
    (
        ("w", "g0", 2), ("s", "g0", 2, "c", 2), ("w", "q0", 3), ("s", "q0", 3, "c", 3), ("w", "o", 3),
        ("s", "o", 3, "c", 3), ("s", "g1", "own", "z", 2), ("s", "o", 1, "y", 3), ("s", "g0", 2, "x", 3),
    ),
    (
        ("w", "o", 7), ("s", "o", 7, "c", 7), ("s", "d", 0, "y", 2), ("w", "q0", "c", 3), ("w", "q1", "c", 3),
        ("w", "q2", "c", 3),
    ),
    (
        ("w", "u0", 2), ("s", "u0", 2, "c", 2), ("w", "g0", 1), ("s", "g0", 1, "c", 1), ("s", "u0", 2, "x", 3),
        ("w", "o", "c", 0), ("w", "o", "c", 1), ("w", "o", "c", 2), ("w", "o", "c", 3), ("w", "o", "c", 4),
        ("w", "o", "c", 5), ("w", "o", "c", 6), ("w", "o", "c", 7),
    ),
    (
        ("w", "u0", 0), ("s", "u0", 0, "c", 0), ("s", "d", 4, "y", 6), ("w", "u1", 2), ("s", "u1", 2, "c", 2),
        ("s", "u1", 2, "x", 3), ("w", "g0", 3), ("s", "g0", 3, "c", 3), ("w", "u1", 0), ("s", "u1", 0, "c", 0),
        ("s", "g0", 3, "y", 3), ("s", "u1", 0, "x", 1), ("w", "g1", 2), ("s", "g1", 2, "c", 2), ("w", "u0", 3),
        ("s", "u0", 3, "c", 3), ("w", "g1", 0), ("s", "g1", 0, "c", 0), ("s", "u0", 3, "y", 3), ("s", "g1", 0, "x", 1),
        ("w", "u1", 3), ("s", "u1", 3, "c", 3), ("w", "d", 2), ("s", "d", 2, "c", 2), ("s", "u1", 3, "y", 3),
        ("s", "g1", 2, "x", 3), ("w", "u1", 1), ("s", "u1", 1, "c", 1), ("w", "d", 6), ("s", "d", 6, "c", 6),
        ("s", "d", 1, "y", 3),
    ),
    (
        ("w", "g1", 1), ("s", "g1", 1, "c", 1), ("s", "d", 6, "x", 7),
    ),
    (
        ("w", "u0", 1), ("s", "u0", 1, "c", 1), ("w", "g0", "c", 0), ("w", "g1", "c", 0), ("w", "u0", "c", 0),
        ("w", "u1", "c", 0),
    ),
    (),
    (),
    (
        ("w", "g1", 3), ("s", "g1", 3, "c", 3), ("w", "g0", "c", 1), ("w", "g1", "c", 1), ("w", "u0", "c", 1),
        ("w", "u1", "c", 1),
    ),
    (
        ("w", "g0", "c", 2), ("w", "g1", "c", 2), ("w", "u0", "c", 2), ("w", "u1", "c", 2),
    ),
    (),
    (
        ("w", "d", 3), ("s", "d", 3, "c", 3), ("w", "g0", "c", 3), ("w", "g1", "c", 3), ("w", "u0", "c", 3),
        ("w", "u1", "c", 3),
    ),
    (),
    (
        ("w", "d", "c", 0), ("w", "d", "c", 4),
    ),
    (
        ("w", "d", 7), ("s", "d", 7, "c", 7),
    ),
    (
        ("w", "d", "c", 1), ("w", "d", "c", 5),
    ),
    (),
    (
        ("w", "d", "c", 2), ("w", "d", "c", 6),
    ),
    (),
    (
        ("w", "d", "c", 3), ("w", "d", "c", 7),
    ),
    (),
)
AWAY_BLOCKS = {
    "attend": ((0, 0), (0, 1), (2, 0), (2, 1), (1, 0), (1, 1), (3, 0), (3, 1)),
    "gated": ((0, 0), (0, 1), (1, 0), (2, 0), (1, 1), (2, 1), (3, 0), (3, 1)),
    "down": ((0, 0), (0, 1), (1, 0), (1, 1), (2, 0), (2, 1), (3, 0), (3, 1)),
}


class Place:
    def __init__(self):
        tp = lax.axis_index("tp")
        dp = lax.axis_index("dp")
        self.z = tp
        self.dp = dp
        self.y = dp // 4
        self.x = (dp // 2) % 2
        self.c = dp % 2
        self.far = lax.rem(self.y + self.z, 2)
        self.device = {
            "x": (tp, dp + 2 - 4 * self.x),
            "y": (tp, dp + 4 - 8 * self.y),
            "c": (tp, dp + 1 - 2 * self.c),
            "z": (1 - tp, dp),
        }

    def at(self, axis, flip):
        here = getattr(self, axis)
        return 1 - here if flip else here

    def row_block(self, k, core=0):
        return (self.at("x", k & 1) * 2 + self.at("c", core)) * 2 + self.at("z", k & 2)

    def col_block(self, k, core=0):
        return (self.at("y", k & 2) * 4 + self.at("x", k & 1) * 2 + self.at("c", core)) * 2 + self.at("z", k & 4)


def remote(src, dst, send, recv, device):
    return pltpu.make_async_remote_copy(
        src_ref=src, dst_ref=dst, send_sem=send, recv_sem=recv, device_id=device, device_id_type=MESH)


class Rows:
    def __init__(self, place, buf, start, own, through, index, sems):
        self.p, self.buf, self.start, self.own, self.through = place, buf, start, own, through
        self.i, (self.send, self.r, self.rc) = index, sems
        self.n = own.shape[0]

    def block(self, k, core=0):
        return self.buf.at[self.p.row_block(k, core), pl.ds(self.start, self.n)]

    def copy(self, k, link, home):
        p = self.p
        slot = {"own": 0, "t": 4}.get(k, k)
        send = self.send.at[self.i, "xyzc".index(link), slot]
        if k == "own" or (home and k == 0):
            src = self.own
        elif k == "t":
            src = self.through
        else:
            src = self.block(k)
        if k == "own" and link == "y":
            dst, recv = self.through, self.r.at[self.i, 4]
        else:
            dst = self.block(0 if k in ("own", "t") else k)
            got = 2 if link == "z" else k ^ 1 if link == "x" else k
            recv = self.rc.at[self.i, k] if link == "c" else self.r.at[self.i, got]
        return remote(src, dst, send, recv, p.device[link])

    def wait(self, k, core):
        if k == "t":
            ref, recv = self.through, self.r.at[self.i, 4]
        else:
            ref, recv = self.block(k, core), (self.rc if core else self.r).at[self.i, k]
        remote(ref, ref, self.send.at[self.i, 0, 0], recv, self.p.device["x"]).wait_recv()

    def local(self):
        @pl.when(self.p.far == 0)
        def _():
            self.buf[self.p.row_block(0), pl.ds(self.start, self.n)] = self.own[...]


class Cols:
    def __init__(self, place, buf, own, index, sems):
        self.p, self.buf, self.own = place, buf, own
        self.n = buf.shape[-1]
        self.i, (self.send, self.r, self.rc) = index, sems

    def block(self, k, core=0):
        return self.buf.at[self.p.col_block(k, core)]

    def half(self, z):
        return self.own.at[:, pl.ds(pl.multiple_of(z * self.n, 128), self.n)]

    def copy(self, k, link, home):
        p = self.p
        if link == "z":
            return remote(self.half(1 - p.z), self.block(0), self.send.at[self.i, 2, 0], self.r.at[self.i, 4], p.device["z"])
        src = self.half(p.z) if k == 0 else self.block(k)
        got = k ^ 1 if link == "x" else k ^ 2
        recv = self.rc.at[self.i, k] if link == "c" else self.r.at[self.i, got]
        return remote(src, self.block(k), self.send.at[self.i, "xyzc".index(link), k], recv, p.device[link])

    def wait(self, k, core):
        ref, recv = self.block(k, core), (self.rc if core else self.r).at[self.i, k]
        remote(ref, ref, self.send.at[self.i, 0, 0], recv, self.p.device["x"]).wait_recv()

    def local(self):
        self.buf[self.p.col_block(0)] = self.own[:, pl.ds(pl.multiple_of(self.p.z * self.n, 128), self.n)]


def layer_kernel(wq_hbm, wk_hbm, wv_hbm, wo_hbm, wg_hbm, wu_hbm, wd_hbm, x_hbm, k_hbm, v_hbm,
                 bq, bk, bv, ga, gm, cos_ref, sin_ref, len_ref,
                 wqkv, wgu, wout, wdn, k_lo, k_hi, v_lo, v_hi, smalls, x1_ref, down,
                 h_ref, sc_ref, o_ref, a_ref, t_q, t_gu, w_q, w_gu, wo, wd, x_ref, small, l_sem,
                 k_sem, v_sem, s_send, s_recv, p_send, p_recv, row_s, row_r, row_c, col_s, col_r, col_c):
    place = Place()
    me = place.dp * 2 + place.z
    row_sem, col_sem = (row_s, row_r, row_c), (col_s, col_r, col_c)
    loads = [(wq_hbm, w_q.at[0]), (wk_hbm, w_q.at[1]), (wv_hbm, w_q.at[2]), (wo_hbm, wo), (wg_hbm, w_gu.at[0]),
             (wu_hbm, w_gu.at[1]), (wd_hbm, wd), (x_hbm, x_ref)]
    loads = [pltpu.make_async_copy(src, dst, l_sem.at[i]) for i, (src, dst) in enumerate(loads)]
    for load in loads:
        load.start()
    chunks = {}
    for i in range(3):
        chunks[f"q{i}"] = Rows(place, wqkv, 64 * i, w_q.at[i], t_q.at[i], i, row_sem)
    for i in range(4):
        ref = w_gu.at[i // 2, pl.ds(88 * (i % 2), 88)]
        chunks["gu"[i // 2] + str(i % 2)] = Rows(place, wgu, 88 * i, ref, t_gu.at[i], 3 + i, row_sem)
    chunks["o"] = Cols(place, wout, wo, 0, col_sem)
    chunks["d"] = Cols(place, wdn, wd, 1, col_sem)
    roles = ((0, HOME_STEPS, HOME_BLOCKS), (1, AWAY_STEPS, AWAY_BLOCKS))
    step = iter(range(len(HOME_STEPS)))

    def go():
        now = next(step)
        for far, steps, _ in roles:
            if steps[now]:
                @pl.when(place.far == far)
                def _(far=far, steps=steps):
                    for action in steps[now]:
                        chunk = chunks[action[1]]
                        if action[0] == "s":
                            chunk.copy(action[2], action[3], far == 0).start()
                        elif action[2] == "c":
                            chunk.wait(action[3], 1)
                        else:
                            chunk.wait(action[2], 0)

    def by_role(kind, i, place_of, swap=False):
        home, away = (place_of(*blocks[kind][i]) for _, _, blocks in roles)
        if swap:
            home, away = away, home
        return home + place.far * (away - home)

    def cache_copy(i):
        head = by_role("attend", i, place.row_block)
        copies = []
        for hbm, lo, hi, sem in ((k_hbm, k_lo, k_hi, k_sem), (v_hbm, v_lo, v_hi, v_sem)):
            copies.append(pltpu.make_async_copy(hbm.at[pl.ds(0, 32), head], lo.at[:, head], sem.at[2 * i]))
            copies.append(pltpu.make_async_copy(hbm.at[pl.ds(32, 32), head], hi.at[:, head], sem.at[2 * i + 1]))
        return copies

    barrier = pltpu.get_barrier_semaphore()
    for i in range(1, 16):
        other = lax.rem(me + i, 16)
        pl.semaphore_signal(barrier, inc=1, device_id=(other % 2, other // 2), device_id_type=MESH)
    for i in range(8):
        for copy in cache_copy(i):
            copy.start()
    vectors = jnp.concatenate([v[...].astype(F32) for v in (bq, bk, bv, ga, gm)] + [jnp.zeros((3, 64), F32)], axis=0)
    vectors = jnp.concatenate([vectors, vectors], axis=1)
    mine = lax.broadcasted_iota(jnp.int32, (8, 128), 1) // 64 == place.z
    vectors = jnp.where(mine, vectors, 0.0).astype(BF16)
    small[...] = vectors
    smalls[me] = vectors
    for load in loads:
        load.wait()
    pl.semaphore_wait(barrier, 15)

    def small_copy(i):
        other = lax.rem(me + i, 16)
        return remote(small, smalls.at[me], s_send.at[i], s_recv.at[i], (other % 2, other // 2))

    for i in range(1, 16):
        small_copy(i).start()
    go()

    for chunk in chunks.values():
        chunk.local()
    for i in range(1, 16):
        small_copy(i).wait_recv()

    def gain_row(i):
        pair = smalls[...].astype(F32).reshape(8, 2, 8, 128)
        rows = pair[:, 0, i] + pair[:, 1, i]
        return jnp.concatenate([rows[d:d + 1] for d in range(8)], axis=1)

    def normed(rows, i):
        inv = lax.rsqrt(jnp.mean(rows * rows, axis=-1, keepdims=True) + EPS)
        return (rows * inv * gain_row(i)).astype(BF16)

    h_ref[...] = normed(x_ref[...].astype(F32), 3)

    eye = lax.broadcasted_iota(jnp.int32, (64, 128), 1) % 64 == lax.broadcasted_iota(jnp.int32, (64, 128), 0)

    def bias_column(head, i):
        row = smalls[place.z * 8 + head].astype(F32)[i:i + 1]
        return jnp.sum(jnp.where(eye, row, 0.0), axis=1, keepdims=True)

    def attend(i):
        head = by_role("attend", i, place.row_block)
        res = dot(wqkv[head], h_ref[...], ROW_BYTES)
        cos, sin = cos_ref[...], sin_ref[...]

        def rotated(start, b):
            v = (res[start:start + 64] + bias_column(head, b)).astype(BF16).astype(F32)
            lo, hi = v[:32], v[32:]
            return jnp.concatenate([lo * cos - hi * sin, hi * cos + lo * sin], axis=0).astype(BF16)

        q = rotated(0, 0).astype(F32)
        k_new = rotated(64, 1)
        v_new = (res[128:192] + bias_column(head, 2)).astype(BF16)
        lens = len_ref[...].astype(F32)
        for copy in cache_copy(i):
            copy.wait()

        for base, buf in ((0, k_lo), (32, k_hi)):
            def score_group(g, carry, base=base, buf=buf):
                rows = []
                for j in range(GROUP):
                    s = g * GROUP + j
                    kv = jnp.where(lens == (base + s).astype(F32), k_new.astype(F32), buf[s, head].astype(F32))
                    buf[s, head] = kv.astype(BF16)
                    rows.append(jnp.sum(q * kv, axis=0, keepdims=True))
                sc_ref[pl.ds(pl.multiple_of(base + g * GROUP, GROUP), GROUP)] = jnp.concatenate(rows, axis=0)
                return carry

            lax.fori_loop(0, 32 // GROUP, score_group, 0)
        slot = lax.broadcasted_iota(jnp.int32, (64, 256), 0).astype(F32)
        scores = jnp.where(slot <= lens, sc_ref[...] * 0.125, -1e30)
        e = jnp.exp(scores - jnp.max(scores, axis=0, keepdims=True))
        sc_ref[...] = (e / jnp.sum(e, axis=0, keepdims=True)).astype(BF16).astype(F32)

        acc = jnp.zeros((64, 256), F32)
        for base, buf in ((0, v_lo), (32, v_hi)):
            def value_group(g, acc, base=base, buf=buf):
                probs = sc_ref[pl.ds(pl.multiple_of(base + g * GROUP, GROUP), GROUP)]
                for j in range(GROUP):
                    s = g * GROUP + j
                    vv = jnp.where(lens == (base + s).astype(F32), v_new.astype(F32), buf[s, head].astype(F32))
                    buf[s, head] = vv.astype(BF16)
                    acc = acc + probs[j:j + 1] * vv
                return acc

            acc = lax.fori_loop(0, 32 // GROUP, value_group, acc)
        o_ref[pl.ds(pl.multiple_of(head * 64, 64), 64)] = acc.astype(BF16)

    go()
    for i in range(8):
        attend(i)
        go()

    o = o_ref[...].T
    part, part_in, h2_ref = down, x1_ref, h_ref
    part[...] = dot(o, wout[...].reshape(1024, 512), ROW_BYTES).astype(BF16)
    swap = remote(part, part_in, p_send, p_recv, place.device["z"])
    swap.start()
    go()
    swap.wait_recv()
    swap.wait_send()
    total = (part[...].astype(F32) + part_in[...].astype(F32)).astype(BF16)
    x1 = (x_ref[...].astype(F32) + total.astype(F32)).astype(BF16)
    x1_ref[...] = x1
    h2_ref[...] = normed(x1.astype(F32), 4)
    go()

    for i in range(8):
        block = by_role("gated", i, place.row_block)
        res = dot(wgu[block], h2_ref[...], ROW_BYTES).astype(BF16).astype(F32)
        g, u = res[:176], res[176:]
        a_ref[block] = (g / (1.0 + jnp.exp(-g)) * u).astype(BF16)
        go()

    for i in range(8):
        pair = by_role("down", i, lambda k, core: place.col_block(k, core) // 2)
        w = wdn[pl.ds(pair * 2, 2)].reshape(128, 1408)
        cols = pl.ds(pl.multiple_of(pair * 128, 128), 128)
        down[:, cols] = dot(w, a_ref[...].reshape(1408, 256), NAT).T.astype(BF16)
        go()

    for far, steps, _ in roles:
        @pl.when(place.far == far)
        def _(far=far, steps=steps):
            for action in sum(steps, ()):
                if action[0] == "s":
                    chunks[action[1]].copy(action[2], action[3], far == 0).wait_send()

    for i in range(1, 16):
        small_copy(i).wait_send()


def store_kernel(wqkv, wgu, wout, wdn, k_lo, k_hi, v_lo, v_hi, smalls,
                 wq, wk, wv, wo, wg, wu, wd, k_out, v_out, bq, bk, bv, ga, gm, sem):
    lo, hi = pl.ds(0, 32), pl.ds(32, 32)
    pairs = [(k_lo, k_out.at[lo]), (k_hi, k_out.at[hi]), (v_lo, v_out.at[lo]), (v_hi, v_out.at[hi]),
             (wdn, wd), (wgu.at[:, pl.ds(0, 176)], wg), (wgu.at[:, pl.ds(176, 176)], wu),
             (wqkv.at[:, pl.ds(0, 64)], wq), (wqkv.at[:, pl.ds(64, 64)], wk), (wqkv.at[:, pl.ds(128, 64)], wv),
             (wout, wo)]
    copies = [pltpu.make_async_copy(src, dst, sem.at[i]) for i, (src, dst) in enumerate(pairs)]
    for copy in copies:
        copy.start()
    z = lax.axis_index("tp")
    plane = smalls[pl.ds(z * 8, 8)].astype(F32).reshape(4, 2, 8, 128)
    whole = smalls[...].astype(F32).reshape(8, 2, 8, 128)
    for i, ref in enumerate((bq, bk, bv)):
        ref[...] = (plane[:, 0, i] + plane[:, 1, i]).astype(BF16)
    for i, ref in enumerate((ga, gm)):
        ref[...] = (whole[:, 0, 3 + i] + whole[:, 1, 3 + i]).astype(BF16)
    for copy in copies:
        copy.wait()


def finish_kernel(x1, mine, peer, hid):
    total = (mine[...].astype(F32) + peer[...].astype(F32)).astype(BF16)
    hid[...] = (x1[...].astype(F32) + total.astype(F32)).astype(BF16)


def local_step(w_query, b_query, w_key, b_key, w_value, b_value, w_out, w_gate, w_up, w_down, gain_attn, gain_mlp,
               hidden, k_cache, v_cache, lengths):
    inv_freq = 1.0 / (THETA ** (jnp.arange(0, 64, 2, dtype=F32) / 64))
    angles = inv_freq[:, None] * lengths.astype(F32)[None, :]
    cos, sin = jnp.cos(angles), jnp.sin(angles)
    lens = lengths[None, :]
    rows = [v[None, :] for v in (b_query, b_key, b_value, gain_attn, gain_mlp)]
    k_view = jnp.transpose(k_cache, (1, 2, 3, 0))
    v_view = jnp.transpose(v_cache, (1, 2, 3, 0))

    vmem = pl.BlockSpec(memory_space=pltpu.VMEM)
    hbm = pl.BlockSpec(memory_space=pltpu.HBM)
    anywhere = pl.BlockSpec(memory_space=pl.ANY)
    dma = pltpu.SemaphoreType.DMA
    shapes = [(8, 192, 1024), (8, 352, 1024), (16, 64, 512), (16, 64, 1408), *[(32, 8, 64, 256)] * 4,
              (16, 8, 128), (256, 1024), (256, 1024)]
    held = pl.pallas_call(
        layer_kernel,
        out_shape=[pltpu.VMEM(s, BF16) for s in shapes],
        in_specs=[hbm] * 10 + [vmem] * 8,
        out_specs=[vmem] * 11,
        scratch_shapes=[
            pltpu.VMEM((256, 1024), BF16),
            pltpu.VMEM((64, 256), F32),
            pltpu.VMEM((512, 256), BF16),
            pltpu.VMEM((8, 176, 256), BF16),
            pltpu.VMEM((3, 64, 1024), BF16),
            pltpu.VMEM((4, 88, 1024), BF16),
            pltpu.VMEM((3, 64, 1024), BF16),
            pltpu.VMEM((2, 176, 1024), BF16),
            pltpu.VMEM((64, 1024), BF16),
            pltpu.VMEM((64, 2816), BF16),
            pltpu.VMEM((256, 1024), BF16),
            pltpu.VMEM((8, 128), BF16),
            dma((8,)),
            dma((16,)), dma((16,)), dma((16,)), dma((16,)), dma, dma,
            dma((7, 4, 5)), dma((7, 5)), dma((7, 4)), dma((2, 4, 8)), dma((2, 8)), dma((2, 8)),
        ],
        compiler_params=pltpu.CompilerParams(collective_id=0, has_side_effects=True, vmem_limit_bytes=9437184),
        name="layer",
    )(w_query, w_key, w_value, w_out, w_gate, w_up, w_down, hidden, k_view, v_view, *rows, cos, sin, lens)

    def shape(*dims):
        return jax.ShapeDtypeStruct(dims, BF16)

    peer = lax.ppermute(held[10], "tp", [(0, 1), (1, 0)])
    outs = pl.pallas_call(
        store_kernel,
        out_shape=[shape(8, 64, 1024)] * 3 + [shape(16, 64, 512), shape(8, 176, 1024), shape(8, 176, 1024),
                   shape(16, 64, 1408), shape(*k_view.shape), shape(*v_view.shape),
                   shape(4, 128), shape(4, 128), shape(4, 128), shape(8, 128), shape(8, 128)],
        in_specs=[anywhere] * 8 + [vmem],
        out_specs=[hbm] * 9 + [vmem] * 5,
        scratch_shapes=[dma((11,))],
        compiler_params=pltpu.CompilerParams(vmem_limit_bytes=9437184),
        cost_estimate=pl.CostEstimate(flops=2 * 10**10, bytes_accessed=5 * 10**7, transcendentals=0),
        name="store",
    )(*held[:9])
    hid = pl.pallas_call(
        finish_kernel,
        out_shape=shape(256, 1024),
        in_specs=[vmem] * 3,
        out_specs=vmem,
        compiler_params=pltpu.CompilerParams(vmem_limit_bytes=9437184),
        name="finish",
    )(held[9], held[10], peer)
    wq, wk, wv, wo, wg, wu, wd, k_out, v_out, bq, bk, bv, ga, gm = outs
    flat = lambda a, n: a.reshape(-1, n)
    return (flat(wq, 1024), bq.reshape(512), flat(wk, 1024), bk.reshape(512), flat(wv, 1024), bv.reshape(512),
            flat(wo, 512), flat(wg, 1024), flat(wu, 1024), flat(wd, 1408), ga.reshape(1024), gm.reshape(1024),
            hid, jnp.transpose(k_out, (3, 0, 1, 2)), jnp.transpose(v_out, (3, 0, 1, 2)))


def solution(mesh):
    row_spec = P(("dp", "tp"), None)
    flat_spec = P(("dp", "tp"))
    cache_spec = P("dp", None, "tp", None)
    in_specs = (row_spec, flat_spec, row_spec, flat_spec, row_spec, flat_spec, row_spec, row_spec, row_spec, row_spec,
                flat_spec, flat_spec, P("dp", None), cache_spec, cache_spec, P("dp"))
    out_specs = (P("tp", None), P("tp"), P("tp", None), P("tp"), P("tp", None), P("tp"), P(None, "tp"), P("tp", None),
                 P("tp", None), P(None, "tp"), P(None), P(None), P("dp", None), cache_spec, cache_spec)
    return jax.shard_map(local_step, mesh=mesh, in_specs=in_specs, out_specs=out_specs, check_vma=False)
```

```python
import jax
import jax.numpy as jnp
from jax import lax
from jax.experimental import pallas as pl
from jax.experimental.pallas import tpu as pltpu
from jax.sharding import PartitionSpec as P

EPS = 1e-6
THETA = 1000000.0
MESH = pl.DeviceIdType.MESH
F32 = jnp.float32
BF16 = jnp.bfloat16
ROW_BYTES = (((1,), (1,)), ((), ()))
NAT = (((1,), (0,)), ((), ()))
GROUP = 8


def dot(lhs, rhs, dims):
    return lax.dot_general(lhs, rhs, dims, preferred_element_type=F32)


HOME_STEPS = (
    (
        ("s", "q0", 0, "c", 0), ("s", "q1", 0, "c", 0), ("s", "q2", 0, "c", 0), ("s", "g0", 0, "c", 0),
        ("s", "g1", 0, "c", 0), ("s", "u0", 0, "c", 0), ("s", "u1", 0, "c", 0), ("s", "o", 0, "c", 0),
        ("s", "d", 0, "c", 0), ("s", "o", "z", "z", 4), ("s", "d", "z", "z", 4), ("s", "q1", 0, "y", 0),
        ("s", "q1", 0, "x", 1),
    ),
    (
        ("s", "o", 0, "y", 2), ("s", "q2", 0, "y", 0), ("s", "o", 0, "x", 1), ("s", "q2", 0, "x", 1),
    ),
    (
        ("w", "o", 4), ("s", "o", 4, "c", 4), ("w", "q0", "c", 0), ("w", "q1", "c", 0), ("w", "q2", "c", 0),
    ),
    (
        ("w", "q1", "t"), ("w", "q1", 1), ("s", "q1", 1, "c", 1), ("s", "q1", "t", "z", 2), ("s", "o", 4, "y", 6),
        ("s", "o", 4, "x", 5), ("w", "q1", 2), ("s", "q1", 2, "c", 2), ("w", "o", 1), ("s", "o", 1, "c", 1),
        ("s", "q0", 0, "y", 0), ("s", "q0", 0, "x", 1), ("w", "q2", "t"), ("s", "q2", "t", "z", 2), ("w", "q2", 1),
        ("s", "q2", 1, "c", 1), ("w", "q2", 2), ("s", "q2", 2, "c", 2), ("s", "g0", 0, "y", 0), ("s", "q1", 2, "x", 3),
        ("w", "o", 5), ("s", "o", 5, "c", 5), ("w", "q0", "t"), ("s", "q0", "t", "z", 2), ("w", "o", 2),
        ("s", "o", 2, "c", 2), ("w", "q0", 2), ("s", "q0", 2, "c", 2),
    ),
    (
        ("w", "o", 6), ("s", "o", 6, "c", 6), ("w", "q0", 1), ("s", "q0", 1, "c", 1), ("s", "q0", 1, "y", 1),
        ("s", "q2", 2, "x", 3),
    ),
    (
        ("s", "q0", 2, "x", 3), ("w", "q0", "c", 1), ("w", "q1", "c", 1), ("w", "q2", "c", 1),
    ),
    (
        ("w", "g0", 2), ("s", "g0", 2, "c", 2), ("w", "q1", 3), ("s", "q1", 3, "c", 3), ("w", "g0", "t"),
        ("s", "g0", "t", "z", 2), ("s", "q1", 3, "y", 3), ("w", "q0", "c", 2), ("w", "q1", "c", 2), ("w", "q2", "c", 2),
    ),
    (
        ("w", "q2", 3), ("s", "q2", 3, "c", 3), ("s", "o", 1, "y", 3), ("s", "g0", 0, "x", 1), ("w", "d", 4),
        ("s", "d", 4, "c", 4), ("s", "o", 5, "y", 7), ("w", "u0", "t"), ("s", "u0", "t", "z", 2),
        ("s", "u0", 0, "y", 0), ("s", "o", 6, "x", 7), ("w", "q0", 3), ("s", "q0", 3, "c", 3),
    ),
    (
        ("w", "u0", 2), ("s", "u0", 2, "c", 2), ("s", "u0", 0, "x", 1), ("w", "q0", "c", 3), ("w", "q1", "c", 3),
        ("w", "q2", "c", 3),
    ),
    (
        ("w", "u1", "t"), ("s", "u1", "t", "z", 2), ("s", "u1", 0, "y", 0), ("w", "g0", 1), ("s", "g0", 1, "c", 1),
        ("s", "u1", 0, "x", 1), ("w", "o", 7), ("s", "o", 7, "c", 7), ("w", "u1", 2), ("s", "u1", 2, "c", 2),
        ("w", "g1", "t"), ("s", "g1", "t", "z", 2), ("s", "g1", 0, "y", 0), ("w", "o", 3), ("s", "o", 3, "c", 3),
        ("s", "g1", 0, "x", 1), ("w", "u0", 1), ("s", "u0", 1, "c", 1), ("w", "g1", 2), ("s", "g1", 2, "c", 2),
        ("w", "o", "c", 0), ("w", "o", "c", 1), ("w", "o", "c", 2), ("w", "o", "c", 3), ("w", "o", "c", 4),
        ("w", "o", "c", 5), ("w", "o", "c", 6), ("w", "o", "c", 7),
    ),
    (
        ("s", "d", 0, "y", 2), ("w", "d", 2), ("s", "d", 2, "c", 2), ("s", "d", 0, "x", 1), ("w", "u1", 1),
        ("s", "u1", 1, "c", 1), ("s", "d", 4, "y", 6), ("w", "d", 6), ("s", "d", 6, "c", 6), ("s", "d", 4, "x", 5),
        ("w", "g1", 1), ("s", "g1", 1, "c", 1), ("s", "u0", 1, "y", 1), ("w", "g0", 3), ("s", "g0", 3, "c", 3),
        ("s", "g1", 2, "x", 3), ("w", "d", 1), ("s", "d", 1, "c", 1),
    ),
    (
        ("s", "d", 1, "y", 3),
    ),
    (
        ("w", "u0", 3), ("s", "u0", 3, "c", 3), ("w", "g0", "c", 0), ("w", "g1", "c", 0), ("w", "u0", "c", 0),
        ("w", "u1", "c", 0),
    ),
    (
        ("w", "d", 5), ("s", "d", 5, "c", 5), ("s", "d", 6, "x", 7),
    ),
    (
        ("w", "g0", "c", 1), ("w", "g1", "c", 1), ("w", "u0", "c", 1), ("w", "u1", "c", 1),
    ),
    (),
    (
        ("w", "g0", "c", 2), ("w", "g1", "c", 2), ("w", "u0", "c", 2), ("w", "u1", "c", 2),
    ),
    (
        ("w", "u1", 3), ("s", "u1", 3, "c", 3), ("w", "g1", 3), ("s", "g1", 3, "c", 3),
    ),
    (
        ("w", "g0", "c", 3), ("w", "g1", "c", 3), ("w", "u0", "c", 3), ("w", "u1", "c", 3),
    ),
    (),
    (
        ("w", "d", "c", 0), ("w", "d", "c", 4),
    ),
    (
        ("w", "d", 3), ("s", "d", 3, "c", 3),
    ),
    (
        ("w", "d", 7), ("s", "d", 7, "c", 7), ("w", "d", "c", 1), ("w", "d", "c", 5),
    ),
    (),
    (
        ("w", "d", "c", 2), ("w", "d", "c", 6),
    ),
    (),
    (
        ("w", "d", "c", 3), ("w", "d", "c", 7),
    ),
    (),
)
HOME_BLOCKS = {
    "attend": ((0, 0), (0, 1), (2, 0), (1, 0), (1, 1), (2, 1), (3, 0), (3, 1)),
    "gated": ((0, 0), (0, 1), (1, 0), (1, 1), (2, 0), (2, 1), (3, 0), (3, 1)),
    "down": ((0, 0), (0, 1), (1, 0), (1, 1), (2, 0), (2, 1), (3, 0), (3, 1)),
}
AWAY_STEPS = (
    (
        ("s", "o", 0, "c", 0), ("s", "d", 0, "c", 0), ("s", "o", "z", "z", 4), ("s", "q1", "own", "z", 2),
        ("s", "q1", "own", "y", "t"), ("s", "o", 0, "x", 1), ("s", "d", 0, "x", 1),
    ),
    (
        ("s", "q2", "own", "z", 2), ("s", "q2", "own", "y", "t"), ("w", "o", 1), ("s", "o", 1, "c", 1), ("w", "o", 4),
        ("s", "o", 4, "c", 4), ("s", "o", 4, "x", 5), ("s", "q0", "own", "y", "t"), ("w", "q1", 0),
        ("s", "q1", 0, "c", 0), ("s", "q1", 0, "x", 1), ("s", "q0", "own", "z", 2), ("w", "o", 2),
        ("s", "o", 2, "c", 2), ("s", "o", 0, "y", 2), ("w", "d", 1), ("s", "d", 1, "c", 1), ("w", "d", 4),
        ("s", "d", 4, "c", 4), ("s", "d", 4, "x", 5), ("s", "g0", "own", "z", 2), ("s", "o", 4, "y", 6), ("w", "o", 5),
        ("s", "o", 5, "c", 5), ("w", "q2", 0), ("s", "q2", 0, "c", 0), ("s", "g0", "own", "y", "t"), ("w", "o", 6),
        ("s", "o", 6, "c", 6), ("w", "q1", 2), ("s", "q1", 2, "c", 2), ("s", "q2", 0, "x", 1), ("w", "q1", 1),
        ("s", "q1", 1, "c", 1), ("s", "d", "z", "z", 4), ("s", "u0", "own", "y", "t"), ("w", "q0", 0),
        ("s", "q0", 0, "c", 0),
    ),
    (
        ("w", "q2", 2), ("s", "q2", 2, "c", 2), ("s", "q2", 2, "x", 3), ("w", "q0", "c", 0), ("w", "q1", "c", 0),
        ("w", "q2", "c", 0),
    ),
    (
        ("w", "d", 5), ("s", "d", 5, "c", 5), ("w", "q0", 2), ("s", "q0", 2, "c", 2), ("s", "u0", "own", "z", 2),
        ("s", "u1", "own", "y", "t"), ("s", "q0", 2, "x", 3),
    ),
    (
        ("w", "g0", 0), ("s", "g0", 0, "c", 0), ("w", "q2", 1), ("s", "q2", 1, "c", 1), ("w", "q0", "c", 2),
        ("w", "q1", "c", 2), ("w", "q2", "c", 2),
    ),
    (
        ("w", "q0", 1), ("s", "q0", 1, "c", 1), ("s", "u1", "own", "z", 2), ("s", "g1", "own", "y", "t"),
        ("s", "g0", 0, "x", 1),
    ),
    (
        ("w", "q2", 3), ("s", "q2", 3, "c", 3), ("w", "q1", 3), ("s", "q1", 3, "c", 3), ("w", "q0", "c", 1),
        ("w", "q1", "c", 1), ("w", "q2", "c", 1),
    ),
    (
        ("w", "g0", 2), ("s", "g0", 2, "c", 2), ("w", "q0", 3), ("s", "q0", 3, "c", 3), ("w", "o", 3),
        ("s", "o", 3, "c", 3), ("s", "g1", "own", "z", 2), ("s", "o", 1, "y", 3), ("s", "g0", 2, "x", 3),
    ),
    (
        ("w", "o", 7), ("s", "o", 7, "c", 7), ("s", "d", 0, "y", 2), ("w", "q0", "c", 3), ("w", "q1", "c", 3),
        ("w", "q2", "c", 3),
    ),
    (
        ("w", "u0", 2), ("s", "u0", 2, "c", 2), ("w", "g0", 1), ("s", "g0", 1, "c", 1), ("s", "u0", 2, "x", 3),
        ("w", "o", "c", 0), ("w", "o", "c", 1), ("w", "o", "c", 2), ("w", "o", "c", 3), ("w", "o", "c", 4),
        ("w", "o", "c", 5), ("w", "o", "c", 6), ("w", "o", "c", 7),
    ),
    (
        ("w", "u0", 0), ("s", "u0", 0, "c", 0), ("s", "d", 4, "y", 6), ("w", "u1", 2), ("s", "u1", 2, "c", 2),
        ("s", "u1", 2, "x", 3), ("w", "g0", 3), ("s", "g0", 3, "c", 3), ("w", "u1", 0), ("s", "u1", 0, "c", 0),
        ("s", "g0", 3, "y", 3), ("s", "u1", 0, "x", 1), ("w", "g1", 2), ("s", "g1", 2, "c", 2), ("w", "u0", 3),
        ("s", "u0", 3, "c", 3), ("w", "g1", 0), ("s", "g1", 0, "c", 0), ("s", "u0", 3, "y", 3), ("s", "g1", 0, "x", 1),
        ("w", "u1", 3), ("s", "u1", 3, "c", 3), ("w", "d", 2), ("s", "d", 2, "c", 2), ("s", "u1", 3, "y", 3),
        ("s", "g1", 2, "x", 3), ("w", "u1", 1), ("s", "u1", 1, "c", 1), ("w", "d", 6), ("s", "d", 6, "c", 6),
        ("s", "d", 1, "y", 3),
    ),
    (
        ("w", "g1", 1), ("s", "g1", 1, "c", 1), ("s", "d", 6, "x", 7),
    ),
    (
        ("w", "u0", 1), ("s", "u0", 1, "c", 1), ("w", "g0", "c", 0), ("w", "g1", "c", 0), ("w", "u0", "c", 0),
        ("w", "u1", "c", 0),
    ),
    (),
    (),
    (
        ("w", "g1", 3), ("s", "g1", 3, "c", 3), ("w", "g0", "c", 1), ("w", "g1", "c", 1), ("w", "u0", "c", 1),
        ("w", "u1", "c", 1),
    ),
    (
        ("w", "g0", "c", 2), ("w", "g1", "c", 2), ("w", "u0", "c", 2), ("w", "u1", "c", 2),
    ),
    (),
    (
        ("w", "d", 3), ("s", "d", 3, "c", 3), ("w", "g0", "c", 3), ("w", "g1", "c", 3), ("w", "u0", "c", 3),
        ("w", "u1", "c", 3),
    ),
    (),
    (
        ("w", "d", "c", 0), ("w", "d", "c", 4),
    ),
    (
        ("w", "d", 7), ("s", "d", 7, "c", 7),
    ),
    (
        ("w", "d", "c", 1), ("w", "d", "c", 5),
    ),
    (),
    (
        ("w", "d", "c", 2), ("w", "d", "c", 6),
    ),
    (),
    (
        ("w", "d", "c", 3), ("w", "d", "c", 7),
    ),
    (),
)
AWAY_BLOCKS = {
    "attend": ((0, 0), (0, 1), (2, 0), (2, 1), (1, 0), (1, 1), (3, 0), (3, 1)),
    "gated": ((0, 0), (0, 1), (1, 0), (2, 0), (1, 1), (2, 1), (3, 0), (3, 1)),
    "down": ((0, 0), (0, 1), (1, 0), (1, 1), (2, 0), (2, 1), (3, 0), (3, 1)),
}


class Place:
    def __init__(self):
        tp = lax.axis_index("tp")
        dp = lax.axis_index("dp")
        self.z = tp
        self.dp = dp
        self.y = dp // 4
        self.x = (dp // 2) % 2
        self.c = dp % 2
        self.far = lax.rem(self.y + self.z, 2)
        self.device = {
            "x": (tp, dp + 2 - 4 * self.x),
            "y": (tp, dp + 4 - 8 * self.y),
            "c": (tp, dp + 1 - 2 * self.c),
            "z": (1 - tp, dp),
        }

    def at(self, axis, flip):
        here = getattr(self, axis)
        return 1 - here if flip else here

    def row_block(self, k, core=0):
        return (self.at("x", k & 1) * 2 + self.at("c", core)) * 2 + self.at("z", k & 2)

    def col_block(self, k, core=0):
        return (self.at("y", k & 2) * 4 + self.at("x", k & 1) * 2 + self.at("c", core)) * 2 + self.at("z", k & 4)


def remote(src, dst, send, recv, device):
    return pltpu.make_async_remote_copy(
        src_ref=src, dst_ref=dst, send_sem=send, recv_sem=recv, device_id=device, device_id_type=MESH)


class Rows:
    def __init__(self, place, buf, start, own, through, index, sems):
        self.p, self.buf, self.start, self.own, self.through = place, buf, start, own, through
        self.i, (self.send, self.r, self.rc) = index, sems
        self.n = own.shape[0]

    def block(self, k, core=0):
        return self.buf.at[self.p.row_block(k, core), pl.ds(self.start, self.n)]

    def copy(self, k, link, home):
        p = self.p
        slot = {"own": 0, "t": 4}.get(k, k)
        send = self.send.at[self.i, "xyzc".index(link), slot]
        if k == "own" or (home and k == 0):
            src = self.own
        elif k == "t":
            src = self.through
        else:
            src = self.block(k)
        if k == "own" and link == "y":
            dst, recv = self.through, self.r.at[self.i, 4]
        else:
            dst = self.block(0 if k in ("own", "t") else k)
            got = 2 if link == "z" else k ^ 1 if link == "x" else k
            recv = self.rc.at[self.i, k] if link == "c" else self.r.at[self.i, got]
        return remote(src, dst, send, recv, p.device[link])

    def wait(self, k, core):
        if k == "t":
            ref, recv = self.through, self.r.at[self.i, 4]
        else:
            ref, recv = self.block(k, core), (self.rc if core else self.r).at[self.i, k]
        remote(ref, ref, self.send.at[self.i, 0, 0], recv, self.p.device["x"]).wait_recv()

    def local(self):
        @pl.when(self.p.far == 0)
        def _():
            self.buf[self.p.row_block(0), pl.ds(self.start, self.n)] = self.own[...]


class Cols:
    def __init__(self, place, buf, own, index, sems):
        self.p, self.buf, self.own = place, buf, own
        self.n = buf.shape[-1]
        self.i, (self.send, self.r, self.rc) = index, sems

    def block(self, k, core=0):
        return self.buf.at[self.p.col_block(k, core)]

    def half(self, z):
        return self.own.at[:, pl.ds(pl.multiple_of(z * self.n, 128), self.n)]

    def copy(self, k, link, home):
        p = self.p
        if link == "z":
            return remote(self.half(1 - p.z), self.block(0), self.send.at[self.i, 2, 0], self.r.at[self.i, 4], p.device["z"])
        src = self.half(p.z) if k == 0 else self.block(k)
        got = k ^ 1 if link == "x" else k ^ 2
        recv = self.rc.at[self.i, k] if link == "c" else self.r.at[self.i, got]
        return remote(src, self.block(k), self.send.at[self.i, "xyzc".index(link), k], recv, p.device[link])

    def wait(self, k, core):
        ref, recv = self.block(k, core), (self.rc if core else self.r).at[self.i, k]
        remote(ref, ref, self.send.at[self.i, 0, 0], recv, self.p.device["x"]).wait_recv()

    def local(self):
        self.buf[self.p.col_block(0)] = self.own[:, pl.ds(pl.multiple_of(self.p.z * self.n, 128), self.n)]


def layer_kernel(wq_hbm, wk_hbm, wv_hbm, wo_hbm, wg_hbm, wu_hbm, wd_hbm, x_hbm, k_hbm, v_hbm,
                 bq, bk, bv, ga, gm, freq_ref, len_ref,
                 wqkv, wgu, wout, wdn, k_lo, k_hi, v_lo, v_hi, smalls, x1_ref, down,
                 h_ref, sc_ref, o_ref, a_ref, cos_ref, sin_ref, t_q, t_gu, w_q, w_gu, wo, wd, x_ref, small, l_sem,
                 k_sem, v_sem, s_send, s_recv, p_send, p_recv, row_s, row_r, row_c, col_s, col_r, col_c):
    place = Place()
    me = place.dp * 2 + place.z
    row_sem, col_sem = (row_s, row_r, row_c), (col_s, col_r, col_c)
    loads = [(wq_hbm, w_q.at[0]), (wk_hbm, w_q.at[1]), (wv_hbm, w_q.at[2]), (wo_hbm, wo), (wg_hbm, w_gu.at[0]),
             (wu_hbm, w_gu.at[1]), (wd_hbm, wd), (x_hbm, x_ref)]
    loads = [pltpu.make_async_copy(src, dst, l_sem.at[i]) for i, (src, dst) in enumerate(loads)]
    for load in loads:
        load.start()
    chunks = {}
    for i in range(3):
        chunks[f"q{i}"] = Rows(place, wqkv, 64 * i, w_q.at[i], t_q.at[i], i, row_sem)
    for i in range(4):
        ref = w_gu.at[i // 2, pl.ds(88 * (i % 2), 88)]
        chunks["gu"[i // 2] + str(i % 2)] = Rows(place, wgu, 88 * i, ref, t_gu.at[i], 3 + i, row_sem)
    chunks["o"] = Cols(place, wout, wo, 0, col_sem)
    chunks["d"] = Cols(place, wdn, wd, 1, col_sem)
    roles = ((0, HOME_STEPS, HOME_BLOCKS), (1, AWAY_STEPS, AWAY_BLOCKS))
    step = iter(range(len(HOME_STEPS)))

    def go():
        now = next(step)
        for far, steps, _ in roles:
            if steps[now]:
                @pl.when(place.far == far)
                def _(far=far, steps=steps):
                    for action in steps[now]:
                        chunk = chunks[action[1]]
                        if action[0] == "s":
                            chunk.copy(action[2], action[3], far == 0).start()
                        elif action[2] == "c":
                            chunk.wait(action[3], 1)
                        else:
                            chunk.wait(action[2], 0)

    def by_role(kind, i, place_of, swap=False):
        home, away = (place_of(*blocks[kind][i]) for _, _, blocks in roles)
        if swap:
            home, away = away, home
        return home + place.far * (away - home)

    def cache_copy(i):
        head = by_role("attend", i, place.row_block)
        copies = []
        for hbm, lo, hi, sem in ((k_hbm, k_lo, k_hi, k_sem), (v_hbm, v_lo, v_hi, v_sem)):
            copies.append(pltpu.make_async_copy(hbm.at[pl.ds(0, 32), head], lo.at[:, head], sem.at[2 * i]))
            copies.append(pltpu.make_async_copy(hbm.at[pl.ds(32, 32), head], hi.at[:, head], sem.at[2 * i + 1]))
        return copies

    barrier = pltpu.get_barrier_semaphore()
    for i in range(1, 16):
        other = lax.rem(me + i, 16)
        pl.semaphore_signal(barrier, inc=1, device_id=(other % 2, other // 2), device_id_type=MESH)
    vectors = jnp.concatenate([v[...].astype(F32) for v in (bq, bk, bv, ga, gm)] + [jnp.zeros((3, 64), F32)], axis=0)
    vectors = jnp.concatenate([vectors, vectors], axis=1)
    mine = lax.broadcasted_iota(jnp.int32, (8, 128), 1) // 64 == place.z
    vectors = jnp.where(mine, vectors, 0.0).astype(BF16)
    small[...] = vectors
    smalls[me] = vectors
    angles = freq_ref[...] * len_ref[...].astype(F32)
    cos_ref[...] = jnp.cos(angles)
    sin_ref[...] = jnp.sin(angles)
    for load in loads:
        load.wait()
    pl.semaphore_wait(barrier, 15)

    def small_copy(i):
        other = lax.rem(me + i, 16)
        return remote(small, smalls.at[me], s_send.at[i], s_recv.at[i], (other % 2, other // 2))

    go()
    for i in range(1, 16):
        small_copy(i).start()
    for i in range(8):
        for copy in cache_copy(i):
            copy.start()

    for chunk in chunks.values():
        chunk.local()
    for i in range(1, 16):
        small_copy(i).wait_recv()

    def gain_row(i):
        pair = smalls[...].astype(F32).reshape(8, 2, 8, 128)
        rows = pair[:, 0, i] + pair[:, 1, i]
        return jnp.concatenate([rows[d:d + 1] for d in range(8)], axis=1)

    def normed(rows, i):
        inv = lax.rsqrt(jnp.mean(rows * rows, axis=-1, keepdims=True) + EPS)
        return (rows * inv * gain_row(i)).astype(BF16)

    h_ref[...] = normed(x_ref[...].astype(F32), 3)

    eye = lax.broadcasted_iota(jnp.int32, (64, 128), 1) % 64 == lax.broadcasted_iota(jnp.int32, (64, 128), 0)

    def bias_column(head, i):
        row = smalls[place.z * 8 + head].astype(F32)[i:i + 1]
        return jnp.sum(jnp.where(eye, row, 0.0), axis=1, keepdims=True)

    def attend(i):
        head = by_role("attend", i, place.row_block)
        res = dot(wqkv[head], h_ref[...], ROW_BYTES)
        cos, sin = cos_ref[...], sin_ref[...]

        def rotated(start, b):
            v = (res[start:start + 64] + bias_column(head, b)).astype(BF16).astype(F32)
            lo, hi = v[:32], v[32:]
            return jnp.concatenate([lo * cos - hi * sin, hi * cos + lo * sin], axis=0).astype(BF16)

        q = rotated(0, 0).astype(F32)
        k_new = rotated(64, 1)
        v_new = (res[128:192] + bias_column(head, 2)).astype(BF16)
        lens = len_ref[...].astype(F32)
        for copy in cache_copy(i):
            copy.wait()

        for base, buf in ((0, k_lo), (32, k_hi)):
            def score_group(g, carry, base=base, buf=buf):
                rows = []
                for j in range(GROUP):
                    s = g * GROUP + j
                    kv = jnp.where(lens == (base + s).astype(F32), k_new.astype(F32), buf[s, head].astype(F32))
                    buf[s, head] = kv.astype(BF16)
                    rows.append(jnp.sum(q * kv, axis=0, keepdims=True))
                sc_ref[pl.ds(pl.multiple_of(base + g * GROUP, GROUP), GROUP)] = jnp.concatenate(rows, axis=0)
                return carry

            lax.fori_loop(0, 32 // GROUP, score_group, 0)
        slot = lax.broadcasted_iota(jnp.int32, (64, 256), 0).astype(F32)
        scores = jnp.where(slot <= lens, sc_ref[...] * 0.125, -1e30)
        e = jnp.exp(scores - jnp.max(scores, axis=0, keepdims=True))
        sc_ref[...] = (e / jnp.sum(e, axis=0, keepdims=True)).astype(BF16).astype(F32)

        acc = jnp.zeros((64, 256), F32)
        for base, buf in ((0, v_lo), (32, v_hi)):
            def value_group(g, acc, base=base, buf=buf):
                probs = sc_ref[pl.ds(pl.multiple_of(base + g * GROUP, GROUP), GROUP)]
                for j in range(GROUP):
                    s = g * GROUP + j
                    vv = jnp.where(lens == (base + s).astype(F32), v_new.astype(F32), buf[s, head].astype(F32))
                    buf[s, head] = vv.astype(BF16)
                    acc = acc + probs[j:j + 1] * vv
                return acc

            acc = lax.fori_loop(0, 32 // GROUP, value_group, acc)
        o_ref[pl.ds(pl.multiple_of(head * 64, 64), 64)] = acc.astype(BF16)

    go()
    for i in range(8):
        attend(i)
        go()

    o = o_ref[...].T
    part, part_in, h2_ref = down, x1_ref, h_ref
    part[...] = dot(o, wout[...].reshape(1024, 512), ROW_BYTES).astype(BF16)
    swap = remote(part, part_in, p_send, p_recv, place.device["z"])
    swap.start()
    go()
    swap.wait_recv()
    swap.wait_send()
    total = (part[...].astype(F32) + part_in[...].astype(F32)).astype(BF16)
    x1 = (x_ref[...].astype(F32) + total.astype(F32)).astype(BF16)
    x1_ref[...] = x1
    h2_ref[...] = normed(x1.astype(F32), 4)
    go()

    for i in range(8):
        block = by_role("gated", i, place.row_block)
        res = dot(wgu[block], h2_ref[...], ROW_BYTES).astype(BF16).astype(F32)
        g, u = res[:176], res[176:]
        a_ref[block] = (g / (1.0 + jnp.exp(-g)) * u).astype(BF16)
        go()

    for i in range(8):
        pair = by_role("down", i, lambda k, core: place.col_block(k, core) // 2)
        w = wdn[pl.ds(pair * 2, 2)].reshape(128, 1408)
        cols = pl.ds(pl.multiple_of(pair * 128, 128), 128)
        down[:, cols] = dot(w, a_ref[...].reshape(1408, 256), NAT).T.astype(BF16)
        go()

    for far, steps, _ in roles:
        @pl.when(place.far == far)
        def _(far=far, steps=steps):
            for action in sum(steps, ()):
                if action[0] == "s":
                    chunks[action[1]].copy(action[2], action[3], far == 0).wait_send()

    for i in range(1, 16):
        small_copy(i).wait_send()


def store_kernel(wqkv, wgu, wout, wdn, k_lo, k_hi, v_lo, v_hi, smalls,
                 wq, wk, wv, wo, wg, wu, wd, k_out, v_out, bq, bk, bv, ga, gm, sem):
    pairs = [(src.at[pl.ds(16 * i, 16)], dst.at[pl.ds(base + 16 * i, 16)]) for src, dst, base in (
        (k_lo, k_out, 0), (k_hi, k_out, 32), (v_lo, v_out, 0), (v_hi, v_out, 32)) for i in range(2)]
    pairs += [(wdn, wd), (wgu.at[:, pl.ds(0, 176)], wg), (wgu.at[:, pl.ds(176, 176)], wu),
             (wqkv.at[:, pl.ds(0, 64)], wq), (wqkv.at[:, pl.ds(64, 64)], wk), (wqkv.at[:, pl.ds(128, 64)], wv),
             (wout, wo)]
    copies = [pltpu.make_async_copy(src, dst, sem.at[i]) for i, (src, dst) in enumerate(pairs)]
    for copy in copies:
        copy.start()
    z = lax.axis_index("tp")
    plane = smalls[pl.ds(z * 8, 8)].astype(F32).reshape(4, 2, 8, 128)
    whole = smalls[...].astype(F32).reshape(8, 2, 8, 128)
    for i, ref in enumerate((bq, bk, bv)):
        ref[...] = (plane[:, 0, i] + plane[:, 1, i]).astype(BF16)
    for i, ref in enumerate((ga, gm)):
        ref[...] = (whole[:, 0, 3 + i] + whole[:, 1, 3 + i]).astype(BF16)
    for copy in copies:
        copy.wait()


def finish_kernel(x1, mine, peer, hid):
    total = (mine[...].astype(F32) + peer[...].astype(F32)).astype(BF16)
    hid[...] = (x1[...].astype(F32) + total.astype(F32)).astype(BF16)


def local_step(w_query, b_query, w_key, b_key, w_value, b_value, w_out, w_gate, w_up, w_down, gain_attn, gain_mlp,
               hidden, k_cache, v_cache, lengths):
    inv_freq = 1.0 / (THETA ** (jnp.arange(0, 64, 2, dtype=F32) / 64))
    freq = jnp.broadcast_to(inv_freq[:, None], (32, 256))
    lens = lengths[None, :]
    rows = [v[None, :] for v in (b_query, b_key, b_value, gain_attn, gain_mlp)]
    k_view = jnp.transpose(k_cache, (1, 2, 3, 0))
    v_view = jnp.transpose(v_cache, (1, 2, 3, 0))

    vmem = pl.BlockSpec(memory_space=pltpu.VMEM)
    hbm = pl.BlockSpec(memory_space=pltpu.HBM)
    anywhere = pl.BlockSpec(memory_space=pl.ANY)
    dma = pltpu.SemaphoreType.DMA
    shapes = [(8, 192, 1024), (8, 352, 1024), (16, 64, 512), (16, 64, 1408), *[(32, 8, 64, 256)] * 4,
              (16, 8, 128), (256, 1024), (256, 1024)]
    held = pl.pallas_call(
        layer_kernel,
        out_shape=[pltpu.VMEM(s, BF16) for s in shapes],
        in_specs=[hbm] * 10 + [vmem] * 7,
        out_specs=[vmem] * 11,
        scratch_shapes=[
            pltpu.VMEM((256, 1024), BF16),
            pltpu.VMEM((64, 256), F32),
            pltpu.VMEM((512, 256), BF16),
            pltpu.VMEM((8, 176, 256), BF16),
            pltpu.VMEM((32, 256), F32),
            pltpu.VMEM((32, 256), F32),
            pltpu.VMEM((3, 64, 1024), BF16),
            pltpu.VMEM((4, 88, 1024), BF16),
            pltpu.VMEM((3, 64, 1024), BF16),
            pltpu.VMEM((2, 176, 1024), BF16),
            pltpu.VMEM((64, 1024), BF16),
            pltpu.VMEM((64, 2816), BF16),
            pltpu.VMEM((256, 1024), BF16),
            pltpu.VMEM((8, 128), BF16),
            dma((8,)),
            dma((16,)), dma((16,)), dma((16,)), dma((16,)), dma, dma,
            dma((7, 4, 5)), dma((7, 5)), dma((7, 4)), dma((2, 4, 8)), dma((2, 8)), dma((2, 8)),
        ],
        compiler_params=pltpu.CompilerParams(collective_id=0, has_side_effects=True, vmem_limit_bytes=9437184),
        name="layer",
    )(w_query, w_key, w_value, w_out, w_gate, w_up, w_down, hidden, k_view, v_view, *rows, freq, lens)

    def shape(*dims):
        return jax.ShapeDtypeStruct(dims, BF16)

    peer = lax.ppermute(held[10], "tp", [(0, 1), (1, 0)])
    outs = pl.pallas_call(
        store_kernel,
        out_shape=[shape(8, 64, 1024)] * 3 + [shape(16, 64, 512), shape(8, 176, 1024), shape(8, 176, 1024),
                   shape(16, 64, 1408), shape(*k_view.shape), shape(*v_view.shape),
                   shape(4, 128), shape(4, 128), shape(4, 128), shape(8, 128), shape(8, 128)],
        in_specs=[anywhere] * 8 + [vmem],
        out_specs=[hbm] * 9 + [vmem] * 5,
        scratch_shapes=[dma((15,))],
        compiler_params=pltpu.CompilerParams(vmem_limit_bytes=9437184),
        cost_estimate=pl.CostEstimate(flops=2 * 10**10, bytes_accessed=5 * 10**7, transcendentals=0),
        name="store",
    )(*held[:9])
    hid = pl.pallas_call(
        finish_kernel,
        out_shape=shape(256, 1024),
        in_specs=[vmem] * 3,
        out_specs=vmem,
        compiler_params=pltpu.CompilerParams(vmem_limit_bytes=9437184),
        name="finish",
    )(held[9], held[10], peer)
    wq, wk, wv, wo, wg, wu, wd, k_out, v_out, bq, bk, bv, ga, gm = outs
    flat = lambda a, n: a.reshape(-1, n)
    return (flat(wq, 1024), bq.reshape(512), flat(wk, 1024), bk.reshape(512), flat(wv, 1024), bv.reshape(512),
            flat(wo, 512), flat(wg, 1024), flat(wu, 1024), flat(wd, 1408), ga.reshape(1024), gm.reshape(1024),
            hid, jnp.transpose(k_out, (3, 0, 1, 2)), jnp.transpose(v_out, (3, 0, 1, 2)))


def solution(mesh):
    row_spec = P(("dp", "tp"), None)
    flat_spec = P(("dp", "tp"))
    cache_spec = P("dp", None, "tp", None)
    in_specs = (row_spec, flat_spec, row_spec, flat_spec, row_spec, flat_spec, row_spec, row_spec, row_spec, row_spec,
                flat_spec, flat_spec, P("dp", None), cache_spec, cache_spec, P("dp"))
    out_specs = (P("tp", None), P("tp"), P("tp", None), P("tp"), P("tp", None), P("tp"), P(None, "tp"), P("tp", None),
                 P("tp", None), P(None, "tp"), P(None), P(None), P("dp", None), cache_spec, cache_spec)
    return jax.shard_map(local_step, mesh=mesh, in_specs=in_specs, out_specs=out_specs, check_vma=False)
```

```python
import jax
import jax.numpy as jnp
import numpy as np
from jax import lax
from jax.experimental import pallas as pl
from jax.experimental.pallas import tpu as pltpu
from jax.sharding import PartitionSpec as P

EPS = 1e-6
THETA = 1000000.0
MESH = pl.DeviceIdType.MESH
F32 = jnp.float32
BF16 = jnp.bfloat16
BY_ROWS = (((1,), (1,)), ((), ()))
NAT = (((1,), (0,)), ((), ()))
GROUP = 8
AHEAD = 3


def dot(lhs, rhs, dims):
    return lax.dot_general(lhs, rhs, dims, preferred_element_type=F32)


HOME_STEPS = (
    (
        ("s", "q0", 0, "c", 0), ("s", "q1", 0, "c", 0), ("s", "q2", 0, "c", 0), ("s", "g0", 0, "c", 0),
        ("s", "g1", 0, "c", 0), ("s", "u0", 0, "c", 0), ("s", "u1", 0, "c", 0), ("s", "o", 0, "c", 0),
        ("s", "d", 0, "c", 0), ("s", "o", "z", "z", 4), ("s", "d", "z", "z", 4), ("s", "q1", 0, "y", 0),
        ("s", "q1", 0, "x", 1),
    ),
    (
        ("s", "o", 0, "y", 2), ("s", "q2", 0, "y", 0), ("s", "o", 0, "x", 1), ("s", "q2", 0, "x", 1),
    ),
    (
        ("w", "o", 4), ("s", "o", 4, "c", 4), ("w", "q0", "c", 0), ("w", "q1", "c", 0), ("w", "q2", "c", 0),
    ),
    (
        ("w", "q1", "t"), ("w", "q1", 1), ("s", "q1", 1, "c", 1), ("s", "q1", "t", "z", 2), ("s", "o", 4, "y", 6),
        ("s", "o", 4, "x", 5), ("w", "q1", 2), ("s", "q1", 2, "c", 2), ("w", "o", 1), ("s", "o", 1, "c", 1),
        ("s", "q0", 0, "y", 0), ("s", "q0", 0, "x", 1), ("w", "q2", "t"), ("s", "q2", "t", "z", 2), ("w", "q2", 1),
        ("s", "q2", 1, "c", 1), ("w", "q2", 2), ("s", "q2", 2, "c", 2), ("s", "g0", 0, "y", 0), ("s", "q1", 2, "x", 3),
        ("w", "o", 5), ("s", "o", 5, "c", 5), ("w", "q0", "t"), ("s", "q0", "t", "z", 2), ("w", "o", 2),
        ("s", "o", 2, "c", 2), ("w", "q0", 2), ("s", "q0", 2, "c", 2),
    ),
    (
        ("w", "o", 6), ("s", "o", 6, "c", 6), ("w", "q0", 1), ("s", "q0", 1, "c", 1), ("s", "q0", 1, "y", 1),
        ("s", "q2", 2, "x", 3),
    ),
    (
        ("s", "q0", 2, "x", 3), ("w", "q0", "c", 1), ("w", "q1", "c", 1), ("w", "q2", "c", 1),
    ),
    (
        ("w", "g0", 2), ("s", "g0", 2, "c", 2), ("w", "q1", 3), ("s", "q1", 3, "c", 3), ("w", "g0", "t"),
        ("s", "g0", "t", "z", 2), ("s", "q1", 3, "y", 3), ("w", "q0", "c", 2), ("w", "q1", "c", 2), ("w", "q2", "c", 2),
    ),
    (
        ("w", "q2", 3), ("s", "q2", 3, "c", 3), ("s", "o", 1, "y", 3), ("s", "g0", 0, "x", 1), ("w", "d", 4),
        ("s", "d", 4, "c", 4), ("s", "o", 5, "y", 7), ("w", "u0", "t"), ("s", "u0", "t", "z", 2),
        ("s", "u0", 0, "y", 0), ("s", "o", 6, "x", 7), ("w", "q0", 3), ("s", "q0", 3, "c", 3),
    ),
    (
        ("w", "u0", 2), ("s", "u0", 2, "c", 2), ("s", "u0", 0, "x", 1), ("w", "q0", "c", 3), ("w", "q1", "c", 3),
        ("w", "q2", "c", 3),
    ),
    (
        ("w", "u1", "t"), ("s", "u1", "t", "z", 2), ("s", "u1", 0, "y", 0), ("w", "g0", 1), ("s", "g0", 1, "c", 1),
        ("s", "u1", 0, "x", 1), ("w", "o", 7), ("s", "o", 7, "c", 7), ("w", "u1", 2), ("s", "u1", 2, "c", 2),
        ("w", "g1", "t"), ("s", "g1", "t", "z", 2), ("s", "g1", 0, "y", 0), ("w", "o", 3), ("s", "o", 3, "c", 3),
        ("s", "g1", 0, "x", 1), ("w", "u0", 1), ("s", "u0", 1, "c", 1), ("w", "g1", 2), ("s", "g1", 2, "c", 2),
        ("w", "o", "c", 0), ("w", "o", "c", 1), ("w", "o", "c", 2), ("w", "o", "c", 3), ("w", "o", "c", 4),
        ("w", "o", "c", 5), ("w", "o", "c", 6), ("w", "o", "c", 7),
    ),
    (
        ("s", "d", 0, "y", 2), ("w", "d", 2), ("s", "d", 2, "c", 2), ("s", "d", 0, "x", 1), ("w", "u1", 1),
        ("s", "u1", 1, "c", 1), ("s", "d", 4, "y", 6), ("w", "d", 6), ("s", "d", 6, "c", 6), ("s", "d", 4, "x", 5),
        ("w", "g1", 1), ("s", "g1", 1, "c", 1), ("s", "u0", 1, "y", 1), ("w", "g0", 3), ("s", "g0", 3, "c", 3),
        ("s", "g1", 2, "x", 3), ("w", "d", 1), ("s", "d", 1, "c", 1),
    ),
    (
        ("s", "d", 1, "y", 3),
    ),
    (
        ("w", "u0", 3), ("s", "u0", 3, "c", 3), ("w", "g0", "c", 0), ("w", "g1", "c", 0), ("w", "u0", "c", 0),
        ("w", "u1", "c", 0),
    ),
    (
        ("w", "d", 5), ("s", "d", 5, "c", 5), ("s", "d", 6, "x", 7),
    ),
    (
        ("w", "g0", "c", 1), ("w", "g1", "c", 1), ("w", "u0", "c", 1), ("w", "u1", "c", 1),
    ),
    (),
    (
        ("w", "g0", "c", 2), ("w", "g1", "c", 2), ("w", "u0", "c", 2), ("w", "u1", "c", 2),
    ),
    (
        ("w", "u1", 3), ("s", "u1", 3, "c", 3), ("w", "g1", 3), ("s", "g1", 3, "c", 3),
    ),
    (
        ("w", "g0", "c", 3), ("w", "g1", "c", 3), ("w", "u0", "c", 3), ("w", "u1", "c", 3),
    ),
    (),
    (
        ("w", "d", "c", 0), ("w", "d", "c", 4),
    ),
    (
        ("w", "d", 3), ("s", "d", 3, "c", 3),
    ),
    (
        ("w", "d", 7), ("s", "d", 7, "c", 7), ("w", "d", "c", 1), ("w", "d", "c", 5),
    ),
    (),
    (
        ("w", "d", "c", 2), ("w", "d", "c", 6),
    ),
    (),
    (
        ("w", "d", "c", 3), ("w", "d", "c", 7),
    ),
    (),
)
HOME_BLOCKS = {
    "attend": ((0, 0), (0, 1), (2, 0), (1, 0), (1, 1), (2, 1), (3, 0), (3, 1)),
    "gated": ((0, 0), (0, 1), (1, 0), (1, 1), (2, 0), (2, 1), (3, 0), (3, 1)),
    "down": ((0, 0), (0, 1), (1, 0), (1, 1), (2, 0), (2, 1), (3, 0), (3, 1)),
}
AWAY_STEPS = (
    (
        ("s", "o", 0, "c", 0), ("s", "d", 0, "c", 0), ("s", "o", "z", "z", 4), ("s", "q1", "own", "z", 2),
        ("s", "q1", "own", "y", "t"), ("s", "o", 0, "x", 1), ("s", "d", 0, "x", 1),
    ),
    (
        ("s", "q2", "own", "z", 2), ("s", "q2", "own", "y", "t"), ("w", "o", 1), ("s", "o", 1, "c", 1), ("w", "o", 4),
        ("s", "o", 4, "c", 4), ("s", "o", 4, "x", 5), ("s", "q0", "own", "y", "t"), ("w", "q1", 0),
        ("s", "q1", 0, "c", 0), ("s", "q1", 0, "x", 1), ("s", "q0", "own", "z", 2), ("w", "o", 2),
        ("s", "o", 2, "c", 2), ("s", "o", 0, "y", 2), ("w", "d", 1), ("s", "d", 1, "c", 1), ("w", "d", 4),
        ("s", "d", 4, "c", 4), ("s", "d", 4, "x", 5), ("s", "g0", "own", "z", 2), ("s", "o", 4, "y", 6), ("w", "o", 5),
        ("s", "o", 5, "c", 5), ("w", "q2", 0), ("s", "q2", 0, "c", 0), ("s", "g0", "own", "y", "t"), ("w", "o", 6),
        ("s", "o", 6, "c", 6), ("w", "q1", 2), ("s", "q1", 2, "c", 2), ("s", "q2", 0, "x", 1), ("w", "q1", 1),
        ("s", "q1", 1, "c", 1), ("s", "d", "z", "z", 4), ("s", "u0", "own", "y", "t"), ("w", "q0", 0),
        ("s", "q0", 0, "c", 0),
    ),
    (
        ("w", "q2", 2), ("s", "q2", 2, "c", 2), ("s", "q2", 2, "x", 3), ("w", "q0", "c", 0), ("w", "q1", "c", 0),
        ("w", "q2", "c", 0),
    ),
    (
        ("w", "d", 5), ("s", "d", 5, "c", 5), ("w", "q0", 2), ("s", "q0", 2, "c", 2), ("s", "u0", "own", "z", 2),
        ("s", "u1", "own", "y", "t"), ("s", "q0", 2, "x", 3),
    ),
    (
        ("w", "g0", 0), ("s", "g0", 0, "c", 0), ("w", "q2", 1), ("s", "q2", 1, "c", 1), ("w", "q0", "c", 2),
        ("w", "q1", "c", 2), ("w", "q2", "c", 2),
    ),
    (
        ("w", "q0", 1), ("s", "q0", 1, "c", 1), ("s", "u1", "own", "z", 2), ("s", "g1", "own", "y", "t"),
        ("s", "g0", 0, "x", 1),
    ),
    (
        ("w", "q2", 3), ("s", "q2", 3, "c", 3), ("w", "q1", 3), ("s", "q1", 3, "c", 3), ("w", "q0", "c", 1),
        ("w", "q1", "c", 1), ("w", "q2", "c", 1),
    ),
    (
        ("w", "g0", 2), ("s", "g0", 2, "c", 2), ("w", "q0", 3), ("s", "q0", 3, "c", 3), ("w", "o", 3),
        ("s", "o", 3, "c", 3), ("s", "g1", "own", "z", 2), ("s", "o", 1, "y", 3), ("s", "g0", 2, "x", 3),
    ),
    (
        ("w", "o", 7), ("s", "o", 7, "c", 7), ("s", "d", 0, "y", 2), ("w", "q0", "c", 3), ("w", "q1", "c", 3),
        ("w", "q2", "c", 3),
    ),
    (
        ("w", "u0", 2), ("s", "u0", 2, "c", 2), ("w", "g0", 1), ("s", "g0", 1, "c", 1), ("s", "u0", 2, "x", 3),
        ("w", "o", "c", 0), ("w", "o", "c", 1), ("w", "o", "c", 2), ("w", "o", "c", 3), ("w", "o", "c", 4),
        ("w", "o", "c", 5), ("w", "o", "c", 6), ("w", "o", "c", 7),
    ),
    (
        ("w", "u0", 0), ("s", "u0", 0, "c", 0), ("s", "d", 4, "y", 6), ("w", "u1", 2), ("s", "u1", 2, "c", 2),
        ("s", "u1", 2, "x", 3), ("w", "g0", 3), ("s", "g0", 3, "c", 3), ("w", "u1", 0), ("s", "u1", 0, "c", 0),
        ("s", "g0", 3, "y", 3), ("s", "u1", 0, "x", 1), ("w", "g1", 2), ("s", "g1", 2, "c", 2), ("w", "u0", 3),
        ("s", "u0", 3, "c", 3), ("w", "g1", 0), ("s", "g1", 0, "c", 0), ("s", "u0", 3, "y", 3), ("s", "g1", 0, "x", 1),
        ("w", "u1", 3), ("s", "u1", 3, "c", 3), ("w", "d", 2), ("s", "d", 2, "c", 2), ("s", "u1", 3, "y", 3),
        ("s", "g1", 2, "x", 3), ("w", "u1", 1), ("s", "u1", 1, "c", 1), ("w", "d", 6), ("s", "d", 6, "c", 6),
        ("s", "d", 1, "y", 3),
    ),
    (
        ("w", "g1", 1), ("s", "g1", 1, "c", 1), ("s", "d", 6, "x", 7),
    ),
    (
        ("w", "u0", 1), ("s", "u0", 1, "c", 1), ("w", "g0", "c", 0), ("w", "g1", "c", 0), ("w", "u0", "c", 0),
        ("w", "u1", "c", 0),
    ),
    (),
    (),
    (
        ("w", "g1", 3), ("s", "g1", 3, "c", 3), ("w", "g0", "c", 1), ("w", "g1", "c", 1), ("w", "u0", "c", 1),
        ("w", "u1", "c", 1),
    ),
    (
        ("w", "g0", "c", 2), ("w", "g1", "c", 2), ("w", "u0", "c", 2), ("w", "u1", "c", 2),
    ),
    (),
    (
        ("w", "d", 3), ("s", "d", 3, "c", 3), ("w", "g0", "c", 3), ("w", "g1", "c", 3), ("w", "u0", "c", 3),
        ("w", "u1", "c", 3),
    ),
    (),
    (
        ("w", "d", "c", 0), ("w", "d", "c", 4),
    ),
    (
        ("w", "d", 7), ("s", "d", 7, "c", 7),
    ),
    (
        ("w", "d", "c", 1), ("w", "d", "c", 5),
    ),
    (),
    (
        ("w", "d", "c", 2), ("w", "d", "c", 6),
    ),
    (),
    (
        ("w", "d", "c", 3), ("w", "d", "c", 7),
    ),
    (),
)
AWAY_BLOCKS = {
    "attend": ((0, 0), (0, 1), (2, 0), (2, 1), (1, 0), (1, 1), (3, 0), (3, 1)),
    "gated": ((0, 0), (0, 1), (1, 0), (2, 0), (1, 1), (2, 1), (3, 0), (3, 1)),
    "down": ((0, 0), (0, 1), (1, 0), (1, 1), (2, 0), (2, 1), (3, 0), (3, 1)),
}


class Place:
    def __init__(self):
        tp = lax.axis_index("tp")
        dp = lax.axis_index("dp")
        self.z = tp
        self.dp = dp
        self.y = dp // 4
        self.x = (dp // 2) % 2
        self.c = dp % 2
        self.far = lax.rem(self.y + self.z, 2)
        self.device = {
            "x": (tp, dp + 2 - 4 * self.x),
            "y": (tp, dp + 4 - 8 * self.y),
            "c": (tp, dp + 1 - 2 * self.c),
            "z": (1 - tp, dp),
        }

    def at(self, axis, flip):
        here = getattr(self, axis)
        return 1 - here if flip else here

    def row_block(self, k, core=0):
        return (self.at("x", k & 1) * 2 + self.at("c", core)) * 2 + self.at("z", k & 2)

    def col_block(self, k, core=0):
        return (self.at("y", k & 2) * 4 + self.at("x", k & 1) * 2 + self.at("c", core)) * 2 + self.at("z", k & 4)


def remote(src, dst, send, recv, device):
    return pltpu.make_async_remote_copy(
        src_ref=src, dst_ref=dst, send_sem=send, recv_sem=recv, device_id=device, device_id_type=MESH)


class Rows:
    def __init__(self, place, buf, start, own, through, index, sems):
        self.p, self.buf, self.start, self.own, self.through = place, buf, start, own, through
        self.i, (self.send, self.r, self.rc) = index, sems
        self.n = own.shape[0]

    def block(self, k, core=0):
        return self.buf.at[self.p.row_block(k, core), pl.ds(self.start, self.n)]

    def copy(self, k, link, home):
        p = self.p
        slot = {"own": 0, "t": 4}.get(k, k)
        send = self.send.at[self.i, "xyzc".index(link), slot]
        if k == "own" or (home and k == 0):
            src = self.own
        elif k == "t":
            src = self.through
        else:
            src = self.block(k)
        if k == "own" and link == "y":
            dst, recv = self.through, self.r.at[self.i, 4]
        else:
            dst = self.block(0 if k in ("own", "t") else k)
            got = 2 if link == "z" else k ^ 1 if link == "x" else k
            recv = self.rc.at[self.i, k] if link == "c" else self.r.at[self.i, got]
        return remote(src, dst, send, recv, p.device[link])

    def wait(self, k, core):
        if k == "t":
            ref, recv = self.through, self.r.at[self.i, 4]
        else:
            ref, recv = self.block(k, core), (self.rc if core else self.r).at[self.i, k]
        remote(ref, ref, self.send.at[self.i, 0, 0], recv, self.p.device["x"]).wait_recv()

    def local(self):
        @pl.when(self.p.far == 0)
        def _():
            self.buf[self.p.row_block(0), pl.ds(self.start, self.n)] = self.own[...]


class Cols:
    def __init__(self, place, buf, own, index, sems):
        self.p, self.buf, self.own = place, buf, own
        self.n = buf.shape[-1]
        self.i, (self.send, self.r, self.rc) = index, sems

    def block(self, k, core=0):
        return self.buf.at[self.p.col_block(k, core)]

    def half(self, z):
        return self.own.at[:, pl.ds(pl.multiple_of(z * self.n, 128), self.n)]

    def copy(self, k, link, home):
        p = self.p
        if link == "z":
            return remote(self.half(1 - p.z), self.block(0), self.send.at[self.i, 2, 0], self.r.at[self.i, 4], p.device["z"])
        src = self.half(p.z) if k == 0 else self.block(k)
        got = k ^ 1 if link == "x" else k ^ 2
        recv = self.rc.at[self.i, k] if link == "c" else self.r.at[self.i, got]
        return remote(src, self.block(k), self.send.at[self.i, "xyzc".index(link), k], recv, p.device[link])

    def wait(self, k, core):
        ref, recv = self.block(k, core), (self.rc if core else self.r).at[self.i, k]
        remote(ref, ref, self.send.at[self.i, 0, 0], recv, self.p.device["x"]).wait_recv()

    def local(self):
        self.buf[self.p.col_block(0)] = self.own[:, pl.ds(pl.multiple_of(self.p.z * self.n, 128), self.n)]


def layer_kernel(wq_hbm, wk_hbm, wv_hbm, wo_hbm, wg_hbm, wu_hbm, wd_hbm, x_hbm, k_hbm, v_hbm,
                 bq, bk, bv, ga, gm, freq_ref, len_ref,
                 wqkv, wgu, wout, wdn, k_lo, k_hi, v_lo, v_hi, smalls, x1_ref, down,
                 h_ref, sc_ref, o_ref, a_ref, cos_ref, sin_ref, t_q, t_gu, w_q, w_gu, wo, wd, x_ref, small, l_sem,
                 k_sem, v_sem, s_send, s_recv, p_send, p_recv, row_s, row_r, row_c, col_s, col_r, col_c):
    place = Place()
    me = place.dp * 2 + place.z
    row_sem, col_sem = (row_s, row_r, row_c), (col_s, col_r, col_c)
    loads = [(wq_hbm, w_q.at[0]), (wk_hbm, w_q.at[1]), (wv_hbm, w_q.at[2]), (wo_hbm, wo), (wg_hbm, w_gu.at[0]),
             (wu_hbm, w_gu.at[1]), (wd_hbm, wd), (x_hbm, x_ref)]
    loads = [pltpu.make_async_copy(src, dst, l_sem.at[i]) for i, (src, dst) in enumerate(loads)]
    for load in loads:
        load.start()
    chunks = {}
    for i in range(3):
        chunks[f"q{i}"] = Rows(place, wqkv, 64 * i, w_q.at[i], t_q.at[i], i, row_sem)
    for i in range(4):
        ref = w_gu.at[i // 2, pl.ds(88 * (i % 2), 88)]
        chunks["gu"[i // 2] + str(i % 2)] = Rows(place, wgu, 88 * i, ref, t_gu.at[i], 3 + i, row_sem)
    chunks["o"] = Cols(place, wout, wo, 0, col_sem)
    chunks["d"] = Cols(place, wdn, wd, 1, col_sem)
    roles = ((0, HOME_STEPS, HOME_BLOCKS), (1, AWAY_STEPS, AWAY_BLOCKS))
    step = iter(range(len(HOME_STEPS)))

    def go():
        now = next(step)
        for far, steps, _ in roles:
            if steps[now]:
                @pl.when(place.far == far)
                def _(far=far, steps=steps):
                    for action in steps[now]:
                        chunk = chunks[action[1]]
                        if action[0] == "s":
                            chunk.copy(action[2], action[3], far == 0).start()
                        elif action[2] == "c":
                            chunk.wait(action[3], 1)
                        else:
                            chunk.wait(action[2], 0)

    def by_role(kind, i, place_of, swap=False):
        home, away = (place_of(*blocks[kind][i]) for _, _, blocks in roles)
        if swap:
            home, away = away, home
        return home + place.far * (away - home)

    def cache_copy(i):
        head = by_role("attend", i, place.row_block)
        copies = []
        for hbm, lo, hi, sem in ((k_hbm, k_lo, k_hi, k_sem), (v_hbm, v_lo, v_hi, v_sem)):
            copies.append(pltpu.make_async_copy(hbm.at[pl.ds(0, 32), head], lo.at[:, head], sem.at[2 * i]))
            copies.append(pltpu.make_async_copy(hbm.at[pl.ds(32, 32), head], hi.at[:, head], sem.at[2 * i + 1]))
        return copies

    barrier = pltpu.get_barrier_semaphore()
    for i in range(1, 16):
        other = lax.rem(me + i, 16)
        pl.semaphore_signal(barrier, inc=1, device_id=(other % 2, other // 2), device_id_type=MESH)
    for i in range(AHEAD):
        for copy in cache_copy(i):
            copy.start()
    vectors = jnp.concatenate([v[...].astype(F32) for v in (bq, bk, bv, ga, gm)] + [jnp.zeros((3, 64), F32)], axis=0)
    vectors = jnp.concatenate([vectors, vectors], axis=1)
    mine = lax.broadcasted_iota(jnp.int32, (8, 128), 1) // 64 == place.z
    vectors = jnp.where(mine, vectors, 0.0).astype(BF16)
    small[...] = vectors
    smalls[me] = vectors
    for load in loads:
        load.wait()
    pl.semaphore_wait(barrier, 15)

    def small_copy(i):
        other = lax.rem(me + i, 16)
        return remote(small, smalls.at[me], s_send.at[i], s_recv.at[i], (other % 2, other // 2))

    go()
    for i in range(1, 16):
        small_copy(i).start()

    for chunk in chunks.values():
        chunk.local()
    angles = freq_ref[...] * len_ref[...].astype(F32)
    cos_ref[...] = jnp.cos(angles)
    sin_ref[...] = jnp.sin(angles)
    for i in range(1, 16):
        small_copy(i).wait_recv()

    def gain_row(i):
        pair = smalls[...].astype(F32).reshape(8, 2, 8, 128)
        rows = pair[:, 0, i] + pair[:, 1, i]
        return jnp.concatenate([rows[d:d + 1] for d in range(8)], axis=1)

    def normed(rows, i):
        inv = lax.rsqrt(jnp.mean(rows * rows, axis=-1, keepdims=True) + EPS)
        return (rows * inv * gain_row(i)).astype(BF16)

    h_ref[...] = normed(x_ref[...].astype(F32), 3)

    eye = lax.broadcasted_iota(jnp.int32, (64, 128), 1) % 64 == lax.broadcasted_iota(jnp.int32, (64, 128), 0)

    def bias_column(head, i):
        row = smalls[place.z * 8 + head].astype(F32)[i:i + 1]
        return jnp.sum(jnp.where(eye, row, 0.0), axis=1, keepdims=True)

    def attend(i):
        head = by_role("attend", i, place.row_block)
        res = dot(wqkv[head], h_ref[...], BY_ROWS)
        cos, sin = cos_ref[...], sin_ref[...]

        def rotated(start, b):
            v = (res[start:start + 64] + bias_column(head, b)).astype(BF16).astype(F32)
            lo, hi = v[:32], v[32:]
            return jnp.concatenate([lo * cos - hi * sin, hi * cos + lo * sin], axis=0).astype(BF16)

        q = rotated(0, 0).astype(F32)
        k_new = rotated(64, 1)
        v_new = (res[128:192] + bias_column(head, 2)).astype(BF16)
        lens = len_ref[...].astype(F32)
        for copy in cache_copy(i):
            copy.wait()

        for base, buf in ((0, k_lo), (32, k_hi)):
            def score_group(g, carry, base=base, buf=buf):
                rows = []
                for j in range(GROUP):
                    s = g * GROUP + j
                    kv = jnp.where(lens == (base + s).astype(F32), k_new.astype(F32), buf[s, head].astype(F32))
                    buf[s, head] = kv.astype(BF16)
                    rows.append(jnp.sum(q * kv, axis=0, keepdims=True))
                sc_ref[pl.ds(pl.multiple_of(base + g * GROUP, GROUP), GROUP)] = jnp.concatenate(rows, axis=0)
                return carry

            lax.fori_loop(0, 32 // GROUP, score_group, 0)
        slot = lax.broadcasted_iota(jnp.int32, (64, 256), 0).astype(F32)
        scores = jnp.where(slot <= lens, sc_ref[...] * 0.125, -1e30)
        e = jnp.exp(scores - jnp.max(scores, axis=0, keepdims=True))
        sc_ref[...] = (e / jnp.sum(e, axis=0, keepdims=True)).astype(BF16).astype(F32)

        acc = jnp.zeros((64, 256), F32)
        for base, buf in ((0, v_lo), (32, v_hi)):
            def value_group(g, acc, base=base, buf=buf):
                probs = sc_ref[pl.ds(pl.multiple_of(base + g * GROUP, GROUP), GROUP)]
                for j in range(GROUP):
                    s = g * GROUP + j
                    vv = jnp.where(lens == (base + s).astype(F32), v_new.astype(F32), buf[s, head].astype(F32))
                    buf[s, head] = vv.astype(BF16)
                    acc = acc + probs[j:j + 1] * vv
                return acc

            acc = lax.fori_loop(0, 32 // GROUP, value_group, acc)
        o_ref[pl.ds(pl.multiple_of(head * 64, 64), 64)] = acc.astype(BF16)

    go()
    for i in range(8):
        if i + AHEAD < 8:
            for copy in cache_copy(i + AHEAD):
                copy.start()
        attend(i)
        go()

    o = o_ref[...].T
    part, part_in, h2_ref = down, x1_ref, h_ref
    part[...] = dot(o, wout[...].reshape(1024, 512), BY_ROWS).astype(BF16)
    swap = remote(part, part_in, p_send, p_recv, place.device["z"])
    swap.start()
    go()
    swap.wait_recv()
    swap.wait_send()
    total = (part[...].astype(F32) + part_in[...].astype(F32)).astype(BF16)
    x1 = (x_ref[...].astype(F32) + total.astype(F32)).astype(BF16)
    x1_ref[...] = x1
    h2_ref[...] = normed(x1.astype(F32), 4)
    go()

    for i in range(8):
        block = by_role("gated", i, place.row_block)
        res = dot(wgu[block], h2_ref[...], BY_ROWS).astype(BF16).astype(F32)
        g, u = res[:176], res[176:]
        a_ref[block] = (g / (1.0 + jnp.exp(-g)) * u).astype(BF16)
        go()

    for i in range(8):
        pair = by_role("down", i, lambda k, core: place.col_block(k, core) // 2)
        w = wdn[pl.ds(pair * 2, 2)].reshape(128, 1408)
        cols = pl.ds(pl.multiple_of(pair * 128, 128), 128)
        down[:, cols] = dot(w, a_ref[...].reshape(1408, 256), NAT).T.astype(BF16)
        go()

    for far, steps, _ in roles:
        @pl.when(place.far == far)
        def _(far=far, steps=steps):
            for action in sum(steps, ()):
                if action[0] == "s":
                    chunks[action[1]].copy(action[2], action[3], far == 0).wait_send()

    for i in range(1, 16):
        small_copy(i).wait_send()


def store_kernel(wqkv, wgu, wout, wdn, k_lo, k_hi, v_lo, v_hi, smalls,
                 wq, wk, wv, wo, wg, wu, wd, k_out, v_out, bq, bk, bv, ga, gm, sem):
    pairs = [(src.at[pl.ds(16 * i, 16)], dst.at[pl.ds(base + 16 * i, 16)]) for src, dst, base in (
        (k_lo, k_out, 0), (k_hi, k_out, 32), (v_lo, v_out, 0), (v_hi, v_out, 32)) for i in range(2)]
    pairs += [(wdn, wd), (wgu.at[:, pl.ds(0, 176)], wg), (wgu.at[:, pl.ds(176, 176)], wu),
             (wqkv.at[:, pl.ds(0, 64)], wq), (wqkv.at[:, pl.ds(64, 64)], wk), (wqkv.at[:, pl.ds(128, 64)], wv),
             (wout, wo)]
    copies = [pltpu.make_async_copy(src, dst, sem.at[i]) for i, (src, dst) in enumerate(pairs)]
    for copy in copies:
        copy.start()
    z = lax.axis_index("tp")
    plane = smalls[pl.ds(z * 8, 8)].astype(F32).reshape(4, 2, 8, 128)
    whole = smalls[...].astype(F32).reshape(8, 2, 8, 128)
    for i, ref in enumerate((bq, bk, bv)):
        ref[...] = (plane[:, 0, i] + plane[:, 1, i]).astype(BF16)
    for i, ref in enumerate((ga, gm)):
        ref[...] = (whole[:, 0, 3 + i] + whole[:, 1, 3 + i]).astype(BF16)
    for copy in copies:
        copy.wait()


def finish_kernel(x1, mine, peer, hid):
    total = (mine[...].astype(F32) + peer[...].astype(F32)).astype(BF16)
    hid[...] = (x1[...].astype(F32) + total.astype(F32)).astype(BF16)


def local_step(w_query, b_query, w_key, b_key, w_value, b_value, w_out, w_gate, w_up, w_down, gain_attn, gain_mlp,
               hidden, k_cache, v_cache, lengths):
    freq = np.tile((1.0 / THETA ** (np.arange(0, 64, 2) / 64)).astype(np.float32)[:, None], (1, 256))
    lens = lengths[None, :]
    rows = [v[None, :] for v in (b_query, b_key, b_value, gain_attn, gain_mlp)]
    k_view = jnp.transpose(k_cache, (1, 2, 3, 0))
    v_view = jnp.transpose(v_cache, (1, 2, 3, 0))

    vmem = pl.BlockSpec(memory_space=pltpu.VMEM)
    hbm = pl.BlockSpec(memory_space=pltpu.HBM)
    anywhere = pl.BlockSpec(memory_space=pl.ANY)
    dma = pltpu.SemaphoreType.DMA
    shapes = [(8, 192, 1024), (8, 352, 1024), (16, 64, 512), (16, 64, 1408), *[(32, 8, 64, 256)] * 4,
              (16, 8, 128), (256, 1024), (256, 1024)]
    held = pl.pallas_call(
        layer_kernel,
        out_shape=[pltpu.VMEM(s, BF16) for s in shapes],
        in_specs=[hbm] * 10 + [vmem] * 7,
        out_specs=[vmem] * 11,
        scratch_shapes=[
            pltpu.VMEM((256, 1024), BF16),
            pltpu.VMEM((64, 256), F32),
            pltpu.VMEM((512, 256), BF16),
            pltpu.VMEM((8, 176, 256), BF16),
            pltpu.VMEM((32, 256), F32),
            pltpu.VMEM((32, 256), F32),
            pltpu.VMEM((3, 64, 1024), BF16),
            pltpu.VMEM((4, 88, 1024), BF16),
            pltpu.VMEM((3, 64, 1024), BF16),
            pltpu.VMEM((2, 176, 1024), BF16),
            pltpu.VMEM((64, 1024), BF16),
            pltpu.VMEM((64, 2816), BF16),
            pltpu.VMEM((256, 1024), BF16),
            pltpu.VMEM((8, 128), BF16),
            dma((8,)),
            dma((16,)), dma((16,)), dma((16,)), dma((16,)), dma, dma,
            dma((7, 4, 5)), dma((7, 5)), dma((7, 4)), dma((2, 4, 8)), dma((2, 8)), dma((2, 8)),
        ],
        compiler_params=pltpu.CompilerParams(collective_id=0, has_side_effects=True, vmem_limit_bytes=9437184),
        name="layer",
    )(w_query, w_key, w_value, w_out, w_gate, w_up, w_down, hidden, k_view, v_view, *rows, freq, lens)

    def shape(*dims):
        return jax.ShapeDtypeStruct(dims, BF16)

    peer = lax.ppermute(held[10], "tp", [(0, 1), (1, 0)])
    outs = pl.pallas_call(
        store_kernel,
        out_shape=[shape(8, 64, 1024)] * 3 + [shape(16, 64, 512), shape(8, 176, 1024), shape(8, 176, 1024),
                   shape(16, 64, 1408), shape(*k_view.shape), shape(*v_view.shape),
                   shape(4, 128), shape(4, 128), shape(4, 128), shape(8, 128), shape(8, 128)],
        in_specs=[anywhere] * 8 + [vmem],
        out_specs=[hbm] * 9 + [vmem] * 5,
        scratch_shapes=[dma((15,))],
        compiler_params=pltpu.CompilerParams(vmem_limit_bytes=9437184),
        cost_estimate=pl.CostEstimate(flops=2 * 10**10, bytes_accessed=5 * 10**7, transcendentals=0),
        name="store",
    )(*held[:9])
    hid = pl.pallas_call(
        finish_kernel,
        out_shape=shape(256, 1024),
        in_specs=[vmem] * 3,
        out_specs=vmem,
        compiler_params=pltpu.CompilerParams(vmem_limit_bytes=9437184),
        name="finish",
    )(held[9], held[10], peer)
    wq, wk, wv, wo, wg, wu, wd, k_out, v_out, bq, bk, bv, ga, gm = outs
    flat = lambda a, n: a.reshape(-1, n)
    return (flat(wq, 1024), bq.reshape(512), flat(wk, 1024), bk.reshape(512), flat(wv, 1024), bv.reshape(512),
            flat(wo, 512), flat(wg, 1024), flat(wu, 1024), flat(wd, 1408), ga.reshape(1024), gm.reshape(1024),
            hid, jnp.transpose(k_out, (3, 0, 1, 2)), jnp.transpose(v_out, (3, 0, 1, 2)))


def solution(mesh):
    row_spec = P(("dp", "tp"), None)
    flat_spec = P(("dp", "tp"))
    cache_spec = P("dp", None, "tp", None)
    in_specs = (row_spec, flat_spec, row_spec, flat_spec, row_spec, flat_spec, row_spec, row_spec, row_spec, row_spec,
                flat_spec, flat_spec, P("dp", None), cache_spec, cache_spec, P("dp"))
    out_specs = (P("tp", None), P("tp"), P("tp", None), P("tp"), P("tp", None), P("tp"), P(None, "tp"), P("tp", None),
                 P("tp", None), P(None, "tp"), P(None), P(None), P("dp", None), cache_spec, cache_spec)
    return jax.shard_map(local_step, mesh=mesh, in_specs=in_specs, out_specs=out_specs, check_vma=False)
```

```python
import jax
import jax.numpy as jnp
import numpy as np
from jax import lax
from jax.experimental import pallas as pl
from jax.experimental.pallas import tpu as pltpu
from jax.sharding import PartitionSpec as P

EPS = 1e-6
THETA = 1000000.0
MESH = pl.DeviceIdType.MESH
F32 = jnp.float32
BF16 = jnp.bfloat16
BY_ROWS = (((1,), (1,)), ((), ()))
NAT = (((1,), (0,)), ((), ()))
GROUP = 8
AHEAD = 3


def dot(lhs, rhs, dims):
    return lax.dot_general(lhs, rhs, dims, preferred_element_type=F32)


HOME_STEPS = (
    (
        ("s", "q1", 0, "y", 0), ("s", "q1", 0, "x", 1), ("s", "q2", 0, "y", 0), ("s", "q2", 0, "x", 1),
        ("s", "q0", 0, "y", 0), ("s", "q0", 0, "x", 1), ("s", "q0", 0, "c", 0), ("s", "q1", 0, "c", 0),
        ("s", "q2", 0, "c", 0), ("s", "g0", 0, "c", 0), ("s", "g1", 0, "c", 0), ("s", "u0", 0, "c", 0),
        ("s", "u1", 0, "c", 0), ("s", "o", 0, "c", 0), ("s", "d", 0, "c", 0), ("s", "o", "z", "z", 4),
        ("s", "d", "z", "z", 4),
    ),
    (
        ("s", "o", 0, "y", 2), ("s", "o", 0, "x", 1),
    ),
    (
        ("w", "o", 4), ("s", "o", 4, "c", 4), ("w", "q0", "c", 0), ("w", "q1", "c", 0), ("w", "q2", "c", 0),
    ),
    (
        ("w", "q1", "t"), ("w", "q1", 1), ("s", "q1", 1, "c", 1), ("s", "q1", "t", "z", 2), ("s", "o", 4, "y", 6),
        ("s", "o", 4, "x", 5), ("w", "q1", 2), ("s", "q1", 2, "c", 2), ("w", "o", 1), ("s", "o", 1, "c", 1),
        ("w", "q2", "t"), ("s", "q2", "t", "z", 2), ("w", "q2", 1), ("s", "q2", 1, "c", 1), ("w", "q2", 2),
        ("s", "q2", 2, "c", 2), ("s", "g0", 0, "y", 0), ("s", "q1", 2, "x", 3), ("w", "o", 5), ("s", "o", 5, "c", 5),
        ("w", "q0", "t"), ("s", "q0", "t", "z", 2), ("w", "o", 2), ("s", "o", 2, "c", 2), ("w", "q0", 2),
        ("s", "q0", 2, "c", 2),
    ),
    (
        ("w", "o", 6), ("s", "o", 6, "c", 6), ("w", "q0", 1), ("s", "q0", 1, "c", 1), ("s", "q0", 1, "y", 1),
        ("s", "q2", 2, "x", 3),
    ),
    (
        ("s", "q0", 2, "x", 3), ("w", "q0", "c", 1), ("w", "q1", "c", 1), ("w", "q2", "c", 1),
    ),
    (
        ("w", "g0", 2), ("s", "g0", 2, "c", 2), ("w", "q1", 3), ("s", "q1", 3, "c", 3), ("w", "g0", "t"),
        ("s", "g0", "t", "z", 2), ("s", "q1", 3, "y", 3), ("w", "q0", "c", 2), ("w", "q1", "c", 2), ("w", "q2", "c", 2),
    ),
    (
        ("w", "q2", 3), ("s", "q2", 3, "c", 3), ("s", "o", 1, "y", 3), ("s", "g0", 0, "x", 1), ("w", "d", 4),
        ("s", "d", 4, "c", 4), ("s", "o", 5, "y", 7), ("w", "u0", "t"), ("s", "u0", "t", "z", 2),
        ("s", "u0", 0, "y", 0), ("s", "o", 6, "x", 7), ("w", "q0", 3), ("s", "q0", 3, "c", 3),
    ),
    (
        ("w", "u0", 2), ("s", "u0", 2, "c", 2), ("s", "u0", 0, "x", 1), ("w", "q0", "c", 3), ("w", "q1", "c", 3),
        ("w", "q2", "c", 3),
    ),
    (
        ("w", "u1", "t"), ("s", "u1", "t", "z", 2), ("s", "u1", 0, "y", 0), ("w", "g0", 1), ("s", "g0", 1, "c", 1),
        ("s", "u1", 0, "x", 1), ("w", "o", 7), ("s", "o", 7, "c", 7), ("w", "u1", 2), ("s", "u1", 2, "c", 2),
        ("w", "g1", "t"), ("s", "g1", "t", "z", 2), ("s", "g1", 0, "y", 0), ("w", "o", 3), ("s", "o", 3, "c", 3),
        ("s", "g1", 0, "x", 1), ("w", "u0", 1), ("s", "u0", 1, "c", 1), ("w", "g1", 2), ("s", "g1", 2, "c", 2),
        ("w", "o", "c", 0), ("w", "o", "c", 1), ("w", "o", "c", 2), ("w", "o", "c", 3), ("w", "o", "c", 4),
        ("w", "o", "c", 5), ("w", "o", "c", 6), ("w", "o", "c", 7),
    ),
    (
        ("s", "d", 0, "y", 2), ("w", "d", 2), ("s", "d", 2, "c", 2), ("s", "d", 0, "x", 1), ("w", "u1", 1),
        ("s", "u1", 1, "c", 1), ("s", "d", 4, "y", 6), ("w", "d", 6), ("s", "d", 6, "c", 6), ("s", "d", 4, "x", 5),
        ("w", "g1", 1), ("s", "g1", 1, "c", 1), ("s", "u0", 1, "y", 1), ("w", "g0", 3), ("s", "g0", 3, "c", 3),
        ("s", "g1", 2, "x", 3), ("w", "d", 1), ("s", "d", 1, "c", 1),
    ),
    (
        ("s", "d", 1, "y", 3),
    ),
    (
        ("w", "u0", 3), ("s", "u0", 3, "c", 3), ("w", "g0", "c", 0), ("w", "g1", "c", 0), ("w", "u0", "c", 0),
        ("w", "u1", "c", 0),
    ),
    (
        ("w", "d", 5), ("s", "d", 5, "c", 5), ("s", "d", 6, "x", 7),
    ),
    (
        ("w", "g0", "c", 1), ("w", "g1", "c", 1), ("w", "u0", "c", 1), ("w", "u1", "c", 1),
    ),
    (),
    (
        ("w", "g0", "c", 2), ("w", "g1", "c", 2), ("w", "u0", "c", 2), ("w", "u1", "c", 2),
    ),
    (
        ("w", "u1", 3), ("s", "u1", 3, "c", 3), ("w", "g1", 3), ("s", "g1", 3, "c", 3),
    ),
    (
        ("w", "g0", "c", 3), ("w", "g1", "c", 3), ("w", "u0", "c", 3), ("w", "u1", "c", 3),
    ),
    (),
    (
        ("w", "d", "c", 0), ("w", "d", "c", 4),
    ),
    (
        ("w", "d", 3), ("s", "d", 3, "c", 3),
    ),
    (
        ("w", "d", 7), ("s", "d", 7, "c", 7), ("w", "d", "c", 1), ("w", "d", "c", 5),
    ),
    (),
    (
        ("w", "d", "c", 2), ("w", "d", "c", 6),
    ),
    (),
    (
        ("w", "d", "c", 3), ("w", "d", "c", 7),
    ),
    (),
)
HOME_BLOCKS = {
    "attend": ((0, 0), (0, 1), (2, 0), (1, 0), (1, 1), (2, 1), (3, 0), (3, 1)),
    "gated": ((0, 0), (0, 1), (1, 0), (1, 1), (2, 0), (2, 1), (3, 0), (3, 1)),
    "down": ((0, 0), (0, 1), (1, 0), (1, 1), (2, 0), (2, 1), (3, 0), (3, 1)),
}
AWAY_STEPS = (
    (
        ("s", "q1", "own", "z", 2), ("s", "q1", "own", "y", "t"), ("s", "q2", "own", "z", 2),
        ("s", "q2", "own", "y", "t"), ("s", "q0", "own", "y", "t"), ("s", "q0", "own", "z", 2), ("s", "o", 0, "c", 0),
        ("s", "d", 0, "c", 0), ("s", "o", "z", "z", 4), ("s", "o", 0, "x", 1), ("s", "d", 0, "x", 1),
    ),
    (
        ("w", "o", 1), ("s", "o", 1, "c", 1), ("w", "o", 4), ("s", "o", 4, "c", 4), ("s", "o", 4, "x", 5),
        ("w", "q1", 0), ("s", "q1", 0, "c", 0), ("s", "q1", 0, "x", 1), ("w", "o", 2), ("s", "o", 2, "c", 2),
        ("s", "o", 0, "y", 2), ("w", "d", 1), ("s", "d", 1, "c", 1), ("w", "d", 4), ("s", "d", 4, "c", 4),
        ("s", "d", 4, "x", 5), ("s", "g0", "own", "z", 2), ("s", "o", 4, "y", 6), ("w", "o", 5), ("s", "o", 5, "c", 5),
        ("w", "q2", 0), ("s", "q2", 0, "c", 0), ("s", "g0", "own", "y", "t"), ("w", "o", 6), ("s", "o", 6, "c", 6),
        ("w", "q1", 2), ("s", "q1", 2, "c", 2), ("s", "q2", 0, "x", 1), ("w", "q1", 1), ("s", "q1", 1, "c", 1),
        ("s", "d", "z", "z", 4), ("s", "u0", "own", "y", "t"), ("w", "q0", 0), ("s", "q0", 0, "c", 0),
    ),
    (
        ("w", "q2", 2), ("s", "q2", 2, "c", 2), ("s", "q2", 2, "x", 3), ("w", "q0", "c", 0), ("w", "q1", "c", 0),
        ("w", "q2", "c", 0),
    ),
    (
        ("w", "d", 5), ("s", "d", 5, "c", 5), ("w", "q0", 2), ("s", "q0", 2, "c", 2), ("s", "u0", "own", "z", 2),
        ("s", "u1", "own", "y", "t"), ("s", "q0", 2, "x", 3),
    ),
    (
        ("w", "g0", 0), ("s", "g0", 0, "c", 0), ("w", "q2", 1), ("s", "q2", 1, "c", 1), ("w", "q0", "c", 2),
        ("w", "q1", "c", 2), ("w", "q2", "c", 2),
    ),
    (
        ("w", "q0", 1), ("s", "q0", 1, "c", 1), ("s", "u1", "own", "z", 2), ("s", "g1", "own", "y", "t"),
        ("s", "g0", 0, "x", 1),
    ),
    (
        ("w", "q2", 3), ("s", "q2", 3, "c", 3), ("w", "q1", 3), ("s", "q1", 3, "c", 3), ("w", "q0", "c", 1),
        ("w", "q1", "c", 1), ("w", "q2", "c", 1),
    ),
    (
        ("w", "g0", 2), ("s", "g0", 2, "c", 2), ("w", "q0", 3), ("s", "q0", 3, "c", 3), ("w", "o", 3),
        ("s", "o", 3, "c", 3), ("s", "g1", "own", "z", 2), ("s", "o", 1, "y", 3), ("s", "g0", 2, "x", 3),
    ),
    (
        ("w", "o", 7), ("s", "o", 7, "c", 7), ("s", "d", 0, "y", 2), ("w", "q0", "c", 3), ("w", "q1", "c", 3),
        ("w", "q2", "c", 3),
    ),
    (
        ("w", "u0", 2), ("s", "u0", 2, "c", 2), ("w", "g0", 1), ("s", "g0", 1, "c", 1), ("s", "u0", 2, "x", 3),
        ("w", "o", "c", 0), ("w", "o", "c", 1), ("w", "o", "c", 2), ("w", "o", "c", 3), ("w", "o", "c", 4),
        ("w", "o", "c", 5), ("w", "o", "c", 6), ("w", "o", "c", 7),
    ),
    (
        ("w", "u0", 0), ("s", "u0", 0, "c", 0), ("s", "d", 4, "y", 6), ("w", "u1", 2), ("s", "u1", 2, "c", 2),
        ("s", "u1", 2, "x", 3), ("w", "g0", 3), ("s", "g0", 3, "c", 3), ("w", "u1", 0), ("s", "u1", 0, "c", 0),
        ("s", "g0", 3, "y", 3), ("s", "u1", 0, "x", 1), ("w", "g1", 2), ("s", "g1", 2, "c", 2), ("w", "u0", 3),
        ("s", "u0", 3, "c", 3), ("w", "g1", 0), ("s", "g1", 0, "c", 0), ("s", "u0", 3, "y", 3), ("s", "g1", 0, "x", 1),
        ("w", "u1", 3), ("s", "u1", 3, "c", 3), ("w", "d", 2), ("s", "d", 2, "c", 2), ("s", "u1", 3, "y", 3),
        ("s", "g1", 2, "x", 3), ("w", "u1", 1), ("s", "u1", 1, "c", 1), ("w", "d", 6), ("s", "d", 6, "c", 6),
        ("s", "d", 1, "y", 3),
    ),
    (
        ("w", "g1", 1), ("s", "g1", 1, "c", 1), ("s", "d", 6, "x", 7),
    ),
    (
        ("w", "u0", 1), ("s", "u0", 1, "c", 1), ("w", "g0", "c", 0), ("w", "g1", "c", 0), ("w", "u0", "c", 0),
        ("w", "u1", "c", 0),
    ),
    (),
    (),
    (
        ("w", "g1", 3), ("s", "g1", 3, "c", 3), ("w", "g0", "c", 1), ("w", "g1", "c", 1), ("w", "u0", "c", 1),
        ("w", "u1", "c", 1),
    ),
    (
        ("w", "g0", "c", 2), ("w", "g1", "c", 2), ("w", "u0", "c", 2), ("w", "u1", "c", 2),
    ),
    (),
    (
        ("w", "d", 3), ("s", "d", 3, "c", 3), ("w", "g0", "c", 3), ("w", "g1", "c", 3), ("w", "u0", "c", 3),
        ("w", "u1", "c", 3),
    ),
    (),
    (
        ("w", "d", "c", 0), ("w", "d", "c", 4),
    ),
    (
        ("w", "d", 7), ("s", "d", 7, "c", 7),
    ),
    (
        ("w", "d", "c", 1), ("w", "d", "c", 5),
    ),
    (),
    (
        ("w", "d", "c", 2), ("w", "d", "c", 6),
    ),
    (),
    (
        ("w", "d", "c", 3), ("w", "d", "c", 7),
    ),
    (),
)
AWAY_BLOCKS = {
    "attend": ((0, 0), (0, 1), (2, 0), (2, 1), (1, 0), (1, 1), (3, 0), (3, 1)),
    "gated": ((0, 0), (0, 1), (1, 0), (2, 0), (1, 1), (2, 1), (3, 0), (3, 1)),
    "down": ((0, 0), (0, 1), (1, 0), (1, 1), (2, 0), (2, 1), (3, 0), (3, 1)),
}


class Place:
    def __init__(self):
        tp = lax.axis_index("tp")
        dp = lax.axis_index("dp")
        self.z = tp
        self.dp = dp
        self.y = dp // 4
        self.x = (dp // 2) % 2
        self.c = dp % 2
        self.far = lax.rem(self.y + self.z, 2)
        self.device = {
            "x": (tp, dp + 2 - 4 * self.x),
            "y": (tp, dp + 4 - 8 * self.y),
            "c": (tp, dp + 1 - 2 * self.c),
            "z": (1 - tp, dp),
        }

    def at(self, axis, flip):
        here = getattr(self, axis)
        return 1 - here if flip else here

    def row_block(self, k, core=0):
        return (self.at("x", k & 1) * 2 + self.at("c", core)) * 2 + self.at("z", k & 2)

    def col_block(self, k, core=0):
        return (self.at("y", k & 2) * 4 + self.at("x", k & 1) * 2 + self.at("c", core)) * 2 + self.at("z", k & 4)


def remote(src, dst, send, recv, device):
    return pltpu.make_async_remote_copy(
        src_ref=src, dst_ref=dst, send_sem=send, recv_sem=recv, device_id=device, device_id_type=MESH)


class Rows:
    def __init__(self, place, buf, start, own, through, index, sems):
        self.p, self.buf, self.start, self.own, self.through = place, buf, start, own, through
        self.i, (self.send, self.r, self.rc) = index, sems
        self.n = own.shape[0]

    def block(self, k, core=0):
        return self.buf.at[self.p.row_block(k, core), pl.ds(self.start, self.n)]

    def copy(self, k, link, home):
        p = self.p
        slot = {"own": 0, "t": 4}.get(k, k)
        send = self.send.at[self.i, "xyzc".index(link), slot]
        if k == "own" or (home and k == 0):
            src = self.own
        elif k == "t":
            src = self.through
        else:
            src = self.block(k)
        if k == "own" and link == "y":
            dst, recv = self.through, self.r.at[self.i, 4]
        else:
            dst = self.block(0 if k in ("own", "t") else k)
            got = 2 if link == "z" else k ^ 1 if link == "x" else k
            recv = self.rc.at[self.i, k] if link == "c" else self.r.at[self.i, got]
        return remote(src, dst, send, recv, p.device[link])

    def wait(self, k, core):
        if k == "t":
            ref, recv = self.through, self.r.at[self.i, 4]
        else:
            ref, recv = self.block(k, core), (self.rc if core else self.r).at[self.i, k]
        remote(ref, ref, self.send.at[self.i, 0, 0], recv, self.p.device["x"]).wait_recv()

    def local(self):
        @pl.when(self.p.far == 0)
        def _():
            self.buf[self.p.row_block(0), pl.ds(self.start, self.n)] = self.own[...]


class Cols:
    def __init__(self, place, buf, own, index, sems):
        self.p, self.buf, self.own = place, buf, own
        self.n = buf.shape[-1]
        self.i, (self.send, self.r, self.rc) = index, sems

    def block(self, k, core=0):
        return self.buf.at[self.p.col_block(k, core)]

    def half(self, z):
        return self.own.at[:, pl.ds(pl.multiple_of(z * self.n, 128), self.n)]

    def copy(self, k, link, home):
        p = self.p
        if link == "z":
            return remote(self.half(1 - p.z), self.block(0), self.send.at[self.i, 2, 0], self.r.at[self.i, 4], p.device["z"])
        src = self.half(p.z) if k == 0 else self.block(k)
        got = k ^ 1 if link == "x" else k ^ 2
        recv = self.rc.at[self.i, k] if link == "c" else self.r.at[self.i, got]
        return remote(src, self.block(k), self.send.at[self.i, "xyzc".index(link), k], recv, p.device[link])

    def wait(self, k, core):
        ref, recv = self.block(k, core), (self.rc if core else self.r).at[self.i, k]
        remote(ref, ref, self.send.at[self.i, 0, 0], recv, self.p.device["x"]).wait_recv()

    def local(self):
        self.buf[self.p.col_block(0)] = self.own[:, pl.ds(pl.multiple_of(self.p.z * self.n, 128), self.n)]


def layer_kernel(wq_hbm, wk_hbm, wv_hbm, wo_hbm, wg_hbm, wu_hbm, wd_hbm, x_hbm, k_hbm, v_hbm,
                 bq, bk, bv, ga, gm, freq_ref, len_ref,
                 wqkv, wgu, wout, wdn, k_lo, k_hi, v_lo, v_hi, smalls, x1_ref, down,
                 h_ref, sc_ref, o_ref, a_ref, cos_ref, sin_ref, t_q, t_gu, w_q, w_gu, wo, wd, x_ref, small, l_sem,
                 k_sem, v_sem, s_send, s_recv, p_send, p_recv, row_s, row_r, row_c, col_s, col_r, col_c):
    place = Place()
    me = place.dp * 2 + place.z
    row_sem, col_sem = (row_s, row_r, row_c), (col_s, col_r, col_c)
    loads = [(wq_hbm, w_q.at[0]), (wk_hbm, w_q.at[1]), (wv_hbm, w_q.at[2]), (wo_hbm, wo), (wg_hbm, w_gu.at[0]),
             (wu_hbm, w_gu.at[1]), (wd_hbm, wd), (x_hbm, x_ref)]
    loads = [pltpu.make_async_copy(src, dst, l_sem.at[i]) for i, (src, dst) in enumerate(loads)]
    for load in loads:
        load.start()
    chunks = {}
    for i in range(3):
        chunks[f"q{i}"] = Rows(place, wqkv, 64 * i, w_q.at[i], t_q.at[i], i, row_sem)
    for i in range(4):
        ref = w_gu.at[i // 2, pl.ds(88 * (i % 2), 88)]
        chunks["gu"[i // 2] + str(i % 2)] = Rows(place, wgu, 88 * i, ref, t_gu.at[i], 3 + i, row_sem)
    chunks["o"] = Cols(place, wout, wo, 0, col_sem)
    chunks["d"] = Cols(place, wdn, wd, 1, col_sem)
    roles = ((0, HOME_STEPS, HOME_BLOCKS), (1, AWAY_STEPS, AWAY_BLOCKS))
    step = iter(range(len(HOME_STEPS)))

    def go():
        now = next(step)
        for far, steps, _ in roles:
            if steps[now]:
                @pl.when(place.far == far)
                def _(far=far, steps=steps):
                    for action in steps[now]:
                        chunk = chunks[action[1]]
                        if action[0] == "s":
                            chunk.copy(action[2], action[3], far == 0).start()
                        elif action[2] == "c":
                            chunk.wait(action[3], 1)
                        else:
                            chunk.wait(action[2], 0)

    def by_role(kind, i, place_of, swap=False):
        home, away = (place_of(*blocks[kind][i]) for _, _, blocks in roles)
        if swap:
            home, away = away, home
        return home + place.far * (away - home)

    def cache_copy(i):
        head = by_role("attend", i, place.row_block)
        copies = []
        for hbm, lo, hi, sem in ((k_hbm, k_lo, k_hi, k_sem), (v_hbm, v_lo, v_hi, v_sem)):
            copies.append(pltpu.make_async_copy(hbm.at[pl.ds(0, 32), head], lo.at[:, head], sem.at[2 * i]))
            copies.append(pltpu.make_async_copy(hbm.at[pl.ds(32, 32), head], hi.at[:, head], sem.at[2 * i + 1]))
        return copies

    barrier = pltpu.get_barrier_semaphore()
    for i in range(1, 16):
        other = lax.rem(me + i, 16)
        pl.semaphore_signal(barrier, inc=1, device_id=(other % 2, other // 2), device_id_type=MESH)
    for i in range(AHEAD):
        for copy in cache_copy(i):
            copy.start()
    vectors = jnp.concatenate([v[...].astype(F32) for v in (bq, bk, bv, ga, gm)] + [jnp.zeros((3, 64), F32)], axis=0)
    vectors = jnp.concatenate([vectors, vectors], axis=1)
    mine = lax.broadcasted_iota(jnp.int32, (8, 128), 1) // 64 == place.z
    vectors = jnp.where(mine, vectors, 0.0).astype(BF16)
    small[...] = vectors
    smalls[me] = vectors
    for load in loads:
        load.wait()
    pl.semaphore_wait(barrier, 15)

    def small_copy(i):
        other = lax.rem(me + i, 16)
        return remote(small, smalls.at[me], s_send.at[i], s_recv.at[i], (other % 2, other // 2))

    for i in range(1, 16):
        small_copy(i).start()
    go()

    for chunk in chunks.values():
        chunk.local()
    angles = freq_ref[...] * len_ref[...].astype(F32)
    cos_ref[...] = jnp.cos(angles)
    sin_ref[...] = jnp.sin(angles)
    for i in range(1, 16):
        small_copy(i).wait_recv()

    def gain_row(i):
        pair = smalls[...].astype(F32).reshape(8, 2, 8, 128)
        rows = pair[:, 0, i] + pair[:, 1, i]
        return jnp.concatenate([rows[d:d + 1] for d in range(8)], axis=1)

    def normed(rows, i):
        inv = lax.rsqrt(jnp.mean(rows * rows, axis=-1, keepdims=True) + EPS)
        return (rows * inv * gain_row(i)).astype(BF16)

    h_ref[...] = normed(x_ref[...].astype(F32), 3)

    eye = lax.broadcasted_iota(jnp.int32, (64, 128), 1) % 64 == lax.broadcasted_iota(jnp.int32, (64, 128), 0)

    def bias_column(head, i):
        row = smalls[place.z * 8 + head].astype(F32)[i:i + 1]
        return jnp.sum(jnp.where(eye, row, 0.0), axis=1, keepdims=True)

    def attend(i):
        head = by_role("attend", i, place.row_block)
        res = dot(wqkv[head], h_ref[...], BY_ROWS)
        cos, sin = cos_ref[...], sin_ref[...]

        def rotated(start, b):
            v = (res[start:start + 64] + bias_column(head, b)).astype(BF16).astype(F32)
            lo, hi = v[:32], v[32:]
            return jnp.concatenate([lo * cos - hi * sin, hi * cos + lo * sin], axis=0).astype(BF16)

        q = rotated(0, 0).astype(F32)
        k_new = rotated(64, 1)
        v_new = (res[128:192] + bias_column(head, 2)).astype(BF16)
        lens = len_ref[...].astype(F32)
        for copy in cache_copy(i):
            copy.wait()

        for base, buf in ((0, k_lo), (32, k_hi)):
            def score_group(g, carry, base=base, buf=buf):
                rows = []
                for j in range(GROUP):
                    s = g * GROUP + j
                    kv = jnp.where(lens == (base + s).astype(F32), k_new.astype(F32), buf[s, head].astype(F32))
                    buf[s, head] = kv.astype(BF16)
                    rows.append(jnp.sum(q * kv, axis=0, keepdims=True))
                sc_ref[pl.ds(pl.multiple_of(base + g * GROUP, GROUP), GROUP)] = jnp.concatenate(rows, axis=0)
                return carry

            lax.fori_loop(0, 32 // GROUP, score_group, 0)
        slot = lax.broadcasted_iota(jnp.int32, (64, 256), 0).astype(F32)
        scores = jnp.where(slot <= lens, sc_ref[...] * 0.125, -1e30)
        e = jnp.exp(scores - jnp.max(scores, axis=0, keepdims=True))
        sc_ref[...] = (e / jnp.sum(e, axis=0, keepdims=True)).astype(BF16).astype(F32)

        acc = jnp.zeros((64, 256), F32)
        for base, buf in ((0, v_lo), (32, v_hi)):
            def value_group(g, acc, base=base, buf=buf):
                probs = sc_ref[pl.ds(pl.multiple_of(base + g * GROUP, GROUP), GROUP)]
                for j in range(GROUP):
                    s = g * GROUP + j
                    vv = jnp.where(lens == (base + s).astype(F32), v_new.astype(F32), buf[s, head].astype(F32))
                    buf[s, head] = vv.astype(BF16)
                    acc = acc + probs[j:j + 1] * vv
                return acc

            acc = lax.fori_loop(0, 32 // GROUP, value_group, acc)
        o_ref[pl.ds(pl.multiple_of(head * 64, 64), 64)] = acc.astype(BF16)

    go()
    for i in range(8):
        if i + AHEAD < 8:
            for copy in cache_copy(i + AHEAD):
                copy.start()
        attend(i)
        go()

    o = o_ref[...].T
    part, part_in, h2_ref = down, x1_ref, h_ref
    part[...] = dot(o, wout[...].reshape(1024, 512), BY_ROWS).astype(BF16)
    swap = remote(part, part_in, p_send, p_recv, place.device["z"])
    swap.start()
    go()
    swap.wait_recv()
    swap.wait_send()
    total = (part[...].astype(F32) + part_in[...].astype(F32)).astype(BF16)
    x1 = (x_ref[...].astype(F32) + total.astype(F32)).astype(BF16)
    x1_ref[...] = x1
    h2_ref[...] = normed(x1.astype(F32), 4)
    go()

    for i in range(8):
        block = by_role("gated", i, place.row_block)
        res = dot(wgu[block], h2_ref[...], BY_ROWS).astype(BF16).astype(F32)
        g, u = res[:176], res[176:]
        a_ref[block] = (g / (1.0 + jnp.exp(-g)) * u).astype(BF16)
        go()

    for i in range(8):
        pair = by_role("down", i, lambda k, core: place.col_block(k, core) // 2)
        w = wdn[pl.ds(pair * 2, 2)].reshape(128, 1408)
        cols = pl.ds(pl.multiple_of(pair * 128, 128), 128)
        down[:, cols] = dot(w, a_ref[...].reshape(1408, 256), NAT).T.astype(BF16)
        go()

    for far, steps, _ in roles:
        @pl.when(place.far == far)
        def _(far=far, steps=steps):
            for action in sum(steps, ()):
                if action[0] == "s":
                    chunks[action[1]].copy(action[2], action[3], far == 0).wait_send()

    for i in range(1, 16):
        small_copy(i).wait_send()


def store_kernel(wqkv, wgu, wout, wdn, k_lo, k_hi, v_lo, v_hi, smalls,
                 wq, wk, wv, wo, wg, wu, wd, k_out, v_out, bq, bk, bv, ga, gm, sem):
    pairs = [(src.at[pl.ds(16 * i, 16)], dst.at[pl.ds(base + 16 * i, 16)]) for src, dst, base in (
        (k_lo, k_out, 0), (k_hi, k_out, 32), (v_lo, v_out, 0), (v_hi, v_out, 32)) for i in range(2)]
    pairs += [(wdn, wd), (wgu.at[:, pl.ds(0, 176)], wg), (wgu.at[:, pl.ds(176, 176)], wu),
             (wqkv.at[:, pl.ds(0, 64)], wq), (wqkv.at[:, pl.ds(64, 64)], wk), (wqkv.at[:, pl.ds(128, 64)], wv),
             (wout, wo)]
    copies = [pltpu.make_async_copy(src, dst, sem.at[i]) for i, (src, dst) in enumerate(pairs)]
    for copy in copies:
        copy.start()
    z = lax.axis_index("tp")
    plane = smalls[pl.ds(z * 8, 8)].astype(F32).reshape(4, 2, 8, 128)
    whole = smalls[...].astype(F32).reshape(8, 2, 8, 128)
    for i, ref in enumerate((bq, bk, bv)):
        ref[...] = (plane[:, 0, i] + plane[:, 1, i]).astype(BF16)
    for i, ref in enumerate((ga, gm)):
        ref[...] = (whole[:, 0, 3 + i] + whole[:, 1, 3 + i]).astype(BF16)
    for copy in copies:
        copy.wait()


def finish_kernel(x1, mine, peer, hid):
    total = (mine[...].astype(F32) + peer[...].astype(F32)).astype(BF16)
    hid[...] = (x1[...].astype(F32) + total.astype(F32)).astype(BF16)


def local_step(w_query, b_query, w_key, b_key, w_value, b_value, w_out, w_gate, w_up, w_down, gain_attn, gain_mlp,
               hidden, k_cache, v_cache, lengths):
    freq = np.tile((1.0 / THETA ** (np.arange(0, 64, 2) / 64)).astype(np.float32)[:, None], (1, 256))
    lens = lengths[None, :]
    rows = [v[None, :] for v in (b_query, b_key, b_value, gain_attn, gain_mlp)]
    k_view = jnp.transpose(k_cache, (1, 2, 3, 0))
    v_view = jnp.transpose(v_cache, (1, 2, 3, 0))

    vmem = pl.BlockSpec(memory_space=pltpu.VMEM)
    hbm = pl.BlockSpec(memory_space=pltpu.HBM)
    anywhere = pl.BlockSpec(memory_space=pl.ANY)
    dma = pltpu.SemaphoreType.DMA
    shapes = [(8, 192, 1024), (8, 352, 1024), (16, 64, 512), (16, 64, 1408), *[(32, 8, 64, 256)] * 4,
              (16, 8, 128), (256, 1024), (256, 1024)]
    held = pl.pallas_call(
        layer_kernel,
        out_shape=[pltpu.VMEM(s, BF16) for s in shapes],
        in_specs=[hbm] * 10 + [vmem] * 7,
        out_specs=[vmem] * 11,
        scratch_shapes=[
            pltpu.VMEM((256, 1024), BF16),
            pltpu.VMEM((64, 256), F32),
            pltpu.VMEM((512, 256), BF16),
            pltpu.VMEM((8, 176, 256), BF16),
            pltpu.VMEM((32, 256), F32),
            pltpu.VMEM((32, 256), F32),
            pltpu.VMEM((3, 64, 1024), BF16),
            pltpu.VMEM((4, 88, 1024), BF16),
            pltpu.VMEM((3, 64, 1024), BF16),
            pltpu.VMEM((2, 176, 1024), BF16),
            pltpu.VMEM((64, 1024), BF16),
            pltpu.VMEM((64, 2816), BF16),
            pltpu.VMEM((256, 1024), BF16),
            pltpu.VMEM((8, 128), BF16),
            dma((8,)),
            dma((16,)), dma((16,)), dma((16,)), dma((16,)), dma, dma,
            dma((7, 4, 5)), dma((7, 5)), dma((7, 4)), dma((2, 4, 8)), dma((2, 8)), dma((2, 8)),
        ],
        compiler_params=pltpu.CompilerParams(collective_id=0, has_side_effects=True, vmem_limit_bytes=9437184),
        name="layer",
    )(w_query, w_key, w_value, w_out, w_gate, w_up, w_down, hidden, k_view, v_view, *rows, freq, lens)

    def shape(*dims):
        return jax.ShapeDtypeStruct(dims, BF16)

    peer = lax.ppermute(held[10], "tp", [(0, 1), (1, 0)])
    outs = pl.pallas_call(
        store_kernel,
        out_shape=[shape(8, 64, 1024)] * 3 + [shape(16, 64, 512), shape(8, 176, 1024), shape(8, 176, 1024),
                   shape(16, 64, 1408), shape(*k_view.shape), shape(*v_view.shape),
                   shape(4, 128), shape(4, 128), shape(4, 128), shape(8, 128), shape(8, 128)],
        in_specs=[anywhere] * 8 + [vmem],
        out_specs=[hbm] * 9 + [vmem] * 5,
        scratch_shapes=[dma((15,))],
        compiler_params=pltpu.CompilerParams(vmem_limit_bytes=9437184),
        cost_estimate=pl.CostEstimate(flops=2 * 10**10, bytes_accessed=5 * 10**7, transcendentals=0),
        name="store",
    )(*held[:9])
    hid = pl.pallas_call(
        finish_kernel,
        out_shape=shape(256, 1024),
        in_specs=[vmem] * 3,
        out_specs=vmem,
        compiler_params=pltpu.CompilerParams(vmem_limit_bytes=9437184),
        name="finish",
    )(held[9], held[10], peer)
    wq, wk, wv, wo, wg, wu, wd, k_out, v_out, bq, bk, bv, ga, gm = outs
    flat = lambda a, n: a.reshape(-1, n)
    return (flat(wq, 1024), bq.reshape(512), flat(wk, 1024), bk.reshape(512), flat(wv, 1024), bv.reshape(512),
            flat(wo, 512), flat(wg, 1024), flat(wu, 1024), flat(wd, 1408), ga.reshape(1024), gm.reshape(1024),
            hid, jnp.transpose(k_out, (3, 0, 1, 2)), jnp.transpose(v_out, (3, 0, 1, 2)))


def solution(mesh):
    row_spec = P(("dp", "tp"), None)
    flat_spec = P(("dp", "tp"))
    cache_spec = P("dp", None, "tp", None)
    in_specs = (row_spec, flat_spec, row_spec, flat_spec, row_spec, flat_spec, row_spec, row_spec, row_spec, row_spec,
                flat_spec, flat_spec, P("dp", None), cache_spec, cache_spec, P("dp"))
    out_specs = (P("tp", None), P("tp"), P("tp", None), P("tp"), P("tp", None), P("tp"), P(None, "tp"), P("tp", None),
                 P("tp", None), P(None, "tp"), P(None), P(None), P("dp", None), cache_spec, cache_spec)
    return jax.shard_map(local_step, mesh=mesh, in_specs=in_specs, out_specs=out_specs, check_vma=False)
```

```python
import jax
import jax.numpy as jnp
import numpy as np
from jax import lax
from jax.experimental import pallas as pl
from jax.experimental.pallas import tpu as pltpu
from jax.sharding import PartitionSpec as P

EPS = 1e-6
THETA = 1000000.0
MESH = pl.DeviceIdType.MESH
F32 = jnp.float32
BF16 = jnp.bfloat16
BY_ROWS = (((1,), (1,)), ((), ()))
NAT = (((1,), (0,)), ((), ()))
GROUP = 8


def dot(lhs, rhs, dims):
    return lax.dot_general(lhs, rhs, dims, preferred_element_type=F32)


HOME_STEPS = (
    (
        ("s", "q1", 0, "y", 0), ("s", "q1", 0, "x", 1), ("s", "q2", 0, "y", 0), ("s", "q2", 0, "x", 1),
        ("s", "q0", 0, "y", 0), ("s", "q0", 0, "x", 1), ("s", "q0", 0, "c", 0), ("s", "q1", 0, "c", 0),
        ("s", "q2", 0, "c", 0), ("s", "g0", 0, "c", 0), ("s", "g1", 0, "c", 0), ("s", "u0", 0, "c", 0),
        ("s", "u1", 0, "c", 0), ("s", "o", 0, "c", 0), ("s", "d", 0, "c", 0), ("s", "o", "z", "z", 4),
        ("s", "d", "z", "z", 4),
    ),
    (
        ("s", "o", 0, "y", 2), ("s", "o", 0, "x", 1),
    ),
    (
        ("w", "o", 4), ("s", "o", 4, "c", 4), ("w", "q0", "c", 0), ("w", "q1", "c", 0), ("w", "q2", "c", 0),
    ),
    (
        ("w", "q1", "t"), ("w", "q1", 1), ("s", "q1", 1, "c", 1), ("s", "q1", "t", "z", 2), ("s", "o", 4, "y", 6),
        ("s", "o", 4, "x", 5), ("w", "q1", 2), ("s", "q1", 2, "c", 2), ("w", "o", 1), ("s", "o", 1, "c", 1),
        ("w", "q2", "t"), ("s", "q2", "t", "z", 2), ("w", "q2", 1), ("s", "q2", 1, "c", 1), ("w", "q2", 2),
        ("s", "q2", 2, "c", 2), ("s", "g0", 0, "y", 0), ("s", "q1", 2, "x", 3), ("w", "o", 5), ("s", "o", 5, "c", 5),
        ("w", "q0", "t"), ("s", "q0", "t", "z", 2), ("w", "o", 2), ("s", "o", 2, "c", 2), ("w", "q0", 2),
        ("s", "q0", 2, "c", 2),
    ),
    (
        ("w", "o", 6), ("s", "o", 6, "c", 6), ("w", "q0", 1), ("s", "q0", 1, "c", 1), ("s", "q0", 1, "y", 1),
        ("s", "q2", 2, "x", 3),
    ),
    (
        ("s", "q0", 2, "x", 3), ("w", "q0", "c", 1), ("w", "q1", "c", 1), ("w", "q2", "c", 1),
    ),
    (
        ("w", "g0", 2), ("s", "g0", 2, "c", 2), ("w", "q1", 3), ("s", "q1", 3, "c", 3), ("w", "g0", "t"),
        ("s", "g0", "t", "z", 2), ("s", "q1", 3, "y", 3), ("w", "q0", "c", 2), ("w", "q1", "c", 2), ("w", "q2", "c", 2),
    ),
    (
        ("w", "q2", 3), ("s", "q2", 3, "c", 3), ("s", "o", 1, "y", 3), ("s", "g0", 0, "x", 1), ("w", "d", 4),
        ("s", "d", 4, "c", 4), ("s", "o", 5, "y", 7), ("w", "u0", "t"), ("s", "u0", "t", "z", 2),
        ("s", "u0", 0, "y", 0), ("s", "o", 6, "x", 7), ("w", "q0", 3), ("s", "q0", 3, "c", 3),
    ),
    (
        ("w", "u0", 2), ("s", "u0", 2, "c", 2), ("s", "u0", 0, "x", 1), ("w", "q0", "c", 3), ("w", "q1", "c", 3),
        ("w", "q2", "c", 3),
    ),
    (
        ("w", "u1", "t"), ("s", "u1", "t", "z", 2), ("s", "u1", 0, "y", 0), ("w", "g0", 1), ("s", "g0", 1, "c", 1),
        ("s", "u1", 0, "x", 1), ("w", "o", 7), ("s", "o", 7, "c", 7), ("w", "u1", 2), ("s", "u1", 2, "c", 2),
        ("w", "g1", "t"), ("s", "g1", "t", "z", 2), ("s", "g1", 0, "y", 0), ("w", "o", 3), ("s", "o", 3, "c", 3),
        ("s", "g1", 0, "x", 1), ("w", "u0", 1), ("s", "u0", 1, "c", 1), ("w", "g1", 2), ("s", "g1", 2, "c", 2),
        ("w", "o", "c", 0), ("w", "o", "c", 1), ("w", "o", "c", 2), ("w", "o", "c", 3), ("w", "o", "c", 4),
        ("w", "o", "c", 5), ("w", "o", "c", 6), ("w", "o", "c", 7),
    ),
    (
        ("s", "d", 0, "y", 2), ("w", "d", 2), ("s", "d", 2, "c", 2), ("s", "d", 0, "x", 1), ("w", "u1", 1),
        ("s", "u1", 1, "c", 1), ("s", "d", 4, "y", 6), ("w", "d", 6), ("s", "d", 6, "c", 6), ("s", "d", 4, "x", 5),
        ("w", "g1", 1), ("s", "g1", 1, "c", 1), ("s", "u0", 1, "y", 1), ("w", "g0", 3), ("s", "g0", 3, "c", 3),
        ("s", "g1", 2, "x", 3), ("w", "d", 1), ("s", "d", 1, "c", 1),
    ),
    (
        ("s", "d", 1, "y", 3),
    ),
    (
        ("w", "u0", 3), ("s", "u0", 3, "c", 3), ("w", "g0", "c", 0), ("w", "g1", "c", 0), ("w", "u0", "c", 0),
        ("w", "u1", "c", 0),
    ),
    (
        ("w", "d", 5), ("s", "d", 5, "c", 5), ("s", "d", 6, "x", 7),
    ),
    (
        ("w", "g0", "c", 1), ("w", "g1", "c", 1), ("w", "u0", "c", 1), ("w", "u1", "c", 1),
    ),
    (),
    (
        ("w", "g0", "c", 2), ("w", "g1", "c", 2), ("w", "u0", "c", 2), ("w", "u1", "c", 2),
    ),
    (
        ("w", "u1", 3), ("s", "u1", 3, "c", 3), ("w", "g1", 3), ("s", "g1", 3, "c", 3),
    ),
    (
        ("w", "g0", "c", 3), ("w", "g1", "c", 3), ("w", "u0", "c", 3), ("w", "u1", "c", 3),
    ),
    (),
    (
        ("w", "d", "c", 0), ("w", "d", "c", 4),
    ),
    (
        ("w", "d", 3), ("s", "d", 3, "c", 3),
    ),
    (
        ("w", "d", 7), ("s", "d", 7, "c", 7), ("w", "d", "c", 1), ("w", "d", "c", 5),
    ),
    (),
    (
        ("w", "d", "c", 2), ("w", "d", "c", 6),
    ),
    (),
    (
        ("w", "d", "c", 3), ("w", "d", "c", 7),
    ),
    (),
)
HOME_BLOCKS = {
    "attend": ((0, 0), (0, 1), (2, 0), (1, 0), (1, 1), (2, 1), (3, 0), (3, 1)),
    "gated": ((0, 0), (0, 1), (1, 0), (1, 1), (2, 0), (2, 1), (3, 0), (3, 1)),
    "down": ((0, 0), (0, 1), (1, 0), (1, 1), (2, 0), (2, 1), (3, 0), (3, 1)),
}
AWAY_STEPS = (
    (
        ("s", "q1", "own", "z", 2), ("s", "q1", "own", "y", "t"), ("s", "q2", "own", "z", 2),
        ("s", "q2", "own", "y", "t"), ("s", "q0", "own", "y", "t"), ("s", "q0", "own", "z", 2), ("s", "o", 0, "c", 0),
        ("s", "d", 0, "c", 0), ("s", "o", "z", "z", 4), ("s", "o", 0, "x", 1), ("s", "d", 0, "x", 1),
    ),
    (
        ("w", "o", 1), ("s", "o", 1, "c", 1), ("w", "o", 4), ("s", "o", 4, "c", 4), ("s", "o", 4, "x", 5),
        ("w", "q1", 0), ("s", "q1", 0, "c", 0), ("s", "q1", 0, "x", 1), ("w", "o", 2), ("s", "o", 2, "c", 2),
        ("s", "o", 0, "y", 2), ("w", "d", 1), ("s", "d", 1, "c", 1), ("w", "d", 4), ("s", "d", 4, "c", 4),
        ("s", "d", 4, "x", 5), ("s", "g0", "own", "z", 2), ("s", "o", 4, "y", 6), ("w", "o", 5), ("s", "o", 5, "c", 5),
        ("w", "q2", 0), ("s", "q2", 0, "c", 0), ("s", "g0", "own", "y", "t"), ("w", "o", 6), ("s", "o", 6, "c", 6),
        ("w", "q1", 2), ("s", "q1", 2, "c", 2), ("s", "q2", 0, "x", 1), ("w", "q1", 1), ("s", "q1", 1, "c", 1),
        ("s", "d", "z", "z", 4), ("s", "u0", "own", "y", "t"), ("w", "q0", 0), ("s", "q0", 0, "c", 0),
    ),
    (
        ("w", "q2", 2), ("s", "q2", 2, "c", 2), ("s", "q2", 2, "x", 3), ("w", "q0", "c", 0), ("w", "q1", "c", 0),
        ("w", "q2", "c", 0),
    ),
    (
        ("w", "d", 5), ("s", "d", 5, "c", 5), ("w", "q0", 2), ("s", "q0", 2, "c", 2), ("s", "u0", "own", "z", 2),
        ("s", "u1", "own", "y", "t"), ("s", "q0", 2, "x", 3),
    ),
    (
        ("w", "g0", 0), ("s", "g0", 0, "c", 0), ("w", "q2", 1), ("s", "q2", 1, "c", 1), ("w", "q0", "c", 2),
        ("w", "q1", "c", 2), ("w", "q2", "c", 2),
    ),
    (
        ("w", "q0", 1), ("s", "q0", 1, "c", 1), ("s", "u1", "own", "z", 2), ("s", "g1", "own", "y", "t"),
        ("s", "g0", 0, "x", 1),
    ),
    (
        ("w", "q2", 3), ("s", "q2", 3, "c", 3), ("w", "q1", 3), ("s", "q1", 3, "c", 3), ("w", "q0", "c", 1),
        ("w", "q1", "c", 1), ("w", "q2", "c", 1),
    ),
    (
        ("w", "g0", 2), ("s", "g0", 2, "c", 2), ("w", "q0", 3), ("s", "q0", 3, "c", 3), ("w", "o", 3),
        ("s", "o", 3, "c", 3), ("s", "g1", "own", "z", 2), ("s", "o", 1, "y", 3), ("s", "g0", 2, "x", 3),
    ),
    (
        ("w", "o", 7), ("s", "o", 7, "c", 7), ("s", "d", 0, "y", 2), ("w", "q0", "c", 3), ("w", "q1", "c", 3),
        ("w", "q2", "c", 3),
    ),
    (
        ("w", "u0", 2), ("s", "u0", 2, "c", 2), ("w", "g0", 1), ("s", "g0", 1, "c", 1), ("s", "u0", 2, "x", 3),
        ("w", "o", "c", 0), ("w", "o", "c", 1), ("w", "o", "c", 2), ("w", "o", "c", 3), ("w", "o", "c", 4),
        ("w", "o", "c", 5), ("w", "o", "c", 6), ("w", "o", "c", 7),
    ),
    (
        ("w", "u0", 0), ("s", "u0", 0, "c", 0), ("s", "d", 4, "y", 6), ("w", "u1", 2), ("s", "u1", 2, "c", 2),
        ("s", "u1", 2, "x", 3), ("w", "g0", 3), ("s", "g0", 3, "c", 3), ("w", "u1", 0), ("s", "u1", 0, "c", 0),
        ("s", "g0", 3, "y", 3), ("s", "u1", 0, "x", 1), ("w", "g1", 2), ("s", "g1", 2, "c", 2), ("w", "u0", 3),
        ("s", "u0", 3, "c", 3), ("w", "g1", 0), ("s", "g1", 0, "c", 0), ("s", "u0", 3, "y", 3), ("s", "g1", 0, "x", 1),
        ("w", "u1", 3), ("s", "u1", 3, "c", 3), ("w", "d", 2), ("s", "d", 2, "c", 2), ("s", "u1", 3, "y", 3),
        ("s", "g1", 2, "x", 3), ("w", "u1", 1), ("s", "u1", 1, "c", 1), ("w", "d", 6), ("s", "d", 6, "c", 6),
        ("s", "d", 1, "y", 3),
    ),
    (
        ("w", "g1", 1), ("s", "g1", 1, "c", 1), ("s", "d", 6, "x", 7),
    ),
    (
        ("w", "u0", 1), ("s", "u0", 1, "c", 1), ("w", "g0", "c", 0), ("w", "g1", "c", 0), ("w", "u0", "c", 0),
        ("w", "u1", "c", 0),
    ),
    (),
    (),
    (
        ("w", "g1", 3), ("s", "g1", 3, "c", 3), ("w", "g0", "c", 1), ("w", "g1", "c", 1), ("w", "u0", "c", 1),
        ("w", "u1", "c", 1),
    ),
    (
        ("w", "g0", "c", 2), ("w", "g1", "c", 2), ("w", "u0", "c", 2), ("w", "u1", "c", 2),
    ),
    (),
    (
        ("w", "d", 3), ("s", "d", 3, "c", 3), ("w", "g0", "c", 3), ("w", "g1", "c", 3), ("w", "u0", "c", 3),
        ("w", "u1", "c", 3),
    ),
    (),
    (
        ("w", "d", "c", 0), ("w", "d", "c", 4),
    ),
    (
        ("w", "d", 7), ("s", "d", 7, "c", 7),
    ),
    (
        ("w", "d", "c", 1), ("w", "d", "c", 5),
    ),
    (),
    (
        ("w", "d", "c", 2), ("w", "d", "c", 6),
    ),
    (),
    (
        ("w", "d", "c", 3), ("w", "d", "c", 7),
    ),
    (),
)
AWAY_BLOCKS = {
    "attend": ((0, 0), (0, 1), (2, 0), (2, 1), (1, 0), (1, 1), (3, 0), (3, 1)),
    "gated": ((0, 0), (0, 1), (1, 0), (2, 0), (1, 1), (2, 1), (3, 0), (3, 1)),
    "down": ((0, 0), (0, 1), (1, 0), (1, 1), (2, 0), (2, 1), (3, 0), (3, 1)),
}


class Place:
    def __init__(self):
        tp = lax.axis_index("tp")
        dp = lax.axis_index("dp")
        self.z = tp
        self.dp = dp
        self.y = dp // 4
        self.x = (dp // 2) % 2
        self.c = dp % 2
        self.far = lax.rem(self.y + self.z, 2)
        self.device = {
            "x": (tp, dp + 2 - 4 * self.x),
            "y": (tp, dp + 4 - 8 * self.y),
            "c": (tp, dp + 1 - 2 * self.c),
            "z": (1 - tp, dp),
        }

    def at(self, axis, flip):
        here = getattr(self, axis)
        return 1 - here if flip else here

    def row_block(self, k, core=0):
        return (self.at("x", k & 1) * 2 + self.at("c", core)) * 2 + self.at("z", k & 2)

    def col_block(self, k, core=0):
        return (self.at("y", k & 2) * 4 + self.at("x", k & 1) * 2 + self.at("c", core)) * 2 + self.at("z", k & 4)


def remote(src, dst, send, recv, device):
    return pltpu.make_async_remote_copy(
        src_ref=src, dst_ref=dst, send_sem=send, recv_sem=recv, device_id=device, device_id_type=MESH)


class Rows:
    def __init__(self, place, buf, start, own, through, index, sems):
        self.p, self.buf, self.start, self.own, self.through = place, buf, start, own, through
        self.i, (self.send, self.r, self.rc) = index, sems
        self.n = own.shape[0]

    def block(self, k, core=0):
        return self.buf.at[self.p.row_block(k, core), pl.ds(self.start, self.n)]

    def copy(self, k, link, home):
        p = self.p
        slot = {"own": 0, "t": 4}.get(k, k)
        send = self.send.at[self.i, "xyzc".index(link), slot]
        if k == "own" or (home and k == 0):
            src = self.own
        elif k == "t":
            src = self.through
        else:
            src = self.block(k)
        if k == "own" and link == "y":
            dst, recv = self.through, self.r.at[self.i, 4]
        else:
            dst = self.block(0 if k in ("own", "t") else k)
            got = 2 if link == "z" else k ^ 1 if link == "x" else k
            recv = self.rc.at[self.i, k] if link == "c" else self.r.at[self.i, got]
        return remote(src, dst, send, recv, p.device[link])

    def wait(self, k, core):
        if k == "t":
            ref, recv = self.through, self.r.at[self.i, 4]
        else:
            ref, recv = self.block(k, core), (self.rc if core else self.r).at[self.i, k]
        remote(ref, ref, self.send.at[self.i, 0, 0], recv, self.p.device["x"]).wait_recv()

    def local(self):
        @pl.when(self.p.far == 0)
        def _():
            self.buf[self.p.row_block(0), pl.ds(self.start, self.n)] = self.own[...]


class Cols:
    def __init__(self, place, buf, own, index, sems):
        self.p, self.buf, self.own = place, buf, own
        self.n = buf.shape[-1]
        self.i, (self.send, self.r, self.rc) = index, sems

    def block(self, k, core=0):
        return self.buf.at[self.p.col_block(k, core)]

    def half(self, z):
        return self.own.at[:, pl.ds(pl.multiple_of(z * self.n, 128), self.n)]

    def copy(self, k, link, home):
        p = self.p
        if link == "z":
            return remote(self.half(1 - p.z), self.block(0), self.send.at[self.i, 2, 0], self.r.at[self.i, 4], p.device["z"])
        src = self.half(p.z) if k == 0 else self.block(k)
        got = k ^ 1 if link == "x" else k ^ 2
        recv = self.rc.at[self.i, k] if link == "c" else self.r.at[self.i, got]
        return remote(src, self.block(k), self.send.at[self.i, "xyzc".index(link), k], recv, p.device[link])

    def wait(self, k, core):
        ref, recv = self.block(k, core), (self.rc if core else self.r).at[self.i, k]
        remote(ref, ref, self.send.at[self.i, 0, 0], recv, self.p.device["x"]).wait_recv()

    def local(self):
        self.buf[self.p.col_block(0)] = self.own[:, pl.ds(pl.multiple_of(self.p.z * self.n, 128), self.n)]


def layer_kernel(wq_hbm, wk_hbm, wv_hbm, wo_hbm, wg_hbm, wu_hbm, wd_hbm, x_hbm, k_hbm, v_hbm,
                 bq, bk, bv, ga, gm, cos_ref, sin_ref, len_ref,
                 wqkv, wgu, wout, wdn, k_lo, k_hi, v_lo, v_hi, smalls, x1_ref, down,
                 h_ref, sc_ref, o_ref, a_ref, t_q, t_gu, w_q, w_gu, wo, wd, x_ref, small, l_sem,
                 k_sem, v_sem, s_send, s_recv, p_send, p_recv, row_s, row_r, row_c, col_s, col_r, col_c):
    place = Place()
    me = place.dp * 2 + place.z
    row_sem, col_sem = (row_s, row_r, row_c), (col_s, col_r, col_c)
    loads = [(wq_hbm, w_q.at[0]), (wk_hbm, w_q.at[1]), (wv_hbm, w_q.at[2]), (wo_hbm, wo), (wg_hbm, w_gu.at[0]),
             (wu_hbm, w_gu.at[1]), (wd_hbm, wd), (x_hbm, x_ref)]
    loads = [pltpu.make_async_copy(src, dst, l_sem.at[i]) for i, (src, dst) in enumerate(loads)]
    for load in loads:
        load.start()
    chunks = {}
    for i in range(3):
        chunks[f"q{i}"] = Rows(place, wqkv, 64 * i, w_q.at[i], t_q.at[i], i, row_sem)
    for i in range(4):
        ref = w_gu.at[i // 2, pl.ds(88 * (i % 2), 88)]
        chunks["gu"[i // 2] + str(i % 2)] = Rows(place, wgu, 88 * i, ref, t_gu.at[i], 3 + i, row_sem)
    chunks["o"] = Cols(place, wout, wo, 0, col_sem)
    chunks["d"] = Cols(place, wdn, wd, 1, col_sem)
    roles = ((0, HOME_STEPS, HOME_BLOCKS), (1, AWAY_STEPS, AWAY_BLOCKS))
    step = iter(range(len(HOME_STEPS)))

    def go():
        now = next(step)
        for far, steps, _ in roles:
            if steps[now]:
                @pl.when(place.far == far)
                def _(far=far, steps=steps):
                    for action in steps[now]:
                        chunk = chunks[action[1]]
                        if action[0] == "s":
                            chunk.copy(action[2], action[3], far == 0).start()
                        elif action[2] == "c":
                            chunk.wait(action[3], 1)
                        else:
                            chunk.wait(action[2], 0)

    def by_role(kind, i, place_of, swap=False):
        home, away = (place_of(*blocks[kind][i]) for _, _, blocks in roles)
        if swap:
            home, away = away, home
        return home + place.far * (away - home)

    def cache_copy(i):
        head = by_role("attend", i, place.row_block)
        copies = []
        for hbm, lo, hi, sem in ((k_hbm, k_lo, k_hi, k_sem), (v_hbm, v_lo, v_hi, v_sem)):
            copies.append(pltpu.make_async_copy(hbm.at[pl.ds(0, 32), head], lo.at[:, head], sem.at[2 * i]))
            copies.append(pltpu.make_async_copy(hbm.at[pl.ds(32, 32), head], hi.at[:, head], sem.at[2 * i + 1]))
        return copies

    barrier = pltpu.get_barrier_semaphore()
    for i in range(1, 16):
        other = lax.rem(me + i, 16)
        pl.semaphore_signal(barrier, inc=1, device_id=(other % 2, other // 2), device_id_type=MESH)
    for i in range(8):
        for copy in cache_copy(i):
            copy.start()
    vectors = jnp.concatenate([v[...].astype(F32) for v in (bq, bk, bv, ga, gm)] + [jnp.zeros((3, 64), F32)], axis=0)
    vectors = jnp.concatenate([vectors, vectors], axis=1)
    mine = lax.broadcasted_iota(jnp.int32, (8, 128), 1) // 64 == place.z
    vectors = jnp.where(mine, vectors, 0.0).astype(BF16)
    small[...] = vectors
    smalls[me] = vectors
    for load in loads:
        load.wait()
    pl.semaphore_wait(barrier, 15)

    def small_copy(i):
        other = lax.rem(me + i, 16)
        return remote(small, smalls.at[me], s_send.at[i], s_recv.at[i], (other % 2, other // 2))

    for i in range(1, 16):
        small_copy(i).start()
    go()

    for chunk in chunks.values():
        chunk.local()
    for i in range(1, 16):
        small_copy(i).wait_recv()

    def gain_row(i):
        pair = smalls[...].astype(F32).reshape(8, 2, 8, 128)
        rows = pair[:, 0, i] + pair[:, 1, i]
        return jnp.concatenate([rows[d:d + 1] for d in range(8)], axis=1)

    def normed(rows, i):
        inv = lax.rsqrt(jnp.mean(rows * rows, axis=-1, keepdims=True) + EPS)
        return (rows * inv * gain_row(i)).astype(BF16)

    h_ref[...] = normed(x_ref[...].astype(F32), 3)

    eye = lax.broadcasted_iota(jnp.int32, (64, 128), 1) % 64 == lax.broadcasted_iota(jnp.int32, (64, 128), 0)

    def bias_column(head, i):
        row = smalls[place.z * 8 + head].astype(F32)[i:i + 1]
        return jnp.sum(jnp.where(eye, row, 0.0), axis=1, keepdims=True)

    def attend(i):
        head = by_role("attend", i, place.row_block)
        res = dot(wqkv[head], h_ref[...], BY_ROWS)
        cos, sin = cos_ref[...], sin_ref[...]

        def rotated(start, b):
            v = (res[start:start + 64] + bias_column(head, b)).astype(BF16).astype(F32)
            lo, hi = v[:32], v[32:]
            return jnp.concatenate([lo * cos - hi * sin, hi * cos + lo * sin], axis=0).astype(BF16)

        q = rotated(0, 0).astype(F32)
        k_new = rotated(64, 1)
        v_new = (res[128:192] + bias_column(head, 2)).astype(BF16)
        lens = len_ref[...].astype(F32)
        for copy in cache_copy(i):
            copy.wait()

        for base, buf in ((0, k_lo), (32, k_hi)):
            def score_group(g, carry, base=base, buf=buf):
                rows = []
                for j in range(GROUP):
                    s = g * GROUP + j
                    kv = jnp.where(lens == (base + s).astype(F32), k_new.astype(F32), buf[s, head].astype(F32))
                    buf[s, head] = kv.astype(BF16)
                    rows.append(jnp.sum(q * kv, axis=0, keepdims=True))
                sc_ref[pl.ds(pl.multiple_of(base + g * GROUP, GROUP), GROUP)] = jnp.concatenate(rows, axis=0)
                return carry

            lax.fori_loop(0, 32 // GROUP, score_group, 0)
        slot = lax.broadcasted_iota(jnp.int32, (64, 256), 0).astype(F32)
        scores = jnp.where(slot <= lens, sc_ref[...] * 0.125, -1e30)
        e = jnp.exp(scores - jnp.max(scores, axis=0, keepdims=True))
        sc_ref[...] = (e / jnp.sum(e, axis=0, keepdims=True)).astype(BF16).astype(F32)

        acc = jnp.zeros((64, 256), F32)
        for base, buf in ((0, v_lo), (32, v_hi)):
            def value_group(g, acc, base=base, buf=buf):
                probs = sc_ref[pl.ds(pl.multiple_of(base + g * GROUP, GROUP), GROUP)]
                for j in range(GROUP):
                    s = g * GROUP + j
                    vv = jnp.where(lens == (base + s).astype(F32), v_new.astype(F32), buf[s, head].astype(F32))
                    buf[s, head] = vv.astype(BF16)
                    acc = acc + probs[j:j + 1] * vv
                return acc

            acc = lax.fori_loop(0, 32 // GROUP, value_group, acc)
        o_ref[pl.ds(pl.multiple_of(head * 64, 64), 64)] = acc.astype(BF16)

    go()
    for i in range(8):
        attend(i)
        go()

    o = o_ref[...].T
    part, part_in, h2_ref = down, x1_ref, h_ref
    part[...] = dot(o, wout[...].reshape(1024, 512), BY_ROWS).astype(BF16)
    swap = remote(part, part_in, p_send, p_recv, place.device["z"])
    swap.start()
    go()
    swap.wait_recv()
    swap.wait_send()
    total = (part[...].astype(F32) + part_in[...].astype(F32)).astype(BF16)
    x1 = (x_ref[...].astype(F32) + total.astype(F32)).astype(BF16)
    x1_ref[...] = x1
    h2_ref[...] = normed(x1.astype(F32), 4)
    go()

    for i in range(8):
        block = by_role("gated", i, place.row_block)
        res = dot(wgu[block], h2_ref[...], BY_ROWS).astype(BF16).astype(F32)
        g, u = res[:176], res[176:]
        a_ref[block] = (g / (1.0 + jnp.exp(-g)) * u).astype(BF16)
        go()

    for i in range(8):
        pair = by_role("down", i, lambda k, core: place.col_block(k, core) // 2)
        w = wdn[pl.ds(pair * 2, 2)].reshape(128, 1408)
        cols = pl.ds(pl.multiple_of(pair * 128, 128), 128)
        down[:, cols] = dot(w, a_ref[...].reshape(1408, 256), NAT).T.astype(BF16)
        go()

    for far, steps, _ in roles:
        @pl.when(place.far == far)
        def _(far=far, steps=steps):
            for action in sum(steps, ()):
                if action[0] == "s":
                    chunks[action[1]].copy(action[2], action[3], far == 0).wait_send()

    for i in range(1, 16):
        small_copy(i).wait_send()


def store_kernel(wqkv, wgu, wout, wdn, k_lo, k_hi, v_lo, v_hi, smalls,
                 wq, wk, wv, wo, wg, wu, wd, k_out, v_out, bq, bk, bv, ga, gm, sem):
    lo, hi = pl.ds(0, 32), pl.ds(32, 32)
    pairs = [(k_lo, k_out.at[lo]), (k_hi, k_out.at[hi]), (v_lo, v_out.at[lo]), (v_hi, v_out.at[hi]),
             (wdn, wd), (wgu.at[:, pl.ds(0, 176)], wg), (wgu.at[:, pl.ds(176, 176)], wu),
             (wqkv.at[:, pl.ds(0, 64)], wq), (wqkv.at[:, pl.ds(64, 64)], wk), (wqkv.at[:, pl.ds(128, 64)], wv),
             (wout, wo)]
    copies = [pltpu.make_async_copy(src, dst, sem.at[i]) for i, (src, dst) in enumerate(pairs)]
    for copy in copies:
        copy.start()
    z = lax.axis_index("tp")
    plane = smalls[pl.ds(z * 8, 8)].astype(F32).reshape(4, 2, 8, 128)
    whole = smalls[...].astype(F32).reshape(8, 2, 8, 128)
    for i, ref in enumerate((bq, bk, bv)):
        ref[...] = (plane[:, 0, i] + plane[:, 1, i]).astype(BF16)
    for i, ref in enumerate((ga, gm)):
        ref[...] = (whole[:, 0, 3 + i] + whole[:, 1, 3 + i]).astype(BF16)
    for copy in copies:
        copy.wait()


def finish_kernel(x1, mine, peer, hid):
    total = (mine[...].astype(F32) + peer[...].astype(F32)).astype(BF16)
    hid[...] = (x1[...].astype(F32) + total.astype(F32)).astype(BF16)


def local_step(w_query, b_query, w_key, b_key, w_value, b_value, w_out, w_gate, w_up, w_down, gain_attn, gain_mlp,
               hidden, k_cache, v_cache, lengths):
    inv_freq = (1.0 / THETA ** (np.arange(0, 64, 2) / 64)).astype(np.float32)
    angles = inv_freq[:, None] * jnp.broadcast_to(lengths[None, :], (32, 256)).astype(F32)
    cos, sin = jnp.cos(angles), jnp.sin(angles)
    lens = lengths[None, :]
    rows = [v[None, :] for v in (b_query, b_key, b_value, gain_attn, gain_mlp)]
    k_view = jnp.transpose(k_cache, (1, 2, 3, 0))
    v_view = jnp.transpose(v_cache, (1, 2, 3, 0))

    vmem = pl.BlockSpec(memory_space=pltpu.VMEM)
    hbm = pl.BlockSpec(memory_space=pltpu.HBM)
    anywhere = pl.BlockSpec(memory_space=pl.ANY)
    dma = pltpu.SemaphoreType.DMA
    shapes = [(8, 192, 1024), (8, 352, 1024), (16, 64, 512), (16, 64, 1408), *[(32, 8, 64, 256)] * 4,
              (16, 8, 128), (256, 1024), (256, 1024)]
    held = pl.pallas_call(
        layer_kernel,
        out_shape=[pltpu.VMEM(s, BF16) for s in shapes],
        in_specs=[hbm] * 10 + [vmem] * 8,
        out_specs=[vmem] * 11,
        scratch_shapes=[
            pltpu.VMEM((256, 1024), BF16),
            pltpu.VMEM((64, 256), F32),
            pltpu.VMEM((512, 256), BF16),
            pltpu.VMEM((8, 176, 256), BF16),
            pltpu.VMEM((3, 64, 1024), BF16),
            pltpu.VMEM((4, 88, 1024), BF16),
            pltpu.VMEM((3, 64, 1024), BF16),
            pltpu.VMEM((2, 176, 1024), BF16),
            pltpu.VMEM((64, 1024), BF16),
            pltpu.VMEM((64, 2816), BF16),
            pltpu.VMEM((256, 1024), BF16),
            pltpu.VMEM((8, 128), BF16),
            dma((8,)),
            dma((16,)), dma((16,)), dma((16,)), dma((16,)), dma, dma,
            dma((7, 4, 5)), dma((7, 5)), dma((7, 4)), dma((2, 4, 8)), dma((2, 8)), dma((2, 8)),
        ],
        compiler_params=pltpu.CompilerParams(collective_id=0, has_side_effects=True, vmem_limit_bytes=9437184),
        name="layer",
    )(w_query, w_key, w_value, w_out, w_gate, w_up, w_down, hidden, k_view, v_view, *rows, cos, sin, lens)

    def shape(*dims):
        return jax.ShapeDtypeStruct(dims, BF16)

    peer = lax.ppermute(held[10], "tp", [(0, 1), (1, 0)])
    outs = pl.pallas_call(
        store_kernel,
        out_shape=[shape(8, 64, 1024)] * 3 + [shape(16, 64, 512), shape(8, 176, 1024), shape(8, 176, 1024),
                   shape(16, 64, 1408), shape(*k_view.shape), shape(*v_view.shape),
                   shape(4, 128), shape(4, 128), shape(4, 128), shape(8, 128), shape(8, 128)],
        in_specs=[anywhere] * 8 + [vmem],
        out_specs=[hbm] * 9 + [vmem] * 5,
        scratch_shapes=[dma((11,))],
        compiler_params=pltpu.CompilerParams(vmem_limit_bytes=9437184),
        cost_estimate=pl.CostEstimate(flops=2 * 10**10, bytes_accessed=5 * 10**7, transcendentals=0),
        name="store",
    )(*held[:9])
    hid = pl.pallas_call(
        finish_kernel,
        out_shape=shape(256, 1024),
        in_specs=[vmem] * 3,
        out_specs=vmem,
        compiler_params=pltpu.CompilerParams(vmem_limit_bytes=9437184),
        name="finish",
    )(held[9], held[10], peer)
    wq, wk, wv, wo, wg, wu, wd, k_out, v_out, bq, bk, bv, ga, gm = outs
    flat = lambda a, n: a.reshape(-1, n)
    return (flat(wq, 1024), bq.reshape(512), flat(wk, 1024), bk.reshape(512), flat(wv, 1024), bv.reshape(512),
            flat(wo, 512), flat(wg, 1024), flat(wu, 1024), flat(wd, 1408), ga.reshape(1024), gm.reshape(1024),
            hid, jnp.transpose(k_out, (3, 0, 1, 2)), jnp.transpose(v_out, (3, 0, 1, 2)))


def solution(mesh):
    row_spec = P(("dp", "tp"), None)
    flat_spec = P(("dp", "tp"))
    cache_spec = P("dp", None, "tp", None)
    in_specs = (row_spec, flat_spec, row_spec, flat_spec, row_spec, flat_spec, row_spec, row_spec, row_spec, row_spec,
                flat_spec, flat_spec, P("dp", None), cache_spec, cache_spec, P("dp"))
    out_specs = (P("tp", None), P("tp"), P("tp", None), P("tp"), P("tp", None), P("tp"), P(None, "tp"), P("tp", None),
                 P("tp", None), P(None, "tp"), P(None), P(None), P("dp", None), cache_spec, cache_spec)
    return jax.shard_map(local_step, mesh=mesh, in_specs=in_specs, out_specs=out_specs, check_vma=False)
```

```python
import jax
import jax.numpy as jnp
import numpy as np
from jax import lax
from jax.experimental import pallas as pl
from jax.experimental.pallas import tpu as pltpu
from jax.sharding import PartitionSpec as P

EPS = 1e-6
THETA = 1000000.0
MESH = pl.DeviceIdType.MESH
F32 = jnp.float32
BF16 = jnp.bfloat16
BY_ROWS = (((1,), (1,)), ((), ()))
NAT = (((1,), (0,)), ((), ()))
GROUP = 8


def dot(lhs, rhs, dims):
    return lax.dot_general(lhs, rhs, dims, preferred_element_type=F32)


HOME_STEPS = (
    (
        ("s", "q0", 0, "c", 0), ("s", "q1", 0, "c", 0), ("s", "q2", 0, "c", 0), ("s", "g0", 0, "c", 0),
        ("s", "g1", 0, "c", 0), ("s", "u0", 0, "c", 0), ("s", "u1", 0, "c", 0), ("s", "o", 0, "c", 0),
        ("s", "d", 0, "c", 0), ("s", "o", "z", "z", 4), ("s", "d", "z", "z", 4), ("s", "q1", 0, "y", 0),
        ("s", "q1", 0, "x", 1),
    ),
    (
        ("s", "o", 0, "y", 2), ("s", "q2", 0, "y", 0), ("s", "o", 0, "x", 1), ("s", "q2", 0, "x", 1),
    ),
    (
        ("w", "o", 4), ("s", "o", 4, "c", 4), ("w", "q0", "c", 0), ("w", "q1", "c", 0), ("w", "q2", "c", 0),
    ),
    (
        ("w", "q1", "t"), ("w", "q1", 1), ("s", "q1", 1, "c", 1), ("s", "q1", "t", "z", 2), ("s", "o", 4, "y", 6),
        ("s", "o", 4, "x", 5), ("w", "q1", 2), ("s", "q1", 2, "c", 2), ("w", "o", 1), ("s", "o", 1, "c", 1),
        ("s", "q0", 0, "y", 0), ("s", "q0", 0, "x", 1), ("w", "q2", "t"), ("s", "q2", "t", "z", 2), ("w", "q2", 1),
        ("s", "q2", 1, "c", 1), ("w", "q2", 2), ("s", "q2", 2, "c", 2), ("s", "g0", 0, "y", 0), ("s", "q1", 2, "x", 3),
        ("w", "o", 5), ("s", "o", 5, "c", 5), ("w", "q0", "t"), ("s", "q0", "t", "z", 2), ("w", "o", 2),
        ("s", "o", 2, "c", 2), ("w", "q0", 2), ("s", "q0", 2, "c", 2),
    ),
    (
        ("w", "o", 6), ("s", "o", 6, "c", 6), ("w", "q0", 1), ("s", "q0", 1, "c", 1), ("s", "q0", 1, "y", 1),
        ("s", "q2", 2, "x", 3),
    ),
    (
        ("s", "q0", 2, "x", 3), ("w", "q0", "c", 1), ("w", "q1", "c", 1), ("w", "q2", "c", 1),
    ),
    (
        ("w", "g0", 2), ("s", "g0", 2, "c", 2), ("w", "q1", 3), ("s", "q1", 3, "c", 3), ("w", "g0", "t"),
        ("s", "g0", "t", "z", 2), ("s", "q1", 3, "y", 3), ("w", "q0", "c", 2), ("w", "q1", "c", 2), ("w", "q2", "c", 2),
    ),
    (
        ("w", "q2", 3), ("s", "q2", 3, "c", 3), ("s", "o", 1, "y", 3), ("s", "g0", 0, "x", 1), ("w", "d", 4),
        ("s", "d", 4, "c", 4), ("s", "o", 5, "y", 7), ("w", "u0", "t"), ("s", "u0", "t", "z", 2),
        ("s", "u0", 0, "y", 0), ("s", "o", 6, "x", 7), ("w", "q0", 3), ("s", "q0", 3, "c", 3),
    ),
    (
        ("w", "u0", 2), ("s", "u0", 2, "c", 2), ("s", "u0", 0, "x", 1), ("w", "q0", "c", 3), ("w", "q1", "c", 3),
        ("w", "q2", "c", 3),
    ),
    (
        ("w", "u1", "t"), ("s", "u1", "t", "z", 2), ("s", "u1", 0, "y", 0), ("w", "g0", 1), ("s", "g0", 1, "c", 1),
        ("s", "u1", 0, "x", 1), ("w", "o", 7), ("s", "o", 7, "c", 7), ("w", "u1", 2), ("s", "u1", 2, "c", 2),
        ("w", "g1", "t"), ("s", "g1", "t", "z", 2), ("s", "g1", 0, "y", 0), ("w", "o", 3), ("s", "o", 3, "c", 3),
        ("s", "g1", 0, "x", 1), ("w", "u0", 1), ("s", "u0", 1, "c", 1), ("w", "g1", 2), ("s", "g1", 2, "c", 2),
        ("w", "o", "c", 0), ("w", "o", "c", 1), ("w", "o", "c", 2), ("w", "o", "c", 3), ("w", "o", "c", 4),
        ("w", "o", "c", 5), ("w", "o", "c", 6), ("w", "o", "c", 7),
    ),
    (
        ("s", "d", 0, "y", 2), ("w", "d", 2), ("s", "d", 2, "c", 2), ("s", "d", 0, "x", 1), ("w", "u1", 1),
        ("s", "u1", 1, "c", 1), ("s", "d", 4, "y", 6), ("w", "d", 6), ("s", "d", 6, "c", 6), ("s", "d", 4, "x", 5),
        ("w", "g1", 1), ("s", "g1", 1, "c", 1), ("s", "u0", 1, "y", 1), ("w", "g0", 3), ("s", "g0", 3, "c", 3),
        ("s", "g1", 2, "x", 3), ("w", "d", 1), ("s", "d", 1, "c", 1),
    ),
    (
        ("s", "d", 1, "y", 3),
    ),
    (
        ("w", "u0", 3), ("s", "u0", 3, "c", 3), ("w", "g0", "c", 0), ("w", "g1", "c", 0), ("w", "u0", "c", 0),
        ("w", "u1", "c", 0),
    ),
    (
        ("w", "d", 5), ("s", "d", 5, "c", 5), ("s", "d", 6, "x", 7),
    ),
    (
        ("w", "g0", "c", 1), ("w", "g1", "c", 1), ("w", "u0", "c", 1), ("w", "u1", "c", 1),
    ),
    (),
    (
        ("w", "g0", "c", 2), ("w", "g1", "c", 2), ("w", "u0", "c", 2), ("w", "u1", "c", 2),
    ),
    (
        ("w", "u1", 3), ("s", "u1", 3, "c", 3), ("w", "g1", 3), ("s", "g1", 3, "c", 3),
    ),
    (
        ("w", "g0", "c", 3), ("w", "g1", "c", 3), ("w", "u0", "c", 3), ("w", "u1", "c", 3),
    ),
    (),
    (
        ("w", "d", "c", 0), ("w", "d", "c", 4),
    ),
    (
        ("w", "d", 3), ("s", "d", 3, "c", 3),
    ),
    (
        ("w", "d", 7), ("s", "d", 7, "c", 7), ("w", "d", "c", 1), ("w", "d", "c", 5),
    ),
    (),
    (
        ("w", "d", "c", 2), ("w", "d", "c", 6),
    ),
    (),
    (
        ("w", "d", "c", 3), ("w", "d", "c", 7),
    ),
    (),
)
HOME_BLOCKS = {
    "attend": ((0, 0), (0, 1), (2, 0), (1, 0), (1, 1), (2, 1), (3, 0), (3, 1)),
    "gated": ((0, 0), (0, 1), (1, 0), (1, 1), (2, 0), (2, 1), (3, 0), (3, 1)),
    "down": ((0, 0), (0, 1), (1, 0), (1, 1), (2, 0), (2, 1), (3, 0), (3, 1)),
}
AWAY_STEPS = (
    (
        ("s", "o", 0, "c", 0), ("s", "d", 0, "c", 0), ("s", "o", "z", "z", 4), ("s", "q1", "own", "z", 2),
        ("s", "q1", "own", "y", "t"), ("s", "o", 0, "x", 1), ("s", "d", 0, "x", 1),
    ),
    (
        ("s", "q2", "own", "z", 2), ("s", "q2", "own", "y", "t"), ("w", "o", 1), ("s", "o", 1, "c", 1), ("w", "o", 4),
        ("s", "o", 4, "c", 4), ("s", "o", 4, "x", 5), ("s", "q0", "own", "y", "t"), ("w", "q1", 0),
        ("s", "q1", 0, "c", 0), ("s", "q1", 0, "x", 1), ("s", "q0", "own", "z", 2), ("w", "o", 2),
        ("s", "o", 2, "c", 2), ("s", "o", 0, "y", 2), ("w", "d", 1), ("s", "d", 1, "c", 1), ("w", "d", 4),
        ("s", "d", 4, "c", 4), ("s", "d", 4, "x", 5), ("s", "g0", "own", "z", 2), ("s", "o", 4, "y", 6), ("w", "o", 5),
        ("s", "o", 5, "c", 5), ("w", "q2", 0), ("s", "q2", 0, "c", 0), ("s", "g0", "own", "y", "t"), ("w", "o", 6),
        ("s", "o", 6, "c", 6), ("w", "q1", 2), ("s", "q1", 2, "c", 2), ("s", "q2", 0, "x", 1), ("w", "q1", 1),
        ("s", "q1", 1, "c", 1), ("s", "d", "z", "z", 4), ("s", "u0", "own", "y", "t"), ("w", "q0", 0),
        ("s", "q0", 0, "c", 0),
    ),
    (
        ("w", "q2", 2), ("s", "q2", 2, "c", 2), ("s", "q2", 2, "x", 3), ("w", "q0", "c", 0), ("w", "q1", "c", 0),
        ("w", "q2", "c", 0),
    ),
    (
        ("w", "d", 5), ("s", "d", 5, "c", 5), ("w", "q0", 2), ("s", "q0", 2, "c", 2), ("s", "u0", "own", "z", 2),
        ("s", "u1", "own", "y", "t"), ("s", "q0", 2, "x", 3),
    ),
    (
        ("w", "g0", 0), ("s", "g0", 0, "c", 0), ("w", "q2", 1), ("s", "q2", 1, "c", 1), ("w", "q0", "c", 2),
        ("w", "q1", "c", 2), ("w", "q2", "c", 2),
    ),
    (
        ("w", "q0", 1), ("s", "q0", 1, "c", 1), ("s", "u1", "own", "z", 2), ("s", "g1", "own", "y", "t"),
        ("s", "g0", 0, "x", 1),
    ),
    (
        ("w", "q2", 3), ("s", "q2", 3, "c", 3), ("w", "q1", 3), ("s", "q1", 3, "c", 3), ("w", "q0", "c", 1),
        ("w", "q1", "c", 1), ("w", "q2", "c", 1),
    ),
    (
        ("w", "g0", 2), ("s", "g0", 2, "c", 2), ("w", "q0", 3), ("s", "q0", 3, "c", 3), ("w", "o", 3),
        ("s", "o", 3, "c", 3), ("s", "g1", "own", "z", 2), ("s", "o", 1, "y", 3), ("s", "g0", 2, "x", 3),
    ),
    (
        ("w", "o", 7), ("s", "o", 7, "c", 7), ("s", "d", 0, "y", 2), ("w", "q0", "c", 3), ("w", "q1", "c", 3),
        ("w", "q2", "c", 3),
    ),
    (
        ("w", "u0", 2), ("s", "u0", 2, "c", 2), ("w", "g0", 1), ("s", "g0", 1, "c", 1), ("s", "u0", 2, "x", 3),
        ("w", "o", "c", 0), ("w", "o", "c", 1), ("w", "o", "c", 2), ("w", "o", "c", 3), ("w", "o", "c", 4),
        ("w", "o", "c", 5), ("w", "o", "c", 6), ("w", "o", "c", 7),
    ),
    (
        ("w", "u0", 0), ("s", "u0", 0, "c", 0), ("s", "d", 4, "y", 6), ("w", "u1", 2), ("s", "u1", 2, "c", 2),
        ("s", "u1", 2, "x", 3), ("w", "g0", 3), ("s", "g0", 3, "c", 3), ("w", "u1", 0), ("s", "u1", 0, "c", 0),
        ("s", "g0", 3, "y", 3), ("s", "u1", 0, "x", 1), ("w", "g1", 2), ("s", "g1", 2, "c", 2), ("w", "u0", 3),
        ("s", "u0", 3, "c", 3), ("w", "g1", 0), ("s", "g1", 0, "c", 0), ("s", "u0", 3, "y", 3), ("s", "g1", 0, "x", 1),
        ("w", "u1", 3), ("s", "u1", 3, "c", 3), ("w", "d", 2), ("s", "d", 2, "c", 2), ("s", "u1", 3, "y", 3),
        ("s", "g1", 2, "x", 3), ("w", "u1", 1), ("s", "u1", 1, "c", 1), ("w", "d", 6), ("s", "d", 6, "c", 6),
        ("s", "d", 1, "y", 3),
    ),
    (
        ("w", "g1", 1), ("s", "g1", 1, "c", 1), ("s", "d", 6, "x", 7),
    ),
    (
        ("w", "u0", 1), ("s", "u0", 1, "c", 1), ("w", "g0", "c", 0), ("w", "g1", "c", 0), ("w", "u0", "c", 0),
        ("w", "u1", "c", 0),
    ),
    (),
    (),
    (
        ("w", "g1", 3), ("s", "g1", 3, "c", 3), ("w", "g0", "c", 1), ("w", "g1", "c", 1), ("w", "u0", "c", 1),
        ("w", "u1", "c", 1),
    ),
    (
        ("w", "g0", "c", 2), ("w", "g1", "c", 2), ("w", "u0", "c", 2), ("w", "u1", "c", 2),
    ),
    (),
    (
        ("w", "d", 3), ("s", "d", 3, "c", 3), ("w", "g0", "c", 3), ("w", "g1", "c", 3), ("w", "u0", "c", 3),
        ("w", "u1", "c", 3),
    ),
    (),
    (
        ("w", "d", "c", 0), ("w", "d", "c", 4),
    ),
    (
        ("w", "d", 7), ("s", "d", 7, "c", 7),
    ),
    (
        ("w", "d", "c", 1), ("w", "d", "c", 5),
    ),
    (),
    (
        ("w", "d", "c", 2), ("w", "d", "c", 6),
    ),
    (),
    (
        ("w", "d", "c", 3), ("w", "d", "c", 7),
    ),
    (),
)
AWAY_BLOCKS = {
    "attend": ((0, 0), (0, 1), (2, 0), (2, 1), (1, 0), (1, 1), (3, 0), (3, 1)),
    "gated": ((0, 0), (0, 1), (1, 0), (2, 0), (1, 1), (2, 1), (3, 0), (3, 1)),
    "down": ((0, 0), (0, 1), (1, 0), (1, 1), (2, 0), (2, 1), (3, 0), (3, 1)),
}


class Place:
    def __init__(self):
        tp = lax.axis_index("tp")
        dp = lax.axis_index("dp")
        self.z = tp
        self.dp = dp
        self.y = dp // 4
        self.x = (dp // 2) % 2
        self.c = dp % 2
        self.far = lax.rem(self.y + self.z, 2)
        self.device = {
            "x": (tp, dp + 2 - 4 * self.x),
            "y": (tp, dp + 4 - 8 * self.y),
            "c": (tp, dp + 1 - 2 * self.c),
            "z": (1 - tp, dp),
        }

    def at(self, axis, flip):
        here = getattr(self, axis)
        return 1 - here if flip else here

    def row_block(self, k, core=0):
        return (self.at("x", k & 1) * 2 + self.at("c", core)) * 2 + self.at("z", k & 2)

    def col_block(self, k, core=0):
        return (self.at("y", k & 2) * 4 + self.at("x", k & 1) * 2 + self.at("c", core)) * 2 + self.at("z", k & 4)


def remote(src, dst, send, recv, device):
    return pltpu.make_async_remote_copy(
        src_ref=src, dst_ref=dst, send_sem=send, recv_sem=recv, device_id=device, device_id_type=MESH)


class Rows:
    def __init__(self, place, buf, start, own, through, index, sems):
        self.p, self.buf, self.start, self.own, self.through = place, buf, start, own, through
        self.i, (self.send, self.r, self.rc) = index, sems
        self.n = own.shape[0]

    def block(self, k, core=0):
        return self.buf.at[self.p.row_block(k, core), pl.ds(self.start, self.n)]

    def copy(self, k, link, home):
        p = self.p
        slot = {"own": 0, "t": 4}.get(k, k)
        send = self.send.at[self.i, "xyzc".index(link), slot]
        if k == "own" or (home and k == 0):
            src = self.own
        elif k == "t":
            src = self.through
        else:
            src = self.block(k)
        if k == "own" and link == "y":
            dst, recv = self.through, self.r.at[self.i, 4]
        else:
            dst = self.block(0 if k in ("own", "t") else k)
            got = 2 if link == "z" else k ^ 1 if link == "x" else k
            recv = self.rc.at[self.i, k] if link == "c" else self.r.at[self.i, got]
        return remote(src, dst, send, recv, p.device[link])

    def wait(self, k, core):
        if k == "t":
            ref, recv = self.through, self.r.at[self.i, 4]
        else:
            ref, recv = self.block(k, core), (self.rc if core else self.r).at[self.i, k]
        remote(ref, ref, self.send.at[self.i, 0, 0], recv, self.p.device["x"]).wait_recv()

    def local(self):
        @pl.when(self.p.far == 0)
        def _():
            self.buf[self.p.row_block(0), pl.ds(self.start, self.n)] = self.own[...]


class Cols:
    def __init__(self, place, buf, own, index, sems):
        self.p, self.buf, self.own = place, buf, own
        self.n = buf.shape[-1]
        self.i, (self.send, self.r, self.rc) = index, sems

    def block(self, k, core=0):
        return self.buf.at[self.p.col_block(k, core)]

    def half(self, z):
        return self.own.at[:, pl.ds(pl.multiple_of(z * self.n, 128), self.n)]

    def copy(self, k, link, home):
        p = self.p
        if link == "z":
            return remote(self.half(1 - p.z), self.block(0), self.send.at[self.i, 2, 0], self.r.at[self.i, 4], p.device["z"])
        src = self.half(p.z) if k == 0 else self.block(k)
        got = k ^ 1 if link == "x" else k ^ 2
        recv = self.rc.at[self.i, k] if link == "c" else self.r.at[self.i, got]
        return remote(src, self.block(k), self.send.at[self.i, "xyzc".index(link), k], recv, p.device[link])

    def wait(self, k, core):
        ref, recv = self.block(k, core), (self.rc if core else self.r).at[self.i, k]
        remote(ref, ref, self.send.at[self.i, 0, 0], recv, self.p.device["x"]).wait_recv()

    def local(self):
        self.buf[self.p.col_block(0)] = self.own[:, pl.ds(pl.multiple_of(self.p.z * self.n, 128), self.n)]


def layer_kernel(wq_hbm, wk_hbm, wv_hbm, wo_hbm, wg_hbm, wu_hbm, wd_hbm, x_hbm, k_hbm, v_hbm,
                 bq, bk, bv, ga, gm, freq_ref, len_ref,
                 wqkv, wgu, wout, wdn, k_lo, k_hi, v_lo, v_hi, smalls, x1_ref, down,
                 h_ref, sc_ref, o_ref, a_ref, cos_ref, sin_ref, t_q, t_gu, w_q, w_gu, wo, wd, x_ref, small, l_sem,
                 k_sem, v_sem, s_send, s_recv, p_send, p_recv, row_s, row_r, row_c, col_s, col_r, col_c):
    place = Place()
    me = place.dp * 2 + place.z
    row_sem, col_sem = (row_s, row_r, row_c), (col_s, col_r, col_c)
    loads = [(wq_hbm, w_q.at[0]), (wk_hbm, w_q.at[1]), (wv_hbm, w_q.at[2]), (wo_hbm, wo), (wg_hbm, w_gu.at[0]),
             (wu_hbm, w_gu.at[1]), (wd_hbm, wd), (x_hbm, x_ref)]
    loads = [pltpu.make_async_copy(src, dst, l_sem.at[i]) for i, (src, dst) in enumerate(loads)]
    for load in loads:
        load.start()
    chunks = {}
    for i in range(3):
        chunks[f"q{i}"] = Rows(place, wqkv, 64 * i, w_q.at[i], t_q.at[i], i, row_sem)
    for i in range(4):
        ref = w_gu.at[i // 2, pl.ds(88 * (i % 2), 88)]
        chunks["gu"[i // 2] + str(i % 2)] = Rows(place, wgu, 88 * i, ref, t_gu.at[i], 3 + i, row_sem)
    chunks["o"] = Cols(place, wout, wo, 0, col_sem)
    chunks["d"] = Cols(place, wdn, wd, 1, col_sem)
    roles = ((0, HOME_STEPS, HOME_BLOCKS), (1, AWAY_STEPS, AWAY_BLOCKS))
    step = iter(range(len(HOME_STEPS)))

    def go():
        now = next(step)
        for far, steps, _ in roles:
            if steps[now]:
                @pl.when(place.far == far)
                def _(far=far, steps=steps):
                    for action in steps[now]:
                        chunk = chunks[action[1]]
                        if action[0] == "s":
                            chunk.copy(action[2], action[3], far == 0).start()
                        elif action[2] == "c":
                            chunk.wait(action[3], 1)
                        else:
                            chunk.wait(action[2], 0)

    def by_role(kind, i, place_of, swap=False):
        home, away = (place_of(*blocks[kind][i]) for _, _, blocks in roles)
        if swap:
            home, away = away, home
        return home + place.far * (away - home)

    def cache_copy(i):
        head = by_role("attend", i, place.row_block)
        copies = []
        for hbm, lo, hi, sem in ((k_hbm, k_lo, k_hi, k_sem), (v_hbm, v_lo, v_hi, v_sem)):
            copies.append(pltpu.make_async_copy(hbm.at[pl.ds(0, 32), head], lo.at[:, head], sem.at[2 * i]))
            copies.append(pltpu.make_async_copy(hbm.at[pl.ds(32, 32), head], hi.at[:, head], sem.at[2 * i + 1]))
        return copies

    barrier = pltpu.get_barrier_semaphore()
    for i in range(1, 16):
        other = lax.rem(me + i, 16)
        pl.semaphore_signal(barrier, inc=1, device_id=(other % 2, other // 2), device_id_type=MESH)
    for i in range(8):
        for copy in cache_copy(i):
            copy.start()
    vectors = jnp.concatenate([v[...].astype(F32) for v in (bq, bk, bv, ga, gm)] + [jnp.zeros((3, 64), F32)], axis=0)
    vectors = jnp.concatenate([vectors, vectors], axis=1)
    mine = lax.broadcasted_iota(jnp.int32, (8, 128), 1) // 64 == place.z
    vectors = jnp.where(mine, vectors, 0.0).astype(BF16)
    small[...] = vectors
    smalls[me] = vectors
    for load in loads:
        load.wait()
    pl.semaphore_wait(barrier, 15)

    def small_copy(i):
        other = lax.rem(me + i, 16)
        return remote(small, smalls.at[me], s_send.at[i], s_recv.at[i], (other % 2, other // 2))

    for i in range(1, 16):
        small_copy(i).start()
    go()

    for chunk in chunks.values():
        chunk.local()
    for i in range(1, 16):
        small_copy(i).wait_recv()

    def gain_row(i):
        pair = smalls[...].astype(F32).reshape(8, 2, 8, 128)
        rows = pair[:, 0, i] + pair[:, 1, i]
        return jnp.concatenate([rows[d:d + 1] for d in range(8)], axis=1)

    def normed(rows, i):
        inv = lax.rsqrt(jnp.mean(rows * rows, axis=-1, keepdims=True) + EPS)
        return (rows * inv * gain_row(i)).astype(BF16)

    h_ref[...] = normed(x_ref[...].astype(F32), 3)

    eye = lax.broadcasted_iota(jnp.int32, (64, 128), 1) % 64 == lax.broadcasted_iota(jnp.int32, (64, 128), 0)

    def bias_column(head, i):
        row = smalls[place.z * 8 + head].astype(F32)[i:i + 1]
        return jnp.sum(jnp.where(eye, row, 0.0), axis=1, keepdims=True)

    def attend(i):
        head = by_role("attend", i, place.row_block)
        res = dot(wqkv[head], h_ref[...], BY_ROWS)
        cos, sin = cos_ref[...], sin_ref[...]

        def rotated(start, b):
            v = (res[start:start + 64] + bias_column(head, b)).astype(BF16).astype(F32)
            lo, hi = v[:32], v[32:]
            return jnp.concatenate([lo * cos - hi * sin, hi * cos + lo * sin], axis=0).astype(BF16)

        q = rotated(0, 0).astype(F32)
        k_new = rotated(64, 1)
        v_new = (res[128:192] + bias_column(head, 2)).astype(BF16)
        lens = len_ref[...].astype(F32)
        for copy in cache_copy(i):
            copy.wait()

        for base, buf in ((0, k_lo), (32, k_hi)):
            def score_group(g, carry, base=base, buf=buf):
                rows = []
                for j in range(GROUP):
                    s = g * GROUP + j
                    kv = jnp.where(lens == (base + s).astype(F32), k_new.astype(F32), buf[s, head].astype(F32))
                    buf[s, head] = kv.astype(BF16)
                    rows.append(jnp.sum(q * kv, axis=0, keepdims=True))
                sc_ref[pl.ds(pl.multiple_of(base + g * GROUP, GROUP), GROUP)] = jnp.concatenate(rows, axis=0)
                return carry

            lax.fori_loop(0, 32 // GROUP, score_group, 0)
        slot = lax.broadcasted_iota(jnp.int32, (64, 256), 0).astype(F32)
        scores = jnp.where(slot <= lens, sc_ref[...] * 0.125, -1e30)
        e = jnp.exp(scores - jnp.max(scores, axis=0, keepdims=True))
        sc_ref[...] = (e / jnp.sum(e, axis=0, keepdims=True)).astype(BF16).astype(F32)

        acc = jnp.zeros((64, 256), F32)
        for base, buf in ((0, v_lo), (32, v_hi)):
            def value_group(g, acc, base=base, buf=buf):
                probs = sc_ref[pl.ds(pl.multiple_of(base + g * GROUP, GROUP), GROUP)]
                for j in range(GROUP):
                    s = g * GROUP + j
                    vv = jnp.where(lens == (base + s).astype(F32), v_new.astype(F32), buf[s, head].astype(F32))
                    buf[s, head] = vv.astype(BF16)
                    acc = acc + probs[j:j + 1] * vv
                return acc

            acc = lax.fori_loop(0, 32 // GROUP, value_group, acc)
        o_ref[pl.ds(pl.multiple_of(head * 64, 64), 64)] = acc.astype(BF16)

    go()
    angles = freq_ref[...] * len_ref[...].astype(F32)
    cos_ref[...] = jnp.cos(angles)
    sin_ref[...] = jnp.sin(angles)
    for i in range(8):
        attend(i)
        go()

    o = o_ref[...].T
    part, part_in, h2_ref = down, x1_ref, h_ref
    part[...] = dot(o, wout[...].reshape(1024, 512), BY_ROWS).astype(BF16)
    swap = remote(part, part_in, p_send, p_recv, place.device["z"])
    swap.start()
    go()
    swap.wait_recv()
    swap.wait_send()
    total = (part[...].astype(F32) + part_in[...].astype(F32)).astype(BF16)
    x1 = (x_ref[...].astype(F32) + total.astype(F32)).astype(BF16)
    x1_ref[...] = x1
    h2_ref[...] = normed(x1.astype(F32), 4)
    go()

    for i in range(8):
        block = by_role("gated", i, place.row_block)
        res = dot(wgu[block], h2_ref[...], BY_ROWS).astype(BF16).astype(F32)
        g, u = res[:176], res[176:]
        a_ref[block] = (g / (1.0 + jnp.exp(-g)) * u).astype(BF16)
        go()

    for i in range(8):
        pair = by_role("down", i, lambda k, core: place.col_block(k, core) // 2)
        w = wdn[pl.ds(pair * 2, 2)].reshape(128, 1408)
        cols = pl.ds(pl.multiple_of(pair * 128, 128), 128)
        down[:, cols] = dot(w, a_ref[...].reshape(1408, 256), NAT).T.astype(BF16)
        go()

    for far, steps, _ in roles:
        @pl.when(place.far == far)
        def _(far=far, steps=steps):
            for action in sum(steps, ()):
                if action[0] == "s":
                    chunks[action[1]].copy(action[2], action[3], far == 0).wait_send()

    for i in range(1, 16):
        small_copy(i).wait_send()


def store_kernel(wqkv, wgu, wout, wdn, k_lo, k_hi, v_lo, v_hi, smalls,
                 wq, wk, wv, wo, wg, wu, wd, k_out, v_out, bq, bk, bv, ga, gm, sem):
    lo, hi = pl.ds(0, 32), pl.ds(32, 32)
    pairs = [(k_lo, k_out.at[lo]), (k_hi, k_out.at[hi]), (v_lo, v_out.at[lo]), (v_hi, v_out.at[hi]),
             (wdn, wd), (wgu.at[:, pl.ds(0, 176)], wg), (wgu.at[:, pl.ds(176, 176)], wu),
             (wqkv.at[:, pl.ds(0, 64)], wq), (wqkv.at[:, pl.ds(64, 64)], wk), (wqkv.at[:, pl.ds(128, 64)], wv),
             (wout, wo)]
    copies = [pltpu.make_async_copy(src, dst, sem.at[i]) for i, (src, dst) in enumerate(pairs)]
    for copy in copies:
        copy.start()
    z = lax.axis_index("tp")
    plane = smalls[pl.ds(z * 8, 8)].astype(F32).reshape(4, 2, 8, 128)
    whole = smalls[...].astype(F32).reshape(8, 2, 8, 128)
    for i, ref in enumerate((bq, bk, bv)):
        ref[...] = (plane[:, 0, i] + plane[:, 1, i]).astype(BF16)
    for i, ref in enumerate((ga, gm)):
        ref[...] = (whole[:, 0, 3 + i] + whole[:, 1, 3 + i]).astype(BF16)
    for copy in copies:
        copy.wait()


def finish_kernel(x1, mine, peer, hid):
    total = (mine[...].astype(F32) + peer[...].astype(F32)).astype(BF16)
    hid[...] = (x1[...].astype(F32) + total.astype(F32)).astype(BF16)


def local_step(w_query, b_query, w_key, b_key, w_value, b_value, w_out, w_gate, w_up, w_down, gain_attn, gain_mlp,
               hidden, k_cache, v_cache, lengths):
    freq = np.tile((1.0 / THETA ** (np.arange(0, 64, 2) / 64)).astype(np.float32)[:, None], (1, 256))
    lens = lengths[None, :]
    rows = [v[None, :] for v in (b_query, b_key, b_value, gain_attn, gain_mlp)]
    k_view = jnp.transpose(k_cache, (1, 2, 3, 0))
    v_view = jnp.transpose(v_cache, (1, 2, 3, 0))

    vmem = pl.BlockSpec(memory_space=pltpu.VMEM)
    hbm = pl.BlockSpec(memory_space=pltpu.HBM)
    anywhere = pl.BlockSpec(memory_space=pl.ANY)
    dma = pltpu.SemaphoreType.DMA
    shapes = [(8, 192, 1024), (8, 352, 1024), (16, 64, 512), (16, 64, 1408), *[(32, 8, 64, 256)] * 4,
              (16, 8, 128), (256, 1024), (256, 1024)]
    held = pl.pallas_call(
        layer_kernel,
        out_shape=[pltpu.VMEM(s, BF16) for s in shapes],
        in_specs=[hbm] * 10 + [vmem] * 7,
        out_specs=[vmem] * 11,
        scratch_shapes=[
            pltpu.VMEM((256, 1024), BF16),
            pltpu.VMEM((64, 256), F32),
            pltpu.VMEM((512, 256), BF16),
            pltpu.VMEM((8, 176, 256), BF16),
            pltpu.VMEM((32, 256), F32),
            pltpu.VMEM((32, 256), F32),
            pltpu.VMEM((3, 64, 1024), BF16),
            pltpu.VMEM((4, 88, 1024), BF16),
            pltpu.VMEM((3, 64, 1024), BF16),
            pltpu.VMEM((2, 176, 1024), BF16),
            pltpu.VMEM((64, 1024), BF16),
            pltpu.VMEM((64, 2816), BF16),
            pltpu.VMEM((256, 1024), BF16),
            pltpu.VMEM((8, 128), BF16),
            dma((8,)),
            dma((16,)), dma((16,)), dma((16,)), dma((16,)), dma, dma,
            dma((7, 4, 5)), dma((7, 5)), dma((7, 4)), dma((2, 4, 8)), dma((2, 8)), dma((2, 8)),
        ],
        compiler_params=pltpu.CompilerParams(collective_id=0, has_side_effects=True, vmem_limit_bytes=9437184),
        name="layer",
    )(w_query, w_key, w_value, w_out, w_gate, w_up, w_down, hidden, k_view, v_view, *rows, freq, lens)

    def shape(*dims):
        return jax.ShapeDtypeStruct(dims, BF16)

    peer = lax.ppermute(held[10], "tp", [(0, 1), (1, 0)])
    outs = pl.pallas_call(
        store_kernel,
        out_shape=[shape(8, 64, 1024)] * 3 + [shape(16, 64, 512), shape(8, 176, 1024), shape(8, 176, 1024),
                   shape(16, 64, 1408), shape(*k_view.shape), shape(*v_view.shape),
                   shape(4, 128), shape(4, 128), shape(4, 128), shape(8, 128), shape(8, 128)],
        in_specs=[anywhere] * 8 + [vmem],
        out_specs=[hbm] * 9 + [vmem] * 5,
        scratch_shapes=[dma((11,))],
        compiler_params=pltpu.CompilerParams(vmem_limit_bytes=9437184),
        cost_estimate=pl.CostEstimate(flops=2 * 10**10, bytes_accessed=5 * 10**7, transcendentals=0),
        name="store",
    )(*held[:9])
    hid = pl.pallas_call(
        finish_kernel,
        out_shape=shape(256, 1024),
        in_specs=[vmem] * 3,
        out_specs=vmem,
        compiler_params=pltpu.CompilerParams(vmem_limit_bytes=9437184),
        name="finish",
    )(held[9], held[10], peer)
    wq, wk, wv, wo, wg, wu, wd, k_out, v_out, bq, bk, bv, ga, gm = outs
    flat = lambda a, n: a.reshape(-1, n)
    return (flat(wq, 1024), bq.reshape(512), flat(wk, 1024), bk.reshape(512), flat(wv, 1024), bv.reshape(512),
            flat(wo, 512), flat(wg, 1024), flat(wu, 1024), flat(wd, 1408), ga.reshape(1024), gm.reshape(1024),
            hid, jnp.transpose(k_out, (3, 0, 1, 2)), jnp.transpose(v_out, (3, 0, 1, 2)))


def solution(mesh):
    row_spec = P(("dp", "tp"), None)
    flat_spec = P(("dp", "tp"))
    cache_spec = P("dp", None, "tp", None)
    in_specs = (row_spec, flat_spec, row_spec, flat_spec, row_spec, flat_spec, row_spec, row_spec, row_spec, row_spec,
                flat_spec, flat_spec, P("dp", None), cache_spec, cache_spec, P("dp"))
    out_specs = (P("tp", None), P("tp"), P("tp", None), P("tp"), P("tp", None), P("tp"), P(None, "tp"), P("tp", None),
                 P("tp", None), P(None, "tp"), P(None), P(None), P("dp", None), cache_spec, cache_spec)
    return jax.shard_map(local_step, mesh=mesh, in_specs=in_specs, out_specs=out_specs, check_vma=False)
```
